32 devices in a mesh: seq: 16 (over z, y, core), ch: 2 (over x).
Axes of the slice: x: 2, y: 2, z: 4, core: 2. Of those that a mesh axis runs over, the one named last changes fastest.
Arguments:
- query_gate: bfloat16 [2, 2048, 2048], P('ch', 'seq'), may hold values from -6 to 6
- key_input: bfloat16 [2, 2048, 2048], P('ch', 'seq'), may hold values from -6 to 6
- value_input: bfloat16 [2, 2048, 2048], P('ch', 'seq'), may hold values from -6 to 6
- grad_output: bfloat16 [2, 2048, 2048], P('ch', 'seq'), may hold values from -6 to 6
- filter_raw: bfloat16 [2048, 2048], P('seq'), may hold values from -6 to 6
- skip_gain: float32 [2048], replicated, may hold values from 0.5 to 1.5
Outputs:
- grad_query: bfloat16 [2, 2048, 2048], P('ch', 'seq')
- grad_key: bfloat16 [2, 2048, 2048], P('ch', 'seq')
- grad_value: bfloat16 [2, 2048, 2048], P('ch', 'seq')
- grad_filter: float32 [2048, 2048], P('seq', 'ch')
The draws below stay inside these ranges and needn't reach their ends.
All inputs are finite; a program needn't handle non-finite values.
Results may differ from the reference program's by a relative error of at most 0.001.
Values sent between devices are 32-bit elements; how exact they have to be, the bound alone decides.
A program may use at most 128 MiB of HBM per device.

```python
import jax
import jax.numpy as jnp
from jax import lax

CHANNELS = 2048
SEQ_LEN = 2048
BATCH = 2


def block_levels(stream_key, extent, cuts, smallest, high):
    def one(axis_at, parts):
        draws = jax.random.uniform(jax.random.fold_in(jax.random.fold_in(stream_key, 6), axis_at), (parts,), jnp.float32, smallest / len(cuts), high / len(cuts))
        return jnp.repeat(jnp.exp(draws), extent[axis_at] // parts).reshape((-1,) + (1,) * (len(extent) - axis_at - 1))

    loudness = one(*cuts[0])
    for cut in cuts[1:]:
        loudness = loudness * one(*cut)
    return loudness


def gaussian(rng, dims, deviation, most, cuts=(), dtype=jnp.bfloat16):
    drawn = deviation * jax.random.normal(rng, dims, jnp.float32)
    if cuts:
        drawn = drawn * block_levels(rng, dims, cuts, -0.22, 0.18)
    return jnp.clip(drawn, -most, most).astype(dtype)


def setup_inputs(seed: int = 0) -> dict:
    key_list = jax.random.split(jax.random.key(seed), 7)
    return {
        "query_gate": gaussian(key_list[0], (BATCH, SEQ_LEN, CHANNELS), 1.0, 6.0, ((0, 2), (1, 16))),
        "key_input": gaussian(key_list[1], (BATCH, SEQ_LEN, CHANNELS), 1.0, 6.0, ((0, 2), (1, 16))),
        "value_input": gaussian(key_list[2], (BATCH, SEQ_LEN, CHANNELS), 1.0, 6.0, ((0, 2), (1, 16))),
        "grad_output": gaussian(key_list[3], (BATCH, SEQ_LEN, CHANNELS), 1.0, 6.0, ((0, 2), (1, 16))),
        "filter_raw": gaussian(key_list[4], (SEQ_LEN, CHANNELS), 1.0, 6.0, ((0, 16),)),
        "skip_gain": jnp.clip(jax.random.uniform(key_list[5], (CHANNELS,), jnp.float32, 0.5, 1.5), 0.5, 1.5),
    }


def block_grads(pieces):
    query_gate, key_input, value_input, grad_output, filter_raw, skip_gain = pieces
    length = 2 * SEQ_LEN
    filter_taps = filter_raw.astype(jnp.float32) * (SEQ_LEN ** -0.5)
    filter_spec = jnp.fft.rfft(filter_taps, n=length, axis=0)
    grads_query = []
    grads_key = []
    grads_value = []
    corr_total = jnp.zeros(filter_taps.shape, jnp.float32)
    for seq_index in range(BATCH):
        key_f = key_input[seq_index].astype(jnp.float32)
        value_f = value_input[seq_index].astype(jnp.float32)
        out_f = grad_output[seq_index].astype(jnp.float32)
        query_f = query_gate[seq_index].astype(jnp.float32)
        mixed_signal = key_f * value_f
        gated_grad = out_f * query_f
        mixed_spec = jnp.fft.rfft(mixed_signal, n=length, axis=0)
        gated_spec = jnp.fft.rfft(gated_grad, n=length, axis=0)
        conv_out = jnp.fft.irfft(mixed_spec * filter_spec, n=length, axis=0)[:SEQ_LEN] + skip_gain * mixed_signal
        back_grad = jnp.fft.irfft(jnp.conj(filter_spec) * gated_spec, n=length, axis=0)[:SEQ_LEN] + skip_gain * gated_grad
        corr_grad = jnp.fft.irfft(jnp.conj(mixed_spec) * gated_spec, n=length, axis=0)[:SEQ_LEN]
        grads_query.append((out_f * conv_out).astype(jnp.bfloat16))
        grads_key.append((back_grad * value_f).astype(jnp.bfloat16))
        grads_value.append((back_grad * key_f).astype(jnp.bfloat16))
        corr_total = corr_total + corr_grad
    return (jnp.stack(grads_query), jnp.stack(grads_key), jnp.stack(grads_value),
            corr_total * (SEQ_LEN ** -0.5))


def reference(query_gate, key_input, value_input, grad_output, filter_raw, skip_gain):
    channel_width = CHANNELS
    block_size = 256 if channel_width % 256 == 0 else channel_width
    groups = channel_width // block_size

    def split_channels(tensor_in):
        reshaped = tensor_in.reshape(tensor_in.shape[:-1] + (groups, block_size))
        return jnp.moveaxis(reshaped, -2, 0)

    def join_channels(tensor_in):
        reshaped = jnp.moveaxis(tensor_in, 0, -2)
        return reshaped.reshape(reshaped.shape[:-2] + (channel_width,))

    stacked = (split_channels(query_gate), split_channels(key_input), split_channels(value_input),
               split_channels(grad_output), split_channels(filter_raw), split_channels(skip_gain))
    results = lax.map(block_grads, stacked)
    return (join_channels(results[0]), join_channels(results[1]), join_channels(results[2]),
            join_channels(results[3]))
```

```python
import math

import numpy as np

import jax
import jax.numpy as jnp
from jax import lax
from jax.experimental import pallas as pl
from jax.experimental.pallas import tpu as pltpu
from jax.sharding import PartitionSpec as P


def angle_table(row_index, col_index, modulus):
    turn_count = row_index[:, None] * col_index[None, :] % modulus
    angles = turn_count.astype(jnp.float32) * (2.0 * math.pi / modulus)
    return (jnp.cos(angles), jnp.sin(angles))


def contract(pattern, table, operand):
    return jnp.einsum(
        pattern, table, operand, precision=lax.Precision.HIGHEST, preferred_element_type=jnp.float32
    )


def rotate(pattern, cos_table, sin_table, sense_sign, real_part, imag_part, want_imag):
    if imag_part is None:
        cos_term = contract(pattern, cos_table, real_part)
        return (cos_term, sense_sign * contract(pattern, sin_table, real_part))
    real_out = contract(pattern, cos_table, real_part) - sense_sign * contract(
        pattern, sin_table, imag_part
    )
    if not want_imag:
        return (real_out, None)
    imag_out = contract(pattern, cos_table, imag_part) + sense_sign * contract(
        pattern, sin_table, real_part
    )
    return (real_out, imag_out)


def twist(cos_table, sin_table, sense_sign, real_part, imag_part):
    return (
        real_part * cos_table - sense_sign * imag_part * sin_table,
        imag_part * cos_table + sense_sign * real_part * sin_table,
    )


def spectral_terms(z_real, z_imag, g_real, g_imag, h_real, h_imag):
    conv_real = z_real * h_real - z_imag * h_imag
    conv_imag = z_real * h_imag + z_imag * h_real
    back_real = h_real * g_real + h_imag * g_imag
    back_imag = h_real * g_imag - h_imag * g_real
    corr_real = z_real * g_real + z_imag * g_imag
    corr_imag = z_real * g_imag - z_imag * g_real
    return (conv_real - back_imag, conv_imag + back_real, corr_real, corr_imag)


def shards(query_gate, key_input, value_input, grad_output, filter_raw, skip_gain):
    seq_count = lax.axis_size("seq")
    key_f = key_input[0].astype(jnp.float32)
    value_f = value_input[0].astype(jnp.float32)
    out_f = grad_output[0].astype(jnp.float32)
    mixed = key_f * value_f
    gated = out_f * query_gate[0].astype(jnp.float32)
    tokens, channels = mixed.shape
    seq_length = tokens * seq_count
    full_length = 2 * seq_length
    inverse_scale = 1.0 / full_length
    filter_taps = filter_raw.astype(jnp.float32) * seq_length ** (-0.5)
    freq_one = jnp.arange(2 * seq_count, dtype=jnp.int32)
    block_index = jnp.arange(seq_count, dtype=jnp.int32)
    offset_index = jnp.arange(tokens, dtype=jnp.int32)
    cos_one, sin_one = angle_table(freq_one, block_index, 2 * seq_count)
    cos_inv, sin_inv = angle_table(block_index, freq_one, 2 * seq_count)
    cos_two, sin_two = angle_table(offset_index, offset_index, tokens)
    local_width = channels // seq_count
    arrived = (
        lax.all_to_all(mixed.T, "seq", split_axis=0, concat_axis=1, tiled=True),
        lax.all_to_all(gated.T, "seq", split_axis=0, concat_axis=1, tiled=True),
        lax.all_to_all(filter_taps.T, "seq", split_axis=0, concat_axis=1, tiled=True),
    )
    cos_tw, sin_tw = angle_table(freq_one, offset_index, full_length)
    spectra = []
    for line_data in arrived:
        lines = line_data.reshape(local_width, seq_count, tokens)
        real_part, imag_part = rotate("kn,cnm->ckm", cos_one, sin_one, -1.0, lines, None, True)
        real_part, imag_part = twist(cos_tw, sin_tw, -1.0, real_part, imag_part)
        spectra.append(rotate("jm,ckm->ckj", cos_two, sin_two, -1.0, real_part, imag_part, True))
    packed_real, packed_imag, corr_real, corr_imag = spectral_terms(
        spectra[0][0], spectra[0][1], spectra[1][0], spectra[1][1], spectra[2][0], spectra[2][1]
    )
    pr_mid, pi_mid = rotate("mj,ckj->ckm", cos_two, sin_two, 1.0, packed_real, packed_imag, True)
    pr_mid, pi_mid = twist(cos_tw, sin_tw, 1.0, pr_mid, pi_mid)
    cr_mid, ci_mid = rotate("mj,ckj->ckm", cos_two, sin_two, 1.0, corr_real, corr_imag, True)
    cr_mid, ci_mid = twist(cos_tw, sin_tw, 1.0, cr_mid, ci_mid)
    conv_lines, back_lines = rotate("nk,ckm->cnm", cos_inv, sin_inv, 1.0, pr_mid, pi_mid, True)
    corr_lines = rotate("nk,ckm->cnm", cos_inv, sin_inv, 1.0, cr_mid, ci_mid, False)[0]
    conv_lines = (conv_lines * inverse_scale).reshape(local_width, seq_length)
    back_lines = (back_lines * inverse_scale).reshape(local_width, seq_length)
    corr_lines = (corr_lines * inverse_scale).reshape(local_width, seq_length)
    returned = (
        lax.all_to_all(conv_lines, "seq", split_axis=1, concat_axis=0, tiled=True),
        lax.all_to_all(back_lines, "seq", split_axis=1, concat_axis=0, tiled=True),
        lax.all_to_all(corr_lines, "seq", split_axis=1, concat_axis=0, tiled=True),
    )
    conv_time = returned[0].T
    back_time = returned[1].T
    corr_time = returned[2].T
    conv_full = conv_time + skip_gain * mixed
    back_full = back_time + skip_gain * gated
    grad_query = (out_f * conv_full).astype(jnp.bfloat16)[None]
    grad_key = (back_full * value_f).astype(jnp.bfloat16)[None]
    grad_value = (back_full * key_f).astype(jnp.bfloat16)[None]
    grad_filter = lax.psum_scatter(
        corr_time * seq_length ** (-0.5), "ch", scatter_dimension=1, tiled=True
    )
    return (grad_query, grad_key, grad_value, grad_filter)


LANES = 128
VMEM_LIMIT = 60 * 1024 * 1024


def times_root(pair, turn, size):
    real, imag = pair
    turn %= size
    if turn == 0:
        return pair
    if 4 * turn == size:
        return (-imag, real)
    if 2 * turn == size:
        return (-real, -imag)
    if 4 * turn == 3 * size:
        return (imag, -real)
    cosine = math.cos(2.0 * math.pi * turn / size)
    sine = math.sin(2.0 * math.pi * turn / size)
    return (real * cosine - imag * sine, real * sine + imag * cosine)


def complex_dft(values, sense):
    size = len(values)
    if size == 1:
        return values
    even = complex_dft(values[0::2], sense)
    odd = complex_dft(values[1::2], sense)
    low, high = [], []
    for k in range(size // 2):
        er, ei = even[k]
        tr, ti = times_root(odd[k], sense * k, size)
        low.append((er + tr, ei + ti))
        high.append((er - tr, ei - ti))
    return low + high


def half_spectrum(values, size):
    if size == 2:
        return [(values[0] + values[1], None), (values[0] - values[1], None)]
    half, quarter = size // 2, size // 4
    if len(values) == half:
        total, difference = values, values
    else:
        total = [values[n] + values[n + half] for n in range(half)]
        difference = [values[n] - values[n + half] for n in range(half)]
    out = [None] * (half + 1)
    out[0::2] = half_spectrum(total, half)
    turned = [times_root((difference[n], -difference[n + quarter]), -n, size) for n in range(quarter)]
    for index, (real, imag) in enumerate(complex_dft(turned, -1)):
        k = 1 + 4 * index
        if k <= half:
            out[k] = (real, imag)
        else:
            out[size - k] = (real, -imag)
    return out


def real_from_half(terms, size, first_half):
    if size == 2:
        return [terms[0][0] + terms[1][0], terms[0][0] - terms[1][0]]
    half, quarter = size // 2, size // 4
    even = real_from_half(terms[0::2], half, False)
    chosen = []
    for index in range(quarter):
        k = 1 + 4 * index
        if k <= half:
            chosen.append(terms[k])
        else:
            real, imag = terms[size - k]
            chosen.append((real, -imag))
    turned = [times_root(pair, n, size) for n, pair in enumerate(complex_dft(chosen, 1))]
    odd = [pair[0] for pair in turned] + [-pair[1] for pair in turned]
    out = [even[n] + odd[n] for n in range(half)]
    if first_half:
        return out
    return out + [even[n] - odd[n] for n in range(half)]


def split_bf16(value):
    high = value.astype(jnp.bfloat16)
    return high, (value - high.astype(jnp.float32)).astype(jnp.bfloat16)


def three_dot(table_high, table_low, value):
    high, low = split_bf16(value)
    dot = lambda a, b: jnp.dot(a, b, preferred_element_type=jnp.float32)
    return dot(table_high, high) + (dot(table_high, low) + dot(table_low, high))


QUARTERS = 4
QUARTER = LANES // QUARTERS
PLAN = ((0, 1), (0, 2), (0, 3), (1, 1), (1, 2), (1, 3), (2, 1), (2, 2))
PLANES = 4
PLAN_STEP = 3
JOB_SLOTS = 3
LOCAL_SLOTS = 5


def left_mask(shape):
    return lax.broadcasted_iota(jnp.int32, shape, 1) < LANES // 2


def even_mask(shape):
    return lax.broadcasted_iota(jnp.int32, shape, 1) & QUARTER == 0


def swap_halves(value):
    return pltpu.roll(value, LANES // 2, 1)


def turn_quarters(value, count):
    count %= QUARTERS
    return pltpu.roll(value, count * QUARTER, 1) if count else value


def choose_quarters(values):
    lane = lax.broadcasted_iota(jnp.int32, values[0].shape, 1)
    out = values[-1]
    for index in reversed(range(QUARTERS - 1)):
        out = jnp.where(lane < (index + 1) * QUARTER, values[index], out)
    return out


def transpose_quarters(values):
    turned = [turn_quarters(value, index) for index, value in enumerate(values)]
    mixed = [choose_quarters([turned[(u - a) % QUARTERS] for u in range(QUARTERS)]) for a in range(QUARTERS)]
    return [turn_quarters(value, -index) for index, value in enumerate(mixed)]


def interleave(one, two):
    even = even_mask(one.shape)
    return jnp.where(even, one, turn_quarters(two, 1)), jnp.where(even, turn_quarters(one, -1), two)


def offsets(count):
    return sorted(range(count), key=lambda step: abs(2 * step - count))


def greet_all(seq_count, ch_count, me_seq, me_ch):
    barrier = pltpu.get_barrier_semaphore()
    for step in offsets(seq_count):
        for turn in range(ch_count):
            if step or turn:
                partner = {"seq": lax.rem(me_seq + step, seq_count), "ch": lax.rem(me_ch + turn, ch_count)}
                pl.semaphore_signal(barrier, inc=1, device_id=partner, device_id_type=pl.DeviceIdType.MESH)
    return barrier


def layer_kernel(
    seq_count, ch_count,
    query_ref, key_ref, value_ref, out_ref, filter_ref, skip_ref, fwd_ref, inv_ref, tw_ref,
    gq_ref, gk_ref, gv_ref, gf_ref,
    send, send_half, taps_send, recv, recv_half, taps_recv,
    result, result_half, corr_result, back, back_half, corr, corr_far,
    lines, taps_lines, spec, taps_spec, corr_spec, tw_scr,
    send_sem, half_send_sem, taps_send_sem, local_taps_send_sem,
    recv_sem, half_recv_sem, taps_recv_sem,
    back_send_sem, back_half_send_sem, corr_send_sem,
    back_sem, back_half_sem, corr_sem, corr_far_sem,
):
    me_seq, me_ch = lax.axis_index("seq"), lax.axis_index("ch")
    tokens, channels = key_ref.shape
    half_tokens, part_tokens = tokens // 2, tokens // QUARTERS
    half_seq = seq_count // 2
    width = seq_count // PLANES
    plane, place = lax.div(me_seq, width), lax.rem(me_seq, width)
    high = lax.div(plane, PLANES // 2)
    low = 1 - high
    scale = (seq_count * tokens) ** -0.5
    side_channels = channels // ch_count
    jobs = QUARTERS * len(PLAN)
    far_groups = [group for group, (_, owner) in enumerate(PLAN) if owner >= PLANES // 2]
    far_jobs = QUARTERS * len(far_groups)
    own = [[group for group, (at, owner) in enumerate(PLAN) if owner == p] for p in range(PLANES)]
    own[0] = far_groups
    kept = [len(groups) for groups in own]
    barrier = greet_all(seq_count, ch_count, me_seq, me_ch)

    def start(source, target, seq, ch, send_at, recv_at):
        pltpu.make_async_remote_copy(
            src_ref=source, dst_ref=target, send_sem=send_at, recv_sem=recv_at,
            device_id={"seq": seq, "ch": ch}, device_id_type=pl.DeviceIdType.MESH,
        ).start()

    def span(ref, count, send_at, recv_at):
        return pltpu.make_async_remote_copy(
            src_ref=ref.at[pl.ds(0, count)], dst_ref=ref.at[pl.ds(0, count)], send_sem=send_at, recv_sem=recv_at,
            device_id={"seq": me_seq, "ch": me_ch}, device_id_type=pl.DeviceIdType.MESH,
        )

    def arrive(ref, count, sem):
        span(ref, count, sem, sem).wait_recv()

    def depart(ref, count, sem):
        if count:
            span(ref, count, sem, sem).wait_send()

    def prepare(group, side):
        lanes = pl.ds(pl.multiple_of(side * side_channels + group * LANES, LANES), LANES)
        base = side * jobs + QUARTERS * group

        def body(chunk, carry):
            pieces = []
            rows = [pl.ds(pl.multiple_of(chunk * 16 + first, 16), 16) for first in (0, half_tokens)]
            for one, two in ((key_ref, value_ref), (out_ref, query_ref)):
                for at in rows:
                    pieces.append(one[at, lanes].astype(jnp.float32) * two[at, lanes].astype(jnp.float32))
            for index, piece in enumerate(transpose_quarters(pieces)):
                send[base + index, rows[0], :] = piece
            return carry

        lax.fori_loop(0, half_tokens // 16, body, 0)

    def halve(group, side):
        far = group - 1 - lax.div(group, PLAN_STEP)
        for index in range(QUARTERS):
            piece = send[side * jobs + QUARTERS * group + index]
            top, bottom = piece[:part_tokens], piece[part_tokens:]
            send_half[side * far_jobs + QUARTERS * far + index] = jnp.where(left_mask(top.shape), top, swap_halves(bottom))

    def prepare_taps(group):
        lanes = pl.ds(pl.multiple_of(me_ch * side_channels + group * LANES, LANES), LANES)
        pieces = [filter_ref[part_tokens * k:part_tokens * (k + 1), lanes].astype(jnp.float32) * scale for k in range(QUARTERS)]
        for index, piece in enumerate(transpose_quarters(pieces)):
            taps_send[QUARTERS * group + index] = piece

    def turns():
        return [(step, turn) for step in offsets(width) for turn in reversed(range(ch_count))]

    def send_taps(group):
        slot = lax.div(group, PLAN_STEP)
        owner = 1 + lax.rem(group, PLAN_STEP)
        far = group - 1 - slot
        is_far = owner > 1
        for step in offsets(width):
            at = lax.rem(place + step, width)
            source = taps_send.at[QUARTERS * group + at]

            def to_owner():
                start(source, taps_recv.at[slot * seq_count + me_seq], owner * width + at, me_ch, taps_send_sem, taps_recv_sem.at[slot])

            def to_local():
                start(source, taps_recv.at[far * half_seq + me_seq], at, me_ch, local_taps_send_sem, taps_recv_sem.at[far])

            if step:
                to_owner()
                pl.when(is_far & (low == 1))(to_local)
            else:
                pl.when(plane != owner)(to_owner)

                @pl.when(plane == owner)
                def _():
                    taps_recv[slot * seq_count + me_seq] = taps_send[QUARTERS * group + place]

                pl.when(is_far & (low == 1) & (plane != 0))(to_local)

                @pl.when(is_far & (plane == 0))
                def _():
                    taps_recv[far * half_seq + me_seq] = taps_send[QUARTERS * group + place]

    def send_group(group):
        slot = lax.div(group, PLAN_STEP)
        owner = 1 + lax.rem(group, PLAN_STEP)
        far = group - 1 - slot

        @pl.when((owner > 1) & (low == 1))
        def _():
            for step, turn in turns():
                at, ch = lax.rem(place + step, width), lax.rem(me_ch + turn, ch_count)
                start(
                    send_half.at[ch * far_jobs + QUARTERS * far + at],
                    recv_half.at[slot * seq_count + me_ch * half_seq + me_seq],
                    owner * width + at, ch, half_send_sem, half_recv_sem.at[slot],
                )

        def whole(target_plane, target_slot, index):
            for step, turn in turns():
                at, ch = lax.rem(place + step, width), lax.rem(me_ch + turn, ch_count)

                def go():
                    start(send.at[ch * jobs + QUARTERS * group + at], recv.at[index], target_plane * width + at, ch, send_sem, recv_sem.at[target_slot])

                if step or turn:
                    go()
                else:
                    pl.when(plane != target_plane)(go)

                    @pl.when(plane == target_plane)
                    def _():
                        recv[index] = send[me_ch * jobs + QUARTERS * group + place]

        @pl.when((owner == 1) | (high == 1))
        def _():
            whole(owner, slot, (slot * ch_count + me_ch) * seq_count + me_seq)

        @pl.when((owner > 1) & (low == 1))
        def _():
            whole(0, far, (far * ch_count + me_ch) * half_seq + me_seq)

    def ready(group):
        other = lax.rem(me_ch + 1, ch_count)
        prepare_taps(group)
        prepare(group, other)
        prepare(group, me_ch)
        slot = lax.div(group, PLAN_STEP)

        @pl.when((group - PLAN_STEP * slot > 0) & (low == 1))
        def _():
            halve(group, 0)
            halve(group, 1)

    ready(0)
    pl.semaphore_wait(barrier, seq_count * ch_count - 1)

    def feed(group, carry):
        pl.when(group > 0)(lambda: ready(group))
        send_group(group)
        send_taps(group)
        return carry

    lax.fori_loop(0, len(PLAN), feed, 0)
    for k in range(seq_count + 1):
        for part in range(2):
            tw_scr[k, part] = jnp.broadcast_to(tw_ref[part, :, k:k + 1], (tokens, LANES))

    def analyse(source, target, blocks):
        def body(chunk, carry):
            rows = pl.ds(pl.multiple_of(chunk * 8, 8), 8)
            for k, (real, imag) in enumerate(half_spectrum([source[n, rows, :] for n in range(blocks)], 2 * blocks)):
                target[k, 0, rows, :] = real
                target[k, 1, rows, :] = jnp.zeros_like(real) if imag is None else imag
            return carry

        lax.fori_loop(0, tokens // 8, body, 0)

    def synthesise(source, target, blocks):
        def body(chunk, carry):
            rows = pl.ds(pl.multiple_of(chunk * 8, 8), 8)
            terms = [(source[k, 0, rows, :], source[k, 1, rows, :]) for k in range(blocks + 1)]
            for n, value in enumerate(real_from_half(terms, 2 * blocks, True)):
                target[n, rows, :] = value
            return carry

        lax.fori_loop(0, tokens // 8, body, 0)

    def across(table, real, imag):
        both = three_dot(table[0], table[1], jnp.concatenate([real, imag], axis=0))
        return both[:tokens], both[tokens:]

    def convolve(blocks):
        stride = seq_count // blocks
        analyse(lines, spec, blocks)
        analyse(taps_lines, taps_spec, blocks)
        forward = (fwd_ref[0], fwd_ref[1])
        inverse = (inv_ref[0], inv_ref[1])

        def middle(k, carry):
            cosine, sine = tw_scr[stride * k, 0], tw_scr[stride * k, 1]
            real, imag = spec[k, 0], spec[k, 1]
            real, imag = real * cosine + imag * sine, imag * cosine - real * sine
            tr, ti = taps_spec[k, 0], taps_spec[k, 1]
            tr, ti = tr * cosine + ti * sine, ti * cosine - tr * sine
            real, imag = across(forward, jnp.concatenate([real, tr], axis=1), jnp.concatenate([imag, ti], axis=1))
            h_r, h_i = real[:, LANES:], imag[:, LANES:]
            a_r, a_i = real[:, :LANES], imag[:, :LANES]
            h_i = jnp.where(left_mask(h_i.shape), h_i, -h_i)
            g_r, g_i = swap_halves(a_r), swap_halves(a_i)
            c_r, c_i = a_r * g_r + a_i * g_i, a_r * g_i - a_i * g_r
            p_r, p_i = a_r * h_r - a_i * h_i, a_r * h_i + a_i * h_r
            weight = jnp.where((k == 0) | (k == blocks), 0.5 / (blocks * tokens), 1.0 / (blocks * tokens))
            cosine, sine = cosine * weight, sine * weight
            both_r, both_i = across(inverse, jnp.concatenate([p_r, c_r], axis=1), jnp.concatenate([p_i, c_i], axis=1))
            br, bi = both_r[:, :LANES], both_i[:, :LANES]
            cr, ci = both_r[:, LANES:], both_i[:, LANES:]
            spec[k, 0] = br * cosine - bi * sine
            spec[k, 1] = bi * cosine + br * sine
            corr_spec[k, 0] = cr * cosine - ci * sine
            corr_spec[k, 1] = ci * cosine + cr * sine
            return carry

        lax.fori_loop(0, blocks + 1, middle, 0)
        synthesise(spec, lines, blocks)
        synthesise(corr_spec, taps_lines, blocks)

    def open_taps(slot, blocks):
        def body(n, carry):
            packed = taps_recv[slot * blocks + n]
            turned = [turn_quarters(packed, count) for count in range(QUARTERS)]
            for k in range(QUARTERS):
                taps_lines[n, part_tokens * k:part_tokens * (k + 1), :] = choose_quarters([turned[(u - k) % QUARTERS] for u in range(QUARTERS)])
            return carry

        lax.fori_loop(0, blocks, body, 0)

    def open_whole(slot, blocks, first):
        def body(n, carry):
            base = slot * ch_count * blocks + n
            top, bottom = interleave(recv[base], recv[base + blocks])
            lines[n, :half_tokens, :] = top
            lines[n, half_tokens:, :] = bottom
            return carry

        lax.fori_loop(first, blocks, body, 0)

    def open_half(slot):
        def body(n, carry):
            one, two = recv_half[slot * seq_count + n], recv_half[slot * seq_count + half_seq + n]
            left = left_mask(one.shape)
            for first in (0, part_tokens):
                top, bottom = interleave(one, two)
                lines[n, first:first + part_tokens, :] = jnp.where(left, top, 0.0)
                lines[n, half_tokens + first:half_tokens + first + part_tokens, :] = jnp.where(left, bottom, 0.0)
                one, two = swap_halves(one), swap_halves(two)
            return carry

        lax.fori_loop(0, half_seq, body, 0)

    def close_whole(slot, blocks, first):
        def body(n, carry):
            base = slot * ch_count * blocks + n
            one, two = interleave(lines[n, :half_tokens, :], lines[n, half_tokens:, :])
            result[base] = one
            result[base + blocks] = two
            return carry

        lax.fori_loop(first, blocks, body, 0)

    def close_half(slot):
        def body(n, carry):
            for index, piece in enumerate(interleave(lines[n, :half_tokens, :], lines[n, half_tokens:, :])):
                top, bottom = piece[:part_tokens], piece[part_tokens:]
                result_half[slot * seq_count + index * half_seq + n] = jnp.where(left_mask(top.shape), swap_halves(bottom), top)
            return carry

        lax.fori_loop(0, half_seq, body, 0)

    def close_corr(slot, blocks):
        def body(n, carry):
            pieces = []
            for k in range(QUARTERS):
                piece = taps_lines[n, part_tokens * k:part_tokens * (k + 1), :]
                pieces.append(turn_quarters((piece + turn_quarters(piece, -1)) * scale, k))
            corr_result[slot * blocks + n] = choose_quarters(pieces)
            return carry

        lax.fori_loop(0, blocks, body, 0)

    def deliver(slot, blocks, group, first, count):
        job = QUARTERS * group + place
        at_round = lax.div(group, PLAN_STEP)
        base = slot * ch_count * blocks
        for step in offsets(count):
            seq = first + lax.rem(me_seq + step, count)
            for turn in range(ch_count):
                ch = lax.rem(me_ch + turn, ch_count)
                if step or turn:
                    start(result.at[base + ch * blocks + seq], back.at[me_ch * jobs + job], seq, ch, back_send_sem, back_sem.at[at_round])
            if step:
                start(corr_result.at[slot * blocks + seq], corr.at[job], seq, me_ch, corr_send_sem, corr_sem.at[at_round])
        back[me_ch * jobs + job] = result[base + me_ch * blocks + me_seq]
        corr[job] = corr_result[slot * blocks + me_seq]

    def deliver_half(slot, group):
        far = QUARTERS * (group - 1 - slot) + place
        for step in offsets(half_seq):
            seq = lax.rem(me_seq + step, half_seq)
            for turn in range(ch_count):
                ch = lax.rem(me_ch + turn, ch_count)
                start(
                    result_half.at[slot * seq_count + ch * half_seq + seq], back_half.at[me_ch * far_jobs + far],
                    seq, ch, back_half_send_sem, back_half_sem.at[slot],
                )
            start(corr_result.at[slot * seq_count + seq], corr_far.at[far], seq, me_ch, corr_send_sem, corr_far_sem.at[slot])

    others = seq_count * ch_count - 1

    def owner_job(slot, carry):
        group = PLAN_STEP * slot + plane - 1
        arrive(taps_recv, seq_count - 1, taps_recv_sem.at[slot])
        open_taps(slot, seq_count)

        @pl.when(high == 0)
        def _():
            arrive(recv, others, recv_sem.at[slot])
            open_whole(slot, seq_count, 0)

        @pl.when(high == 1)
        def _():
            arrive(recv_half, seq_count, half_recv_sem.at[slot])
            open_half(slot)
            arrive(recv, seq_count - 1, recv_sem.at[slot])
            open_whole(slot, seq_count, half_seq)

        convolve(seq_count)
        close_corr(slot, seq_count)

        @pl.when(high == 0)
        def _():
            close_whole(slot, seq_count, 0)
            deliver(slot, seq_count, group, 0, seq_count)

        @pl.when(high == 1)
        def _():
            close_half(slot)
            close_whole(slot, seq_count, half_seq)
            deliver_half(slot, group)
            deliver(slot, seq_count, group, half_seq, half_seq)

        return carry

    def local_job(slot, carry):
        group = slot + 1 + lax.div(slot, 2)
        arrive(taps_recv, half_seq - 1, taps_recv_sem.at[slot])
        open_taps(slot, half_seq)
        arrive(recv, seq_count - 1, recv_sem.at[slot])
        open_whole(slot, half_seq, 0)
        convolve(half_seq)
        close_corr(slot, half_seq)
        close_whole(slot, half_seq, 0)
        deliver(slot, half_seq, group, 0, half_seq)
        return carry

    @pl.when(plane > 0)
    def _():
        lax.fori_loop(0, JOB_SLOTS - lax.div(plane, PLANES - 1), owner_job, 0)

    @pl.when(plane == 0)
    def _():
        lax.fori_loop(0, LOCAL_SLOTS, local_job, 0)

    def finish(group, side):
        lanes = pl.ds(pl.multiple_of(side * side_channels + group * LANES, LANES), LANES)
        base = side * jobs + QUARTERS * group
        skip = skip_ref[:, lanes]

        def body(chunk, carry):
            rows = [pl.ds(pl.multiple_of(chunk * 16 + first, 16), 16) for first in (0, half_tokens)]
            pieces = transpose_quarters([back[base + index, rows[0], :] for index in range(QUARTERS)])
            for at, conv, behind in zip(rows, pieces[:2], pieces[2:]):
                query_f = query_ref[at, lanes].astype(jnp.float32)
                key_f = key_ref[at, lanes].astype(jnp.float32)
                value_f = value_ref[at, lanes].astype(jnp.float32)
                out_f = out_ref[at, lanes].astype(jnp.float32)
                conv = conv + skip * (key_f * value_f)
                behind = behind + skip * (out_f * query_f)
                gq_ref[at, lanes] = (out_f * conv).astype(jnp.bfloat16)
                gk_ref[at, lanes] = (behind * value_f).astype(jnp.bfloat16)
                gv_ref[at, lanes] = (behind * key_f).astype(jnp.bfloat16)
            return carry

        lax.fori_loop(0, half_tokens // 16, body, 0)

    def finish_corr(group):
        lanes = pl.ds(pl.multiple_of(group * LANES, LANES), LANES)
        pieces = transpose_quarters([corr[QUARTERS * group + index] for index in range(QUARTERS)])
        for k, piece in enumerate(pieces):
            gf_ref[part_tokens * k:part_tokens * (k + 1), lanes] = piece

    def join_half(far, group):
        for side in range(ch_count):
            for index in range(QUARTERS):
                piece = back_half[side * far_jobs + QUARTERS * far + index]
                left = left_mask(piece.shape)
                place_at = side * jobs + QUARTERS * group + index
                back[place_at, :part_tokens, :] += jnp.where(left, 0.0, piece)
                back[place_at, part_tokens:, :] += jnp.where(left, 0.0, swap_halves(piece))
        for index in range(QUARTERS):
            corr[QUARTERS * group + index] += corr_far[QUARTERS * far + index]

    for at_round in range(JOB_SLOTS):
        groups = [group for group, (when, _) in enumerate(PLAN) if when == at_round]
        for p in range(PLANES):
            mine = sum(PLAN[group][0] == at_round for group in own[p])

            @pl.when(plane == p)
            def _():
                arrive(back, QUARTERS * ch_count * len(groups) - mine, back_sem.at[at_round])
                arrive(corr, QUARTERS * len(groups) - mine, corr_sem.at[at_round])

        @pl.when(low == 1)
        def _():
            count = QUARTERS * sum(group in far_groups for group in groups)
            arrive(back_half, count * ch_count, back_half_sem.at[at_round])
            arrive(corr_far, count, corr_far_sem.at[at_round])
            for group in groups:
                if group in far_groups:
                    join_half(far_groups.index(group), group)

        def finish_group(index, carry):
            group = groups[0] + index
            finish(group, 0)
            finish(group, 1)
            finish_corr(group)
            return carry

        lax.fori_loop(0, len(groups), finish_group, 0)

    for p in range(PLANES):
        is_low = p < PLANES // 2
        count = kept[p]

        @pl.when(plane == p)
        def _():
            depart(send, ch_count * jobs - count, send_sem)
            depart(send_half, ch_count * far_jobs if is_low else 0, half_send_sem)
            depart(taps_send, jobs - (count if p else 0), taps_send_sem)
            depart(taps_send, far_jobs - (0 if p else count) if is_low else 0, local_taps_send_sem)
            whole = (others if is_low else seq_count - 1) if p else seq_count - 1
            depart(result, count * whole, back_send_sem)
            depart(result_half, 0 if is_low else count * seq_count, back_half_send_sem)
            depart(corr_result, count * ((seq_count if p else half_seq) - 1), corr_send_sem)


def tables(seq_count, tokens):
    index = np.arange(tokens)
    angle = 2.0 * np.pi / tokens * (index[:, None] * index[None, :] % tokens)
    cosine, sine = np.cos(angle), np.sin(angle)
    forward = np.block([[cosine, sine], [-sine, cosine]]).astype(np.float32)
    inverse = np.block([[cosine, -sine], [sine, cosine]]).astype(np.float32)

    def pieces(table):
        table = jnp.asarray(table)
        return jnp.stack(split_bf16(table))

    turn = 2.0 * np.pi / (2 * seq_count * tokens) * (np.arange(seq_count + 1)[:, None] * index[None, :])
    twiddle = jnp.asarray(np.stack([np.cos(turn).T, np.sin(turn).T]).astype(np.float32))
    return pieces(forward), pieces(inverse), twiddle


def fast_shards(query_gate, key_input, value_input, grad_output, filter_raw, skip_gain):
    seq_count, ch_count = lax.axis_size("seq"), lax.axis_size("ch")
    _, tokens, channels = key_input.shape
    vmem = pl.BlockSpec(memory_space=pltpu.VMEM)
    jobs = QUARTERS * len(PLAN)
    far_jobs = QUARTERS * LOCAL_SLOTS
    whole = lambda count: pltpu.VMEM((count, tokens // 2, LANES), jnp.float32)
    part = lambda count: pltpu.VMEM((count, tokens // QUARTERS, LANES), jnp.float32)
    spectrum = pltpu.VMEM((seq_count + 1, 2, tokens, LANES), jnp.float32)
    lines = pltpu.VMEM((seq_count, tokens, LANES), jnp.float32)
    slots = JOB_SLOTS * seq_count
    single = pltpu.SemaphoreType.DMA
    several = lambda count: pltpu.SemaphoreType.DMA((count,))
    grads = pl.pallas_call(
        lambda *refs: layer_kernel(seq_count, ch_count, *refs),
        in_specs=[vmem] * 9,
        out_specs=[vmem] * 4,
        out_shape=[jax.ShapeDtypeStruct((tokens, channels), jnp.bfloat16)] * 3
        + [jax.ShapeDtypeStruct((tokens, channels // ch_count), jnp.float32)],
        scratch_shapes=[
            whole(ch_count * jobs), part(ch_count * far_jobs), part(jobs), whole(ch_count * slots), part(slots), part(slots),
            whole(ch_count * slots), part(slots), part(slots), whole(ch_count * jobs), part(ch_count * far_jobs), part(jobs), part(far_jobs),
            lines, lines, spectrum, spectrum, spectrum, spectrum,
            single, single, single, single,
            several(LOCAL_SLOTS), several(JOB_SLOTS), several(LOCAL_SLOTS),
            single, single, single,
            several(JOB_SLOTS), several(JOB_SLOTS), several(JOB_SLOTS), several(JOB_SLOTS),
        ],
        compiler_params=pltpu.CompilerParams(vmem_limit_bytes=VMEM_LIMIT, collective_id=0, has_side_effects=True),
        name="layer",
    )(query_gate[0], key_input[0], value_input[0], grad_output[0], filter_raw, skip_gain[None], *tables(seq_count, tokens))
    return (grads[0][None], grads[1][None], grads[2][None], grads[3])


def solution(mesh):
    in_specs = (
        P("ch", "seq", None),
        P("ch", "seq", None),
        P("ch", "seq", None),
        P("ch", "seq", None),
        P("seq", None),
        P(),
    )
    out_specs = (P("ch", "seq", None), P("ch", "seq", None), P("ch", "seq", None), P("seq", "ch"))

    def body(*arrays):
        seq_count, ch_count = mesh.shape["seq"], mesh.shape["ch"]
        _, tokens, channels = arrays[0].shape
        fits = ch_count == 2 and tokens == LANES and seq_count == PLANES * QUARTERS and channels == ch_count * len(PLAN) * LANES
        return (fast_shards if fits else shards)(*arrays)

    return jax.shard_map(body, mesh=mesh, in_specs=in_specs, out_specs=out_specs, check_vma=False)
```

```python
import math

import numpy as np

import jax
import jax.numpy as jnp
from jax import lax
from jax.experimental import pallas as pl
from jax.experimental.pallas import tpu as pltpu
from jax.sharding import PartitionSpec as P


def angle_table(row_index, col_index, modulus):
    turn_count = row_index[:, None] * col_index[None, :] % modulus
    angles = turn_count.astype(jnp.float32) * (2.0 * math.pi / modulus)
    return (jnp.cos(angles), jnp.sin(angles))


def contract(pattern, table, operand):
    return jnp.einsum(
        pattern, table, operand, precision=lax.Precision.HIGHEST, preferred_element_type=jnp.float32
    )


def rotate(pattern, cos_table, sin_table, sense_sign, real_part, imag_part, want_imag):
    if imag_part is None:
        cos_term = contract(pattern, cos_table, real_part)
        return (cos_term, sense_sign * contract(pattern, sin_table, real_part))
    real_out = contract(pattern, cos_table, real_part) - sense_sign * contract(
        pattern, sin_table, imag_part
    )
    if not want_imag:
        return (real_out, None)
    imag_out = contract(pattern, cos_table, imag_part) + sense_sign * contract(
        pattern, sin_table, real_part
    )
    return (real_out, imag_out)


def twist(cos_table, sin_table, sense_sign, real_part, imag_part):
    return (
        real_part * cos_table - sense_sign * imag_part * sin_table,
        imag_part * cos_table + sense_sign * real_part * sin_table,
    )


def spectral_terms(z_real, z_imag, g_real, g_imag, h_real, h_imag):
    conv_real = z_real * h_real - z_imag * h_imag
    conv_imag = z_real * h_imag + z_imag * h_real
    back_real = h_real * g_real + h_imag * g_imag
    back_imag = h_real * g_imag - h_imag * g_real
    corr_real = z_real * g_real + z_imag * g_imag
    corr_imag = z_real * g_imag - z_imag * g_real
    return (conv_real - back_imag, conv_imag + back_real, corr_real, corr_imag)


def shards(query_gate, key_input, value_input, grad_output, filter_raw, skip_gain):
    seq_count = lax.axis_size("seq")
    key_f = key_input[0].astype(jnp.float32)
    value_f = value_input[0].astype(jnp.float32)
    out_f = grad_output[0].astype(jnp.float32)
    mixed = key_f * value_f
    gated = out_f * query_gate[0].astype(jnp.float32)
    tokens, channels = mixed.shape
    seq_length = tokens * seq_count
    full_length = 2 * seq_length
    inverse_scale = 1.0 / full_length
    filter_taps = filter_raw.astype(jnp.float32) * seq_length ** (-0.5)
    freq_one = jnp.arange(2 * seq_count, dtype=jnp.int32)
    block_index = jnp.arange(seq_count, dtype=jnp.int32)
    offset_index = jnp.arange(tokens, dtype=jnp.int32)
    cos_one, sin_one = angle_table(freq_one, block_index, 2 * seq_count)
    cos_inv, sin_inv = angle_table(block_index, freq_one, 2 * seq_count)
    cos_two, sin_two = angle_table(offset_index, offset_index, tokens)
    local_width = channels // seq_count
    arrived = (
        lax.all_to_all(mixed.T, "seq", split_axis=0, concat_axis=1, tiled=True),
        lax.all_to_all(gated.T, "seq", split_axis=0, concat_axis=1, tiled=True),
        lax.all_to_all(filter_taps.T, "seq", split_axis=0, concat_axis=1, tiled=True),
    )
    cos_tw, sin_tw = angle_table(freq_one, offset_index, full_length)
    spectra = []
    for line_data in arrived:
        lines = line_data.reshape(local_width, seq_count, tokens)
        real_part, imag_part = rotate("kn,cnm->ckm", cos_one, sin_one, -1.0, lines, None, True)
        real_part, imag_part = twist(cos_tw, sin_tw, -1.0, real_part, imag_part)
        spectra.append(rotate("jm,ckm->ckj", cos_two, sin_two, -1.0, real_part, imag_part, True))
    packed_real, packed_imag, corr_real, corr_imag = spectral_terms(
        spectra[0][0], spectra[0][1], spectra[1][0], spectra[1][1], spectra[2][0], spectra[2][1]
    )
    pr_mid, pi_mid = rotate("mj,ckj->ckm", cos_two, sin_two, 1.0, packed_real, packed_imag, True)
    pr_mid, pi_mid = twist(cos_tw, sin_tw, 1.0, pr_mid, pi_mid)
    cr_mid, ci_mid = rotate("mj,ckj->ckm", cos_two, sin_two, 1.0, corr_real, corr_imag, True)
    cr_mid, ci_mid = twist(cos_tw, sin_tw, 1.0, cr_mid, ci_mid)
    conv_lines, back_lines = rotate("nk,ckm->cnm", cos_inv, sin_inv, 1.0, pr_mid, pi_mid, True)
    corr_lines = rotate("nk,ckm->cnm", cos_inv, sin_inv, 1.0, cr_mid, ci_mid, False)[0]
    conv_lines = (conv_lines * inverse_scale).reshape(local_width, seq_length)
    back_lines = (back_lines * inverse_scale).reshape(local_width, seq_length)
    corr_lines = (corr_lines * inverse_scale).reshape(local_width, seq_length)
    returned = (
        lax.all_to_all(conv_lines, "seq", split_axis=1, concat_axis=0, tiled=True),
        lax.all_to_all(back_lines, "seq", split_axis=1, concat_axis=0, tiled=True),
        lax.all_to_all(corr_lines, "seq", split_axis=1, concat_axis=0, tiled=True),
    )
    conv_time = returned[0].T
    back_time = returned[1].T
    corr_time = returned[2].T
    conv_full = conv_time + skip_gain * mixed
    back_full = back_time + skip_gain * gated
    grad_query = (out_f * conv_full).astype(jnp.bfloat16)[None]
    grad_key = (back_full * value_f).astype(jnp.bfloat16)[None]
    grad_value = (back_full * key_f).astype(jnp.bfloat16)[None]
    grad_filter = lax.psum_scatter(
        corr_time * seq_length ** (-0.5), "ch", scatter_dimension=1, tiled=True
    )
    return (grad_query, grad_key, grad_value, grad_filter)


LANES = 128
VMEM_LIMIT = 60 * 1024 * 1024


def times_root(pair, turn, size):
    real, imag = pair
    turn %= size
    if turn == 0:
        return pair
    if 4 * turn == size:
        return (-imag, real)
    if 2 * turn == size:
        return (-real, -imag)
    if 4 * turn == 3 * size:
        return (imag, -real)
    cosine = math.cos(2.0 * math.pi * turn / size)
    sine = math.sin(2.0 * math.pi * turn / size)
    return (real * cosine - imag * sine, real * sine + imag * cosine)


def complex_dft(values, sense):
    size = len(values)
    if size == 1:
        return values
    even = complex_dft(values[0::2], sense)
    odd = complex_dft(values[1::2], sense)
    low, high = [], []
    for k in range(size // 2):
        er, ei = even[k]
        tr, ti = times_root(odd[k], sense * k, size)
        low.append((er + tr, ei + ti))
        high.append((er - tr, ei - ti))
    return low + high


def half_spectrum(values, size):
    if size == 2:
        return [(values[0] + values[1], None), (values[0] - values[1], None)]
    half, quarter = size // 2, size // 4
    if len(values) == half:
        total, difference = values, values
    else:
        total = [values[n] + values[n + half] for n in range(half)]
        difference = [values[n] - values[n + half] for n in range(half)]
    out = [None] * (half + 1)
    out[0::2] = half_spectrum(total, half)
    turned = [times_root((difference[n], -difference[n + quarter]), -n, size) for n in range(quarter)]
    for index, (real, imag) in enumerate(complex_dft(turned, -1)):
        k = 1 + 4 * index
        if k <= half:
            out[k] = (real, imag)
        else:
            out[size - k] = (real, -imag)
    return out


def real_from_half(terms, size, first_half):
    if size == 2:
        return [terms[0][0] + terms[1][0], terms[0][0] - terms[1][0]]
    half, quarter = size // 2, size // 4
    even = real_from_half(terms[0::2], half, False)
    chosen = []
    for index in range(quarter):
        k = 1 + 4 * index
        if k <= half:
            chosen.append(terms[k])
        else:
            real, imag = terms[size - k]
            chosen.append((real, -imag))
    turned = [times_root(pair, n, size) for n, pair in enumerate(complex_dft(chosen, 1))]
    odd = [pair[0] for pair in turned] + [-pair[1] for pair in turned]
    out = [even[n] + odd[n] for n in range(half)]
    if first_half:
        return out
    return out + [even[n] - odd[n] for n in range(half)]


def split_bf16(value):
    high = value.astype(jnp.bfloat16)
    return high, (value - high.astype(jnp.float32)).astype(jnp.bfloat16)


def three_dot(table_high, table_low, value):
    high, low = split_bf16(value)
    dot = lambda a, b: jnp.dot(a, b, preferred_element_type=jnp.float32)
    return dot(table_high, high) + (dot(table_high, low) + dot(table_low, high))


QUARTERS = 4
QUARTER = LANES // QUARTERS
PLAN = ((0, 1), (0, 2), (0, 3), (1, 1), (1, 2), (1, 3), (2, 1), (2, 2))
PLANES = 4
PLAN_STEP = 3
JOB_SLOTS = 3
LOCAL_SLOTS = 5
AT_ONCE = 2


def left_mask(shape):
    return lax.broadcasted_iota(jnp.int32, shape, 1) < LANES // 2


def even_mask(shape):
    return lax.broadcasted_iota(jnp.int32, shape, 1) & QUARTER == 0


def swap_halves(value):
    return pltpu.roll(value, LANES // 2, 1)


def turn_quarters(value, count):
    count %= QUARTERS
    return pltpu.roll(value, count * QUARTER, 1) if count else value


def choose_quarters(values):
    lane = lax.broadcasted_iota(jnp.int32, values[0].shape, 1)
    out = values[-1]
    for index in reversed(range(QUARTERS - 1)):
        out = jnp.where(lane < (index + 1) * QUARTER, values[index], out)
    return out


def transpose_quarters(values):
    turned = [turn_quarters(value, index) for index, value in enumerate(values)]
    mixed = [choose_quarters([turned[(u - a) % QUARTERS] for u in range(QUARTERS)]) for a in range(QUARTERS)]
    return [turn_quarters(value, -index) for index, value in enumerate(mixed)]


def interleave(one, two):
    even = even_mask(one.shape)
    return jnp.where(even, one, turn_quarters(two, 1)), jnp.where(even, turn_quarters(one, -1), two)


def offsets(count):
    return sorted(range(count), key=lambda step: abs(2 * step - count))


def repeat(first, count, at_once, body):
    def several(index, carry):
        for inner in range(at_once):
            body(first + index * at_once + inner)
        return carry

    lax.fori_loop(0, (count - first) // at_once, several, 0)


def greet_all(seq_count, ch_count, me_seq, me_ch):
    barrier = pltpu.get_barrier_semaphore()
    for step in offsets(seq_count):
        for turn in range(ch_count):
            if step or turn:
                partner = {"seq": lax.rem(me_seq + step, seq_count), "ch": lax.rem(me_ch + turn, ch_count)}
                pl.semaphore_signal(barrier, inc=1, device_id=partner, device_id_type=pl.DeviceIdType.MESH)
    return barrier


def layer_kernel(
    seq_count, ch_count,
    query_ref, key_ref, value_ref, out_ref, filter_ref, skip_ref, fwd_ref, inv_ref, tw_ref,
    gq_ref, gk_ref, gv_ref, gf_ref,
    send, send_half, taps_send, recv, recv_half, taps_recv,
    result, result_half, corr_result, back, back_half, corr, corr_far,
    lines, taps_lines, spec, taps_spec, corr_spec, tw_scr,
    send_sem, half_send_sem, taps_send_sem, local_taps_send_sem,
    recv_sem, half_recv_sem, taps_recv_sem,
    back_send_sem, back_half_send_sem, corr_send_sem,
    back_sem, back_half_sem, corr_sem, corr_far_sem,
):
    me_seq, me_ch = lax.axis_index("seq"), lax.axis_index("ch")
    tokens, channels = key_ref.shape
    half_tokens, part_tokens = tokens // 2, tokens // QUARTERS
    half_seq = seq_count // 2
    width = seq_count // PLANES
    plane, place = lax.div(me_seq, width), lax.rem(me_seq, width)
    high = lax.div(plane, PLANES // 2)
    low = 1 - high
    scale = (seq_count * tokens) ** -0.5
    side_channels = channels // ch_count
    jobs = QUARTERS * len(PLAN)
    far_groups = [group for group, (_, owner) in enumerate(PLAN) if owner >= PLANES // 2]
    far_jobs = QUARTERS * len(far_groups)
    own = [[group for group, (at, owner) in enumerate(PLAN) if owner == p] for p in range(PLANES)]
    own[0] = far_groups
    kept = [len(groups) for groups in own]
    barrier = greet_all(seq_count, ch_count, me_seq, me_ch)

    def start(source, target, seq, ch, send_at, recv_at):
        pltpu.make_async_remote_copy(
            src_ref=source, dst_ref=target, send_sem=send_at, recv_sem=recv_at,
            device_id={"seq": seq, "ch": ch}, device_id_type=pl.DeviceIdType.MESH,
        ).start()

    def span(ref, count, send_at, recv_at):
        return pltpu.make_async_remote_copy(
            src_ref=ref.at[pl.ds(0, count)], dst_ref=ref.at[pl.ds(0, count)], send_sem=send_at, recv_sem=recv_at,
            device_id={"seq": me_seq, "ch": me_ch}, device_id_type=pl.DeviceIdType.MESH,
        )

    def arrive(ref, count, sem):
        span(ref, count, sem, sem).wait_recv()

    def depart(ref, count, sem):
        if count:
            span(ref, count, sem, sem).wait_send()

    def prepare(group, side):
        lanes = pl.ds(pl.multiple_of(side * side_channels + group * LANES, LANES), LANES)
        base = side * jobs + QUARTERS * group

        for chunk in range(half_tokens // 16):
            pieces = []
            rows = [pl.ds(chunk * 16 + first, 16) for first in (0, half_tokens)]
            for one, two in ((key_ref, value_ref), (out_ref, query_ref)):
                for at in rows:
                    pieces.append(one[at, lanes].astype(jnp.float32) * two[at, lanes].astype(jnp.float32))
            for index, piece in enumerate(transpose_quarters(pieces)):
                send[base + index, rows[0], :] = piece

    def halve(group, side):
        far = group - 1 - lax.div(group, PLAN_STEP)
        for index in range(QUARTERS):
            piece = send[side * jobs + QUARTERS * group + index]
            top, bottom = piece[:part_tokens], piece[part_tokens:]
            send_half[side * far_jobs + QUARTERS * far + index] = jnp.where(left_mask(top.shape), top, swap_halves(bottom))

    def prepare_taps(group):
        lanes = pl.ds(pl.multiple_of(me_ch * side_channels + group * LANES, LANES), LANES)
        pieces = [filter_ref[part_tokens * k:part_tokens * (k + 1), lanes].astype(jnp.float32) * scale for k in range(QUARTERS)]
        for index, piece in enumerate(transpose_quarters(pieces)):
            taps_send[QUARTERS * group + index] = piece

    def turns():
        return [(step, turn) for step in offsets(width) for turn in reversed(range(ch_count))]

    def send_taps(group):
        slot = lax.div(group, PLAN_STEP)
        owner = 1 + lax.rem(group, PLAN_STEP)
        far = group - 1 - slot
        is_far = owner > 1
        for step in offsets(width):
            at = lax.rem(place + step, width)
            source = taps_send.at[QUARTERS * group + at]

            def to_owner():
                start(source, taps_recv.at[slot * seq_count + me_seq], owner * width + at, me_ch, taps_send_sem, taps_recv_sem.at[slot])

            def to_local():
                start(source, taps_recv.at[far * half_seq + me_seq], at, me_ch, local_taps_send_sem, taps_recv_sem.at[far])

            if step:
                to_owner()
                pl.when(is_far & (low == 1))(to_local)
            else:
                pl.when(plane != owner)(to_owner)

                @pl.when(plane == owner)
                def _():
                    taps_recv[slot * seq_count + me_seq] = taps_send[QUARTERS * group + place]

                pl.when(is_far & (low == 1) & (plane != 0))(to_local)

                @pl.when(is_far & (plane == 0))
                def _():
                    taps_recv[far * half_seq + me_seq] = taps_send[QUARTERS * group + place]

    def send_group(group):
        slot = lax.div(group, PLAN_STEP)
        owner = 1 + lax.rem(group, PLAN_STEP)
        far = group - 1 - slot

        @pl.when((owner > 1) & (low == 1))
        def _():
            for step, turn in turns():
                at, ch = lax.rem(place + step, width), lax.rem(me_ch + turn, ch_count)
                start(
                    send_half.at[ch * far_jobs + QUARTERS * far + at],
                    recv_half.at[slot * seq_count + me_ch * half_seq + me_seq],
                    owner * width + at, ch, half_send_sem, half_recv_sem.at[slot],
                )

        def whole(target_plane, target_slot, index):
            for step, turn in turns():
                at, ch = lax.rem(place + step, width), lax.rem(me_ch + turn, ch_count)

                def go():
                    start(send.at[ch * jobs + QUARTERS * group + at], recv.at[index], target_plane * width + at, ch, send_sem, recv_sem.at[target_slot])

                if step or turn:
                    go()
                else:
                    pl.when(plane != target_plane)(go)

                    @pl.when(plane == target_plane)
                    def _():
                        recv[index] = send[me_ch * jobs + QUARTERS * group + place]

        @pl.when((owner == 1) | (high == 1))
        def _():
            whole(owner, slot, (slot * ch_count + me_ch) * seq_count + me_seq)

        @pl.when((owner > 1) & (low == 1))
        def _():
            whole(0, far, (far * ch_count + me_ch) * half_seq + me_seq)

    def ready(group):
        other = lax.rem(me_ch + 1, ch_count)
        prepare_taps(group)
        prepare(group, other)
        prepare(group, me_ch)
        slot = lax.div(group, PLAN_STEP)

        @pl.when((group - PLAN_STEP * slot > 0) & (low == 1))
        def _():
            halve(group, 0)
            halve(group, 1)

    ready(0)
    pl.semaphore_wait(barrier, seq_count * ch_count - 1)

    def feed(group, carry):
        pl.when(group > 0)(lambda: ready(group))
        send_group(group)
        send_taps(group)
        return carry

    lax.fori_loop(0, len(PLAN), feed, 0)
    for k in range(seq_count + 1):
        for part in range(2):
            tw_scr[k, part] = jnp.broadcast_to(tw_ref[part, :, k:k + 1], (tokens, LANES))

    def analyse(source, target, blocks):
        def body(chunk, carry):
            rows = pl.ds(pl.multiple_of(chunk * 8, 8), 8)
            for k, (real, imag) in enumerate(half_spectrum([source[n, rows, :] for n in range(blocks)], 2 * blocks)):
                target[k, 0, rows, :] = real
                target[k, 1, rows, :] = jnp.zeros_like(real) if imag is None else imag
            return carry

        lax.fori_loop(0, tokens // 8, body, 0)

    def synthesise(source, target, blocks):
        def body(chunk, carry):
            rows = pl.ds(pl.multiple_of(chunk * 8, 8), 8)
            terms = [(source[k, 0, rows, :], source[k, 1, rows, :]) for k in range(blocks + 1)]
            for n, value in enumerate(real_from_half(terms, 2 * blocks, True)):
                target[n, rows, :] = value
            return carry

        lax.fori_loop(0, tokens // 8, body, 0)

    def across(table, real, imag):
        both = three_dot(table[0], table[1], jnp.concatenate([real, imag], axis=0))
        return both[:tokens], both[tokens:]

    def convolve(blocks):
        stride = seq_count // blocks
        analyse(lines, spec, blocks)
        analyse(taps_lines, taps_spec, blocks)
        forward = (fwd_ref[0], fwd_ref[1])
        inverse = (inv_ref[0], inv_ref[1])

        def middle(index, carry):
            ks = [index * AT_ONCE + inner for inner in range(AT_ONCE)]
            turns_at = [(tw_scr[stride * k, 0], tw_scr[stride * k, 1]) for k in ks]
            reals, imags = [], []
            for k, (cosine, sine) in zip(ks, turns_at):
                for held in (spec, taps_spec):
                    real, imag = held[k, 0], held[k, 1]
                    reals.append(real * cosine + imag * sine)
                    imags.append(imag * cosine - real * sine)
            real, imag = across(forward, jnp.concatenate(reals, axis=1), jnp.concatenate(imags, axis=1))
            reals, imags = [], []
            for inner in range(AT_ONCE):
                first = 2 * LANES * inner
                a_r, a_i = real[:, first:first + LANES], imag[:, first:first + LANES]
                h_r, h_i = real[:, first + LANES:first + 2 * LANES], imag[:, first + LANES:first + 2 * LANES]
                h_i = jnp.where(left_mask(h_i.shape), h_i, -h_i)
                g_r, g_i = swap_halves(a_r), swap_halves(a_i)
                reals += [a_r * h_r - a_i * h_i, a_r * g_r + a_i * g_i]
                imags += [a_r * h_i + a_i * h_r, a_r * g_i - a_i * g_r]
            real, imag = across(inverse, jnp.concatenate(reals, axis=1), jnp.concatenate(imags, axis=1))
            for inner, (k, (cosine, sine)) in enumerate(zip(ks, turns_at)):
                weight = jnp.where((k == 0) | (k == blocks), 0.5 / (blocks * tokens), 1.0 / (blocks * tokens))
                cosine, sine = cosine * weight, sine * weight
                for side, held in enumerate((spec, corr_spec)):
                    first = LANES * (2 * inner + side)
                    br, bi = real[:, first:first + LANES], imag[:, first:first + LANES]
                    held[k, 0] = br * cosine - bi * sine
                    held[k, 1] = bi * cosine + br * sine
            return carry

        lax.fori_loop(0, blocks // AT_ONCE + 1, middle, 0)
        synthesise(spec, lines, blocks)
        synthesise(corr_spec, taps_lines, blocks)

    def open_taps(slot, blocks):
        def body(n):
            packed = taps_recv[slot * blocks + n]
            turned = [turn_quarters(packed, count) for count in range(QUARTERS)]
            for k in range(QUARTERS):
                taps_lines[n, part_tokens * k:part_tokens * (k + 1), :] = choose_quarters([turned[(u - k) % QUARTERS] for u in range(QUARTERS)])

        repeat(0, blocks, 8, body)

    def open_whole(slot, blocks, first):
        def body(n):
            base = slot * ch_count * blocks + n
            top, bottom = interleave(recv[base], recv[base + blocks])
            lines[n, :half_tokens, :] = top
            lines[n, half_tokens:, :] = bottom

        repeat(first, blocks, 4, body)

    def open_half(slot):
        def body(n):
            one, two = recv_half[slot * seq_count + n], recv_half[slot * seq_count + half_seq + n]
            left = left_mask(one.shape)
            for first in (0, part_tokens):
                top, bottom = interleave(one, two)
                lines[n, first:first + part_tokens, :] = jnp.where(left, top, 0.0)
                lines[n, half_tokens + first:half_tokens + first + part_tokens, :] = jnp.where(left, bottom, 0.0)
                one, two = swap_halves(one), swap_halves(two)

        repeat(0, half_seq, 4, body)

    def close_whole(slot, blocks, first):
        def body(n):
            base = slot * ch_count * blocks + n
            one, two = interleave(lines[n, :half_tokens, :], lines[n, half_tokens:, :])
            result[base] = one
            result[base + blocks] = two

        repeat(first, blocks, 4, body)

    def close_half(slot):
        def body(n):
            for index, piece in enumerate(interleave(lines[n, :half_tokens, :], lines[n, half_tokens:, :])):
                top, bottom = piece[:part_tokens], piece[part_tokens:]
                result_half[slot * seq_count + index * half_seq + n] = jnp.where(left_mask(top.shape), swap_halves(bottom), top)

        repeat(0, half_seq, 4, body)

    def close_corr(slot, blocks):
        def body(n):
            pieces = []
            for k in range(QUARTERS):
                piece = taps_lines[n, part_tokens * k:part_tokens * (k + 1), :]
                pieces.append(turn_quarters((piece + turn_quarters(piece, -1)) * scale, k))
            corr_result[slot * blocks + n] = choose_quarters(pieces)

        repeat(0, blocks, 4, body)

    def deliver(slot, blocks, group, first, count):
        job = QUARTERS * group + place
        at_round = lax.div(group, PLAN_STEP)
        base = slot * ch_count * blocks
        for step in offsets(count):
            seq = first + lax.rem(me_seq + step, count)
            for turn in range(ch_count):
                ch = lax.rem(me_ch + turn, ch_count)
                if step or turn:
                    start(result.at[base + ch * blocks + seq], back.at[me_ch * jobs + job], seq, ch, back_send_sem, back_sem.at[at_round])
            if step:
                start(corr_result.at[slot * blocks + seq], corr.at[job], seq, me_ch, corr_send_sem, corr_sem.at[at_round])
        back[me_ch * jobs + job] = result[base + me_ch * blocks + me_seq]
        corr[job] = corr_result[slot * blocks + me_seq]

    def deliver_half(slot, group):
        far = QUARTERS * (group - 1 - slot) + place
        for step in offsets(half_seq):
            seq = lax.rem(me_seq + step, half_seq)
            for turn in range(ch_count):
                ch = lax.rem(me_ch + turn, ch_count)
                start(
                    result_half.at[slot * seq_count + ch * half_seq + seq], back_half.at[me_ch * far_jobs + far],
                    seq, ch, back_half_send_sem, back_half_sem.at[slot],
                )
            start(corr_result.at[slot * seq_count + seq], corr_far.at[far], seq, me_ch, corr_send_sem, corr_far_sem.at[slot])

    others = seq_count * ch_count - 1

    def owner_job(slot, carry):
        group = PLAN_STEP * slot + plane - 1
        arrive(taps_recv, seq_count - 1, taps_recv_sem.at[slot])
        open_taps(slot, seq_count)

        @pl.when(high == 0)
        def _():
            arrive(recv, others, recv_sem.at[slot])
            open_whole(slot, seq_count, 0)

        @pl.when(high == 1)
        def _():
            arrive(recv_half, seq_count, half_recv_sem.at[slot])
            open_half(slot)
            arrive(recv, seq_count - 1, recv_sem.at[slot])
            open_whole(slot, seq_count, half_seq)

        convolve(seq_count)
        close_corr(slot, seq_count)

        @pl.when(high == 0)
        def _():
            close_whole(slot, seq_count, 0)
            deliver(slot, seq_count, group, 0, seq_count)

        @pl.when(high == 1)
        def _():
            close_half(slot)
            close_whole(slot, seq_count, half_seq)
            deliver_half(slot, group)
            deliver(slot, seq_count, group, half_seq, half_seq)

        return carry

    def local_job(slot, carry):
        group = slot + 1 + lax.div(slot, 2)
        arrive(taps_recv, half_seq - 1, taps_recv_sem.at[slot])
        open_taps(slot, half_seq)
        arrive(recv, seq_count - 1, recv_sem.at[slot])
        open_whole(slot, half_seq, 0)
        convolve(half_seq)
        close_corr(slot, half_seq)
        close_whole(slot, half_seq, 0)
        deliver(slot, half_seq, group, 0, half_seq)
        return carry

    @pl.when(plane > 0)
    def _():
        lax.fori_loop(0, JOB_SLOTS - lax.div(plane, PLANES - 1), owner_job, 0)

    @pl.when(plane == 0)
    def _():
        lax.fori_loop(0, LOCAL_SLOTS, local_job, 0)

    def finish(group, side):
        lanes = pl.ds(pl.multiple_of(side * side_channels + group * LANES, LANES), LANES)
        base = side * jobs + QUARTERS * group
        skip = skip_ref[:, lanes]

        for chunk in range(half_tokens // 16):
            rows = [pl.ds(chunk * 16 + first, 16) for first in (0, half_tokens)]
            pieces = transpose_quarters([back[base + index, rows[0], :] for index in range(QUARTERS)])
            for at, conv, behind in zip(rows, pieces[:2], pieces[2:]):
                query_f = query_ref[at, lanes].astype(jnp.float32)
                key_f = key_ref[at, lanes].astype(jnp.float32)
                value_f = value_ref[at, lanes].astype(jnp.float32)
                out_f = out_ref[at, lanes].astype(jnp.float32)
                conv = conv + skip * (key_f * value_f)
                behind = behind + skip * (out_f * query_f)
                gq_ref[at, lanes] = (out_f * conv).astype(jnp.bfloat16)
                gk_ref[at, lanes] = (behind * value_f).astype(jnp.bfloat16)
                gv_ref[at, lanes] = (behind * key_f).astype(jnp.bfloat16)

    def finish_corr(group):
        lanes = pl.ds(pl.multiple_of(group * LANES, LANES), LANES)
        pieces = transpose_quarters([corr[QUARTERS * group + index] for index in range(QUARTERS)])
        for k, piece in enumerate(pieces):
            gf_ref[part_tokens * k:part_tokens * (k + 1), lanes] = piece

    def join_half(far, group):
        for side in range(ch_count):
            for index in range(QUARTERS):
                piece = back_half[side * far_jobs + QUARTERS * far + index]
                left = left_mask(piece.shape)
                place_at = side * jobs + QUARTERS * group + index
                back[place_at, :part_tokens, :] += jnp.where(left, 0.0, piece)
                back[place_at, part_tokens:, :] += jnp.where(left, 0.0, swap_halves(piece))
        for index in range(QUARTERS):
            corr[QUARTERS * group + index] += corr_far[QUARTERS * far + index]

    for at_round in range(JOB_SLOTS):
        groups = [group for group, (when, _) in enumerate(PLAN) if when == at_round]
        for p in range(PLANES):
            mine = sum(PLAN[group][0] == at_round for group in own[p])

            @pl.when(plane == p)
            def _():
                arrive(back, QUARTERS * ch_count * len(groups) - mine, back_sem.at[at_round])
                arrive(corr, QUARTERS * len(groups) - mine, corr_sem.at[at_round])

        @pl.when(low == 1)
        def _():
            count = QUARTERS * sum(group in far_groups for group in groups)
            arrive(back_half, count * ch_count, back_half_sem.at[at_round])
            arrive(corr_far, count, corr_far_sem.at[at_round])
            for group in groups:
                if group in far_groups:
                    join_half(far_groups.index(group), group)

        def finish_group(index, carry):
            group = groups[0] + index
            finish(group, 0)
            finish(group, 1)
            finish_corr(group)
            return carry

        lax.fori_loop(0, len(groups), finish_group, 0)

    for p in range(PLANES):
        is_low = p < PLANES // 2
        count = kept[p]

        @pl.when(plane == p)
        def _():
            depart(send, ch_count * jobs - count, send_sem)
            depart(send_half, ch_count * far_jobs if is_low else 0, half_send_sem)
            depart(taps_send, jobs - (count if p else 0), taps_send_sem)
            depart(taps_send, far_jobs - (0 if p else count) if is_low else 0, local_taps_send_sem)
            whole = (others if is_low else seq_count - 1) if p else seq_count - 1
            depart(result, count * whole, back_send_sem)
            depart(result_half, 0 if is_low else count * seq_count, back_half_send_sem)
            depart(corr_result, count * ((seq_count if p else half_seq) - 1), corr_send_sem)


def tables(seq_count, tokens):
    index = np.arange(tokens)
    angle = 2.0 * np.pi / tokens * (index[:, None] * index[None, :] % tokens)
    cosine, sine = np.cos(angle), np.sin(angle)
    forward = np.block([[cosine, sine], [-sine, cosine]]).astype(np.float32)
    inverse = np.block([[cosine, -sine], [sine, cosine]]).astype(np.float32)

    def pieces(table):
        table = jnp.asarray(table)
        return jnp.stack(split_bf16(table))

    turn = 2.0 * np.pi / (2 * seq_count * tokens) * (np.arange(seq_count + 1)[:, None] * index[None, :])
    twiddle = jnp.asarray(np.stack([np.cos(turn).T, np.sin(turn).T]).astype(np.float32))
    return pieces(forward), pieces(inverse), twiddle


def fast_shards(query_gate, key_input, value_input, grad_output, filter_raw, skip_gain):
    seq_count, ch_count = lax.axis_size("seq"), lax.axis_size("ch")
    _, tokens, channels = key_input.shape
    vmem = pl.BlockSpec(memory_space=pltpu.VMEM)
    jobs = QUARTERS * len(PLAN)
    far_jobs = QUARTERS * LOCAL_SLOTS
    whole = lambda count: pltpu.VMEM((count, tokens // 2, LANES), jnp.float32)
    part = lambda count: pltpu.VMEM((count, tokens // QUARTERS, LANES), jnp.float32)
    spectrum = pltpu.VMEM((seq_count + AT_ONCE, 2, tokens, LANES), jnp.float32)
    turning = pltpu.VMEM((seq_count + 2 * AT_ONCE, 2, tokens, LANES), jnp.float32)
    lines = pltpu.VMEM((seq_count, tokens, LANES), jnp.float32)
    slots = JOB_SLOTS * seq_count
    single = pltpu.SemaphoreType.DMA
    several = lambda count: pltpu.SemaphoreType.DMA((count,))
    grads = pl.pallas_call(
        lambda *refs: layer_kernel(seq_count, ch_count, *refs),
        in_specs=[vmem] * 9,
        out_specs=[vmem] * 4,
        out_shape=[jax.ShapeDtypeStruct((tokens, channels), jnp.bfloat16)] * 3
        + [jax.ShapeDtypeStruct((tokens, channels // ch_count), jnp.float32)],
        scratch_shapes=[
            whole(ch_count * jobs), part(ch_count * far_jobs), part(jobs), whole(ch_count * slots), part(slots), part(slots),
            whole(ch_count * slots), part(slots), part(slots), whole(ch_count * jobs), part(ch_count * far_jobs), part(jobs), part(far_jobs),
            lines, lines, spectrum, spectrum, spectrum, turning,
            single, single, single, single,
            several(LOCAL_SLOTS), several(JOB_SLOTS), several(LOCAL_SLOTS),
            single, single, single,
            several(JOB_SLOTS), several(JOB_SLOTS), several(JOB_SLOTS), several(JOB_SLOTS),
        ],
        compiler_params=pltpu.CompilerParams(vmem_limit_bytes=VMEM_LIMIT, collective_id=0, has_side_effects=True),
        name="layer",
    )(query_gate[0], key_input[0], value_input[0], grad_output[0], filter_raw, skip_gain[None], *tables(seq_count, tokens))
    return (grads[0][None], grads[1][None], grads[2][None], grads[3])


def solution(mesh):
    in_specs = (
        P("ch", "seq", None),
        P("ch", "seq", None),
        P("ch", "seq", None),
        P("ch", "seq", None),
        P("seq", None),
        P(),
    )
    out_specs = (P("ch", "seq", None), P("ch", "seq", None), P("ch", "seq", None), P("seq", "ch"))

    def body(*arrays):
        seq_count, ch_count = mesh.shape["seq"], mesh.shape["ch"]
        _, tokens, channels = arrays[0].shape
        fits = ch_count == 2 and tokens == LANES and seq_count == PLANES * QUARTERS and channels == ch_count * len(PLAN) * LANES
        return (fast_shards if fits else shards)(*arrays)

    return jax.shard_map(body, mesh=mesh, in_specs=in_specs, out_specs=out_specs, check_vma=False)
```

```python
import math

import numpy as np

import jax
import jax.numpy as jnp
from jax import lax
from jax.experimental import pallas as pl
from jax.experimental.pallas import tpu as pltpu
from jax.sharding import PartitionSpec as P


def angle_table(row_index, col_index, modulus):
    turn_count = row_index[:, None] * col_index[None, :] % modulus
    angles = turn_count.astype(jnp.float32) * (2.0 * math.pi / modulus)
    return (jnp.cos(angles), jnp.sin(angles))


def contract(pattern, table, operand):
    return jnp.einsum(
        pattern, table, operand, precision=lax.Precision.HIGHEST, preferred_element_type=jnp.float32
    )


def rotate(pattern, cos_table, sin_table, sense_sign, real_part, imag_part, want_imag):
    if imag_part is None:
        cos_term = contract(pattern, cos_table, real_part)
        return (cos_term, sense_sign * contract(pattern, sin_table, real_part))
    real_out = contract(pattern, cos_table, real_part) - sense_sign * contract(
        pattern, sin_table, imag_part
    )
    if not want_imag:
        return (real_out, None)
    imag_out = contract(pattern, cos_table, imag_part) + sense_sign * contract(
        pattern, sin_table, real_part
    )
    return (real_out, imag_out)


def twist(cos_table, sin_table, sense_sign, real_part, imag_part):
    return (
        real_part * cos_table - sense_sign * imag_part * sin_table,
        imag_part * cos_table + sense_sign * real_part * sin_table,
    )


def spectral_terms(z_real, z_imag, g_real, g_imag, h_real, h_imag):
    conv_real = z_real * h_real - z_imag * h_imag
    conv_imag = z_real * h_imag + z_imag * h_real
    back_real = h_real * g_real + h_imag * g_imag
    back_imag = h_real * g_imag - h_imag * g_real
    corr_real = z_real * g_real + z_imag * g_imag
    corr_imag = z_real * g_imag - z_imag * g_real
    return (conv_real - back_imag, conv_imag + back_real, corr_real, corr_imag)


def shards(query_gate, key_input, value_input, grad_output, filter_raw, skip_gain):
    seq_count = lax.axis_size("seq")
    key_f = key_input[0].astype(jnp.float32)
    value_f = value_input[0].astype(jnp.float32)
    out_f = grad_output[0].astype(jnp.float32)
    mixed = key_f * value_f
    gated = out_f * query_gate[0].astype(jnp.float32)
    tokens, channels = mixed.shape
    seq_length = tokens * seq_count
    full_length = 2 * seq_length
    inverse_scale = 1.0 / full_length
    filter_taps = filter_raw.astype(jnp.float32) * seq_length ** (-0.5)
    freq_one = jnp.arange(2 * seq_count, dtype=jnp.int32)
    block_index = jnp.arange(seq_count, dtype=jnp.int32)
    offset_index = jnp.arange(tokens, dtype=jnp.int32)
    cos_one, sin_one = angle_table(freq_one, block_index, 2 * seq_count)
    cos_inv, sin_inv = angle_table(block_index, freq_one, 2 * seq_count)
    cos_two, sin_two = angle_table(offset_index, offset_index, tokens)
    local_width = channels // seq_count
    arrived = (
        lax.all_to_all(mixed.T, "seq", split_axis=0, concat_axis=1, tiled=True),
        lax.all_to_all(gated.T, "seq", split_axis=0, concat_axis=1, tiled=True),
        lax.all_to_all(filter_taps.T, "seq", split_axis=0, concat_axis=1, tiled=True),
    )
    cos_tw, sin_tw = angle_table(freq_one, offset_index, full_length)
    spectra = []
    for line_data in arrived:
        lines = line_data.reshape(local_width, seq_count, tokens)
        real_part, imag_part = rotate("kn,cnm->ckm", cos_one, sin_one, -1.0, lines, None, True)
        real_part, imag_part = twist(cos_tw, sin_tw, -1.0, real_part, imag_part)
        spectra.append(rotate("jm,ckm->ckj", cos_two, sin_two, -1.0, real_part, imag_part, True))
    packed_real, packed_imag, corr_real, corr_imag = spectral_terms(
        spectra[0][0], spectra[0][1], spectra[1][0], spectra[1][1], spectra[2][0], spectra[2][1]
    )
    pr_mid, pi_mid = rotate("mj,ckj->ckm", cos_two, sin_two, 1.0, packed_real, packed_imag, True)
    pr_mid, pi_mid = twist(cos_tw, sin_tw, 1.0, pr_mid, pi_mid)
    cr_mid, ci_mid = rotate("mj,ckj->ckm", cos_two, sin_two, 1.0, corr_real, corr_imag, True)
    cr_mid, ci_mid = twist(cos_tw, sin_tw, 1.0, cr_mid, ci_mid)
    conv_lines, back_lines = rotate("nk,ckm->cnm", cos_inv, sin_inv, 1.0, pr_mid, pi_mid, True)
    corr_lines = rotate("nk,ckm->cnm", cos_inv, sin_inv, 1.0, cr_mid, ci_mid, False)[0]
    conv_lines = (conv_lines * inverse_scale).reshape(local_width, seq_length)
    back_lines = (back_lines * inverse_scale).reshape(local_width, seq_length)
    corr_lines = (corr_lines * inverse_scale).reshape(local_width, seq_length)
    returned = (
        lax.all_to_all(conv_lines, "seq", split_axis=1, concat_axis=0, tiled=True),
        lax.all_to_all(back_lines, "seq", split_axis=1, concat_axis=0, tiled=True),
        lax.all_to_all(corr_lines, "seq", split_axis=1, concat_axis=0, tiled=True),
    )
    conv_time = returned[0].T
    back_time = returned[1].T
    corr_time = returned[2].T
    conv_full = conv_time + skip_gain * mixed
    back_full = back_time + skip_gain * gated
    grad_query = (out_f * conv_full).astype(jnp.bfloat16)[None]
    grad_key = (back_full * value_f).astype(jnp.bfloat16)[None]
    grad_value = (back_full * key_f).astype(jnp.bfloat16)[None]
    grad_filter = lax.psum_scatter(
        corr_time * seq_length ** (-0.5), "ch", scatter_dimension=1, tiled=True
    )
    return (grad_query, grad_key, grad_value, grad_filter)


LANES = 128
VMEM_LIMIT = 60 * 1024 * 1024


def times_root(pair, turn, size):
    real, imag = pair
    turn %= size
    if turn == 0:
        return pair
    if 4 * turn == size:
        return (-imag, real)
    if 2 * turn == size:
        return (-real, -imag)
    if 4 * turn == 3 * size:
        return (imag, -real)
    cosine = math.cos(2.0 * math.pi * turn / size)
    sine = math.sin(2.0 * math.pi * turn / size)
    return (real * cosine - imag * sine, real * sine + imag * cosine)


def complex_dft(values, sense):
    size = len(values)
    if size == 1:
        return values
    even = complex_dft(values[0::2], sense)
    odd = complex_dft(values[1::2], sense)
    low, high = [], []
    for k in range(size // 2):
        er, ei = even[k]
        tr, ti = times_root(odd[k], sense * k, size)
        low.append((er + tr, ei + ti))
        high.append((er - tr, ei - ti))
    return low + high


def half_spectrum(values, size):
    if size == 2:
        return [(values[0] + values[1], None), (values[0] - values[1], None)]
    half, quarter = size // 2, size // 4
    if len(values) == half:
        total, difference = values, values
    else:
        total = [values[n] + values[n + half] for n in range(half)]
        difference = [values[n] - values[n + half] for n in range(half)]
    out = [None] * (half + 1)
    out[0::2] = half_spectrum(total, half)
    turned = [times_root((difference[n], -difference[n + quarter]), -n, size) for n in range(quarter)]
    for index, (real, imag) in enumerate(complex_dft(turned, -1)):
        k = 1 + 4 * index
        if k <= half:
            out[k] = (real, imag)
        else:
            out[size - k] = (real, -imag)
    return out


def real_from_half(terms, size, first_half):
    if size == 2:
        return [terms[0][0] + terms[1][0], terms[0][0] - terms[1][0]]
    half, quarter = size // 2, size // 4
    even = real_from_half(terms[0::2], half, False)
    chosen = []
    for index in range(quarter):
        k = 1 + 4 * index
        if k <= half:
            chosen.append(terms[k])
        else:
            real, imag = terms[size - k]
            chosen.append((real, -imag))
    turned = [times_root(pair, n, size) for n, pair in enumerate(complex_dft(chosen, 1))]
    odd = [pair[0] for pair in turned] + [-pair[1] for pair in turned]
    out = [even[n] + odd[n] for n in range(half)]
    if first_half:
        return out
    return out + [even[n] - odd[n] for n in range(half)]


def split_bf16(value):
    high = value.astype(jnp.bfloat16)
    return high, (value - high.astype(jnp.float32)).astype(jnp.bfloat16)


def three_dot(table_high, table_low, value):
    high, low = split_bf16(value)
    dot = lambda a, b: jnp.dot(a, b, preferred_element_type=jnp.float32)
    return dot(table_high, high) + (dot(table_high, low) + dot(table_low, high))


QUARTERS = 4
QUARTER = LANES // QUARTERS
PLAN = ((0, 1), (0, 2), (0, 3), (1, 1), (1, 2), (1, 3), (2, 1), (2, 2))
PLANES = 4
PLAN_STEP = 3
JOB_SLOTS = 3
LOCAL_SLOTS = 5
AT_ONCE = 2


def left_mask(shape):
    return lax.broadcasted_iota(jnp.int32, shape, 1) < LANES // 2


def even_mask(shape):
    return lax.broadcasted_iota(jnp.int32, shape, 1) & QUARTER == 0


def swap_halves(value):
    return pltpu.roll(value, LANES // 2, 1)


def turn_quarters(value, count):
    count %= QUARTERS
    return pltpu.roll(value, count * QUARTER, 1) if count else value


def choose_quarters(values):
    lane = lax.broadcasted_iota(jnp.int32, values[0].shape, 1)
    out = values[-1]
    for index in reversed(range(QUARTERS - 1)):
        out = jnp.where(lane < (index + 1) * QUARTER, values[index], out)
    return out


def transpose_quarters(values):
    turned = [turn_quarters(value, index) for index, value in enumerate(values)]
    mixed = [choose_quarters([turned[(u - a) % QUARTERS] for u in range(QUARTERS)]) for a in range(QUARTERS)]
    return [turn_quarters(value, -index) for index, value in enumerate(mixed)]


def interleave(one, two):
    even = even_mask(one.shape)
    return jnp.where(even, one, turn_quarters(two, 1)), jnp.where(even, turn_quarters(one, -1), two)


def offsets(count):
    return sorted(range(count), key=lambda step: abs(2 * step - count))


def repeat(first, count, at_once, body):
    def several(index, carry):
        for inner in range(at_once):
            body(first + index * at_once + inner)
        return carry

    lax.fori_loop(0, (count - first) // at_once, several, 0)


def greet_all(seq_count, ch_count, me_seq, me_ch):
    barrier = pltpu.get_barrier_semaphore()
    for step in offsets(seq_count):
        for turn in range(ch_count):
            if step or turn:
                partner = {"seq": lax.rem(me_seq + step, seq_count), "ch": lax.rem(me_ch + turn, ch_count)}
                pl.semaphore_signal(barrier, inc=1, device_id=partner, device_id_type=pl.DeviceIdType.MESH)
    return barrier


def layer_kernel(
    seq_count, ch_count,
    query_hbm, key_hbm, value_hbm, out_hbm, filter_hbm, skip_hbm, fwd_hbm, inv_hbm, tw_hbm,
    gq_ref, gk_ref, gv_ref, gf_ref,
    query_ref, key_ref, value_ref, out_ref, filter_ref, skip_ref, fwd_ref, inv_ref, tw_ref, load_sem,
    send, send_half, taps_send, recv, recv_half, taps_recv,
    result, result_half, corr_result, back, back_half, corr, corr_far,
    lines, taps_lines, spec, taps_spec, corr_spec, tw_scr,
    send_sem, half_send_sem, taps_send_sem, local_taps_send_sem,
    recv_sem, half_recv_sem, taps_recv_sem,
    back_send_sem, back_half_send_sem, corr_send_sem,
    back_sem, back_half_sem, corr_sem, corr_far_sem,
):
    me_seq, me_ch = lax.axis_index("seq"), lax.axis_index("ch")
    tokens, channels = key_ref.shape
    half_tokens, part_tokens = tokens // 2, tokens // QUARTERS
    half_seq = seq_count // 2
    width = seq_count // PLANES
    plane, place = lax.div(me_seq, width), lax.rem(me_seq, width)
    high = lax.div(plane, PLANES // 2)
    low = 1 - high
    scale = (seq_count * tokens) ** -0.5
    side_channels = channels // ch_count
    jobs = QUARTERS * len(PLAN)
    far_groups = [group for group, (_, owner) in enumerate(PLAN) if owner >= PLANES // 2]
    far_jobs = QUARTERS * len(far_groups)
    own = [[group for group, (at, owner) in enumerate(PLAN) if owner == p] for p in range(PLANES)]
    own[0] = far_groups
    kept = [len(groups) for groups in own]
    loads = [
        pltpu.make_async_copy(source, target, load_sem.at[index])
        for index, (source, target) in enumerate((
            (key_hbm, key_ref), (value_hbm, value_ref), (out_hbm, out_ref), (query_hbm, query_ref), (filter_hbm, filter_ref),
            (tw_hbm, tw_ref), (fwd_hbm, fwd_ref), (inv_hbm, inv_ref), (skip_hbm, skip_ref),
        ))
    ]
    for load in loads:
        load.start()
    barrier = greet_all(seq_count, ch_count, me_seq, me_ch)

    def start(source, target, seq, ch, send_at, recv_at):
        pltpu.make_async_remote_copy(
            src_ref=source, dst_ref=target, send_sem=send_at, recv_sem=recv_at,
            device_id={"seq": seq, "ch": ch}, device_id_type=pl.DeviceIdType.MESH,
        ).start()

    def span(ref, count, send_at, recv_at):
        return pltpu.make_async_remote_copy(
            src_ref=ref.at[pl.ds(0, count)], dst_ref=ref.at[pl.ds(0, count)], send_sem=send_at, recv_sem=recv_at,
            device_id={"seq": me_seq, "ch": me_ch}, device_id_type=pl.DeviceIdType.MESH,
        )

    def arrive(ref, count, sem):
        span(ref, count, sem, sem).wait_recv()

    def depart(ref, count, sem):
        if count:
            span(ref, count, sem, sem).wait_send()

    def prepare(group, side):
        lanes = pl.ds(pl.multiple_of(side * side_channels + group * LANES, LANES), LANES)
        base = side * jobs + QUARTERS * group

        for chunk in range(half_tokens // 16):
            pieces = []
            rows = [pl.ds(chunk * 16 + first, 16) for first in (0, half_tokens)]
            for one, two in ((key_ref, value_ref), (out_ref, query_ref)):
                for at in rows:
                    pieces.append(one[at, lanes].astype(jnp.float32) * two[at, lanes].astype(jnp.float32))
            for index, piece in enumerate(transpose_quarters(pieces)):
                send[base + index, rows[0], :] = piece

    def halve(group, side):
        far = group - 1 - lax.div(group, PLAN_STEP)
        for index in range(QUARTERS):
            piece = send[side * jobs + QUARTERS * group + index]
            top, bottom = piece[:part_tokens], piece[part_tokens:]
            send_half[side * far_jobs + QUARTERS * far + index] = jnp.where(left_mask(top.shape), top, swap_halves(bottom))

    def prepare_taps(group):
        lanes = pl.ds(pl.multiple_of(me_ch * side_channels + group * LANES, LANES), LANES)
        pieces = [filter_ref[part_tokens * k:part_tokens * (k + 1), lanes].astype(jnp.float32) * scale for k in range(QUARTERS)]
        for index, piece in enumerate(transpose_quarters(pieces)):
            taps_send[QUARTERS * group + index] = piece

    def turns():
        return [(step, turn) for step in offsets(width) for turn in reversed(range(ch_count))]

    def send_taps(group):
        slot = lax.div(group, PLAN_STEP)
        owner = 1 + lax.rem(group, PLAN_STEP)
        far = group - 1 - slot
        is_far = owner > 1
        for step in offsets(width):
            at = lax.rem(place + step, width)
            source = taps_send.at[QUARTERS * group + at]

            def to_owner():
                start(source, taps_recv.at[slot * seq_count + me_seq], owner * width + at, me_ch, taps_send_sem, taps_recv_sem.at[slot])

            def to_local():
                start(source, taps_recv.at[far * half_seq + me_seq], at, me_ch, local_taps_send_sem, taps_recv_sem.at[far])

            if step:
                to_owner()
                pl.when(is_far & (low == 1))(to_local)
            else:
                pl.when(plane != owner)(to_owner)

                @pl.when(plane == owner)
                def _():
                    taps_recv[slot * seq_count + me_seq] = taps_send[QUARTERS * group + place]

                pl.when(is_far & (low == 1) & (plane != 0))(to_local)

                @pl.when(is_far & (plane == 0))
                def _():
                    taps_recv[far * half_seq + me_seq] = taps_send[QUARTERS * group + place]

    def send_group(group):
        slot = lax.div(group, PLAN_STEP)
        owner = 1 + lax.rem(group, PLAN_STEP)
        far = group - 1 - slot

        @pl.when((owner > 1) & (low == 1))
        def _():
            for step, turn in turns():
                at, ch = lax.rem(place + step, width), lax.rem(me_ch + turn, ch_count)
                start(
                    send_half.at[ch * far_jobs + QUARTERS * far + at],
                    recv_half.at[slot * seq_count + me_ch * half_seq + me_seq],
                    owner * width + at, ch, half_send_sem, half_recv_sem.at[slot],
                )

        def whole(target_plane, target_slot, index):
            for step, turn in turns():
                at, ch = lax.rem(place + step, width), lax.rem(me_ch + turn, ch_count)

                def go():
                    start(send.at[ch * jobs + QUARTERS * group + at], recv.at[index], target_plane * width + at, ch, send_sem, recv_sem.at[target_slot])

                if step or turn:
                    go()
                else:
                    pl.when(plane != target_plane)(go)

                    @pl.when(plane == target_plane)
                    def _():
                        recv[index] = send[me_ch * jobs + QUARTERS * group + place]

        @pl.when((owner == 1) | (high == 1))
        def _():
            whole(owner, slot, (slot * ch_count + me_ch) * seq_count + me_seq)

        @pl.when((owner > 1) & (low == 1))
        def _():
            whole(0, far, (far * ch_count + me_ch) * half_seq + me_seq)

    def ready(group):
        other = lax.rem(me_ch + 1, ch_count)
        prepare_taps(group)
        prepare(group, other)
        prepare(group, me_ch)
        slot = lax.div(group, PLAN_STEP)

        @pl.when((group - PLAN_STEP * slot > 0) & (low == 1))
        def _():
            halve(group, 0)
            halve(group, 1)

    for load in loads[:5]:
        load.wait()
    ready(0)
    pl.semaphore_wait(barrier, seq_count * ch_count - 1)

    def feed(group, carry):
        pl.when(group > 0)(lambda: ready(group))
        send_group(group)
        send_taps(group)
        return carry

    lax.fori_loop(0, len(PLAN), feed, 0)
    for load in loads[5:]:
        load.wait()
    for k in range(seq_count + 1):
        for part in range(2):
            tw_scr[k, part] = jnp.broadcast_to(tw_ref[part, :, k:k + 1], (tokens, LANES))

    def analyse(source, target, blocks):
        def body(chunk, carry):
            rows = pl.ds(pl.multiple_of(chunk * 8, 8), 8)
            for k, (real, imag) in enumerate(half_spectrum([source[n, rows, :] for n in range(blocks)], 2 * blocks)):
                target[k, 0, rows, :] = real
                target[k, 1, rows, :] = jnp.zeros_like(real) if imag is None else imag
            return carry

        lax.fori_loop(0, tokens // 8, body, 0)

    def synthesise(source, target, blocks):
        def body(chunk, carry):
            rows = pl.ds(pl.multiple_of(chunk * 8, 8), 8)
            terms = [(source[k, 0, rows, :], source[k, 1, rows, :]) for k in range(blocks + 1)]
            for n, value in enumerate(real_from_half(terms, 2 * blocks, True)):
                target[n, rows, :] = value
            return carry

        lax.fori_loop(0, tokens // 8, body, 0)

    def across(table, real, imag):
        both = three_dot(table[0], table[1], jnp.concatenate([real, imag], axis=0))
        return both[:tokens], both[tokens:]

    def convolve(blocks):
        stride = seq_count // blocks
        analyse(lines, spec, blocks)
        analyse(taps_lines, taps_spec, blocks)
        forward = (fwd_ref[0], fwd_ref[1])
        inverse = (inv_ref[0], inv_ref[1])

        def middle(index, carry):
            ks = [index * AT_ONCE + inner for inner in range(AT_ONCE)]
            turns_at = [(tw_scr[stride * k, 0], tw_scr[stride * k, 1]) for k in ks]
            reals, imags = [], []
            for k, (cosine, sine) in zip(ks, turns_at):
                for held in (spec, taps_spec):
                    real, imag = held[k, 0], held[k, 1]
                    reals.append(real * cosine + imag * sine)
                    imags.append(imag * cosine - real * sine)
            real, imag = across(forward, jnp.concatenate(reals, axis=1), jnp.concatenate(imags, axis=1))
            reals, imags = [], []
            for inner in range(AT_ONCE):
                first = 2 * LANES * inner
                a_r, a_i = real[:, first:first + LANES], imag[:, first:first + LANES]
                h_r, h_i = real[:, first + LANES:first + 2 * LANES], imag[:, first + LANES:first + 2 * LANES]
                h_i = jnp.where(left_mask(h_i.shape), h_i, -h_i)
                g_r, g_i = swap_halves(a_r), swap_halves(a_i)
                reals += [a_r * h_r - a_i * h_i, a_r * g_r + a_i * g_i]
                imags += [a_r * h_i + a_i * h_r, a_r * g_i - a_i * g_r]
            real, imag = across(inverse, jnp.concatenate(reals, axis=1), jnp.concatenate(imags, axis=1))
            for inner, (k, (cosine, sine)) in enumerate(zip(ks, turns_at)):
                weight = jnp.where((k == 0) | (k == blocks), 0.5 / (blocks * tokens), 1.0 / (blocks * tokens))
                cosine, sine = cosine * weight, sine * weight
                for side, held in enumerate((spec, corr_spec)):
                    first = LANES * (2 * inner + side)
                    br, bi = real[:, first:first + LANES], imag[:, first:first + LANES]
                    held[k, 0] = br * cosine - bi * sine
                    held[k, 1] = bi * cosine + br * sine
            return carry

        lax.fori_loop(0, blocks // AT_ONCE + 1, middle, 0)
        synthesise(spec, lines, blocks)
        synthesise(corr_spec, taps_lines, blocks)

    def open_taps(slot, blocks):
        def body(n):
            packed = taps_recv[slot * blocks + n]
            turned = [turn_quarters(packed, count) for count in range(QUARTERS)]
            for k in range(QUARTERS):
                taps_lines[n, part_tokens * k:part_tokens * (k + 1), :] = choose_quarters([turned[(u - k) % QUARTERS] for u in range(QUARTERS)])

        repeat(0, blocks, 8, body)

    def open_whole(slot, blocks, first):
        def body(n):
            base = slot * ch_count * blocks + n
            top, bottom = interleave(recv[base], recv[base + blocks])
            lines[n, :half_tokens, :] = top
            lines[n, half_tokens:, :] = bottom

        repeat(first, blocks, 4, body)

    def open_half(slot):
        def body(n):
            one, two = recv_half[slot * seq_count + n], recv_half[slot * seq_count + half_seq + n]
            left = left_mask(one.shape)
            for first in (0, part_tokens):
                top, bottom = interleave(one, two)
                lines[n, first:first + part_tokens, :] = jnp.where(left, top, 0.0)
                lines[n, half_tokens + first:half_tokens + first + part_tokens, :] = jnp.where(left, bottom, 0.0)
                one, two = swap_halves(one), swap_halves(two)

        repeat(0, half_seq, 4, body)

    def close_whole(slot, blocks, first):
        def body(n):
            base = slot * ch_count * blocks + n
            one, two = interleave(lines[n, :half_tokens, :], lines[n, half_tokens:, :])
            result[base] = one
            result[base + blocks] = two

        repeat(first, blocks, 4, body)

    def close_half(slot):
        def body(n):
            for index, piece in enumerate(interleave(lines[n, :half_tokens, :], lines[n, half_tokens:, :])):
                top, bottom = piece[:part_tokens], piece[part_tokens:]
                result_half[slot * seq_count + index * half_seq + n] = jnp.where(left_mask(top.shape), swap_halves(bottom), top)

        repeat(0, half_seq, 4, body)

    def close_corr(slot, blocks):
        def body(n):
            pieces = []
            for k in range(QUARTERS):
                piece = taps_lines[n, part_tokens * k:part_tokens * (k + 1), :]
                pieces.append(turn_quarters((piece + turn_quarters(piece, -1)) * scale, k))
            corr_result[slot * blocks + n] = choose_quarters(pieces)

        repeat(0, blocks, 4, body)

    def deliver(slot, blocks, group, first, count):
        job = QUARTERS * group + place
        at_round = lax.div(group, PLAN_STEP)
        base = slot * ch_count * blocks
        for step in offsets(count):
            seq = first + lax.rem(me_seq + step, count)
            for turn in range(ch_count):
                ch = lax.rem(me_ch + turn, ch_count)
                if step or turn:
                    start(result.at[base + ch * blocks + seq], back.at[me_ch * jobs + job], seq, ch, back_send_sem, back_sem.at[at_round])
            if step:
                start(corr_result.at[slot * blocks + seq], corr.at[job], seq, me_ch, corr_send_sem, corr_sem.at[at_round])
        back[me_ch * jobs + job] = result[base + me_ch * blocks + me_seq]
        corr[job] = corr_result[slot * blocks + me_seq]

    def deliver_half(slot, group):
        far = QUARTERS * (group - 1 - slot) + place
        for step in offsets(half_seq):
            seq = lax.rem(me_seq + step, half_seq)
            for turn in range(ch_count):
                ch = lax.rem(me_ch + turn, ch_count)
                start(
                    result_half.at[slot * seq_count + ch * half_seq + seq], back_half.at[me_ch * far_jobs + far],
                    seq, ch, back_half_send_sem, back_half_sem.at[slot],
                )
            start(corr_result.at[slot * seq_count + seq], corr_far.at[far], seq, me_ch, corr_send_sem, corr_far_sem.at[slot])

    others = seq_count * ch_count - 1

    def owner_job(slot, carry):
        group = PLAN_STEP * slot + plane - 1
        arrive(taps_recv, seq_count - 1, taps_recv_sem.at[slot])
        open_taps(slot, seq_count)

        @pl.when(high == 0)
        def _():
            arrive(recv, others, recv_sem.at[slot])
            open_whole(slot, seq_count, 0)

        @pl.when(high == 1)
        def _():
            arrive(recv_half, seq_count, half_recv_sem.at[slot])
            open_half(slot)
            arrive(recv, seq_count - 1, recv_sem.at[slot])
            open_whole(slot, seq_count, half_seq)

        convolve(seq_count)
        close_corr(slot, seq_count)

        @pl.when(high == 0)
        def _():
            close_whole(slot, seq_count, 0)
            deliver(slot, seq_count, group, 0, seq_count)

        @pl.when(high == 1)
        def _():
            close_half(slot)
            close_whole(slot, seq_count, half_seq)
            deliver_half(slot, group)
            deliver(slot, seq_count, group, half_seq, half_seq)

        return carry

    def local_job(slot, carry):
        group = slot + 1 + lax.div(slot, 2)
        arrive(taps_recv, half_seq - 1, taps_recv_sem.at[slot])
        open_taps(slot, half_seq)
        arrive(recv, seq_count - 1, recv_sem.at[slot])
        open_whole(slot, half_seq, 0)
        convolve(half_seq)
        close_corr(slot, half_seq)
        close_whole(slot, half_seq, 0)
        deliver(slot, half_seq, group, 0, half_seq)
        return carry

    @pl.when(plane > 0)
    def _():
        lax.fori_loop(0, JOB_SLOTS - lax.div(plane, PLANES - 1), owner_job, 0)

    @pl.when(plane == 0)
    def _():
        lax.fori_loop(0, LOCAL_SLOTS, local_job, 0)

    def finish(group, side):
        lanes = pl.ds(pl.multiple_of(side * side_channels + group * LANES, LANES), LANES)
        base = side * jobs + QUARTERS * group
        skip = skip_ref[:, lanes]

        for chunk in range(half_tokens // 16):
            rows = [pl.ds(chunk * 16 + first, 16) for first in (0, half_tokens)]
            pieces = transpose_quarters([back[base + index, rows[0], :] for index in range(QUARTERS)])
            for at, conv, behind in zip(rows, pieces[:2], pieces[2:]):
                query_f = query_ref[at, lanes].astype(jnp.float32)
                key_f = key_ref[at, lanes].astype(jnp.float32)
                value_f = value_ref[at, lanes].astype(jnp.float32)
                out_f = out_ref[at, lanes].astype(jnp.float32)
                conv = conv + skip * (key_f * value_f)
                behind = behind + skip * (out_f * query_f)
                gq_ref[at, lanes] = (out_f * conv).astype(jnp.bfloat16)
                gk_ref[at, lanes] = (behind * value_f).astype(jnp.bfloat16)
                gv_ref[at, lanes] = (behind * key_f).astype(jnp.bfloat16)

    def finish_corr(group):
        lanes = pl.ds(pl.multiple_of(group * LANES, LANES), LANES)
        pieces = transpose_quarters([corr[QUARTERS * group + index] for index in range(QUARTERS)])
        for k, piece in enumerate(pieces):
            gf_ref[part_tokens * k:part_tokens * (k + 1), lanes] = piece

    def join_half(far, group):
        for side in range(ch_count):
            for index in range(QUARTERS):
                piece = back_half[side * far_jobs + QUARTERS * far + index]
                left = left_mask(piece.shape)
                place_at = side * jobs + QUARTERS * group + index
                back[place_at, :part_tokens, :] += jnp.where(left, 0.0, piece)
                back[place_at, part_tokens:, :] += jnp.where(left, 0.0, swap_halves(piece))
        for index in range(QUARTERS):
            corr[QUARTERS * group + index] += corr_far[QUARTERS * far + index]

    for at_round in range(JOB_SLOTS):
        groups = [group for group, (when, _) in enumerate(PLAN) if when == at_round]
        for p in range(PLANES):
            mine = sum(PLAN[group][0] == at_round for group in own[p])

            @pl.when(plane == p)
            def _():
                arrive(back, QUARTERS * ch_count * len(groups) - mine, back_sem.at[at_round])
                arrive(corr, QUARTERS * len(groups) - mine, corr_sem.at[at_round])

        @pl.when(low == 1)
        def _():
            count = QUARTERS * sum(group in far_groups for group in groups)
            arrive(back_half, count * ch_count, back_half_sem.at[at_round])
            arrive(corr_far, count, corr_far_sem.at[at_round])
            for group in groups:
                if group in far_groups:
                    join_half(far_groups.index(group), group)

        def finish_group(index, carry):
            group = groups[0] + index
            finish(group, 0)
            finish(group, 1)
            finish_corr(group)
            return carry

        lax.fori_loop(0, len(groups), finish_group, 0)

    for p in range(PLANES):
        is_low = p < PLANES // 2
        count = kept[p]

        @pl.when(plane == p)
        def _():
            depart(send, ch_count * jobs - count, send_sem)
            depart(send_half, ch_count * far_jobs if is_low else 0, half_send_sem)
            depart(taps_send, jobs - (count if p else 0), taps_send_sem)
            depart(taps_send, far_jobs - (0 if p else count) if is_low else 0, local_taps_send_sem)
            whole = (others if is_low else seq_count - 1) if p else seq_count - 1
            depart(result, count * whole, back_send_sem)
            depart(result_half, 0 if is_low else count * seq_count, back_half_send_sem)
            depart(corr_result, count * ((seq_count if p else half_seq) - 1), corr_send_sem)


def tables(seq_count, tokens):
    index = np.arange(tokens)
    angle = 2.0 * np.pi / tokens * (index[:, None] * index[None, :] % tokens)
    cosine, sine = np.cos(angle), np.sin(angle)
    forward = np.block([[cosine, sine], [-sine, cosine]]).astype(np.float32)
    inverse = np.block([[cosine, -sine], [sine, cosine]]).astype(np.float32)

    def pieces(table):
        table = jnp.asarray(table)
        return jnp.stack(split_bf16(table))

    turn = 2.0 * np.pi / (2 * seq_count * tokens) * (np.arange(seq_count + 1)[:, None] * index[None, :])
    twiddle = jnp.asarray(np.stack([np.cos(turn).T, np.sin(turn).T]).astype(np.float32))
    return pieces(forward), pieces(inverse), twiddle


def hand_out(*refs):
    count = len(refs) // 2
    copies = [pltpu.make_async_copy(refs[i], refs[count + i], refs[-1].at[i]) for i in range(count)]
    for copy in copies:
        copy.start()
    for copy in copies:
        copy.wait()


def fast_shards(query_gate, key_input, value_input, grad_output, filter_raw, skip_gain):
    seq_count, ch_count = lax.axis_size("seq"), lax.axis_size("ch")
    _, tokens, channels = key_input.shape
    vmem = pl.BlockSpec(memory_space=pltpu.VMEM)
    jobs = QUARTERS * len(PLAN)
    far_jobs = QUARTERS * LOCAL_SLOTS
    whole = lambda count: pltpu.VMEM((count, tokens // 2, LANES), jnp.float32)
    part = lambda count: pltpu.VMEM((count, tokens // QUARTERS, LANES), jnp.float32)
    spectrum = pltpu.VMEM((seq_count + AT_ONCE, 2, tokens, LANES), jnp.float32)
    turning = pltpu.VMEM((seq_count + 2 * AT_ONCE, 2, tokens, LANES), jnp.float32)
    lines = pltpu.VMEM((seq_count, tokens, LANES), jnp.float32)
    slots = JOB_SLOTS * seq_count
    single = pltpu.SemaphoreType.DMA
    several = lambda count: pltpu.SemaphoreType.DMA((count,))
    inputs = (query_gate[0], key_input[0], value_input[0], grad_output[0], filter_raw, skip_gain[None], *tables(seq_count, tokens))
    grads = pl.pallas_call(
        lambda *refs: layer_kernel(seq_count, ch_count, *refs),
        in_specs=[pl.BlockSpec(memory_space=pltpu.HBM)] * len(inputs),
        out_specs=[vmem] * 4,
        out_shape=[pltpu.VMEM((tokens, channels), jnp.bfloat16)] * 3 + [pltpu.VMEM((tokens, channels // ch_count), jnp.float32)],
        scratch_shapes=[pltpu.VMEM(array.shape, array.dtype) for array in inputs] + [several(len(inputs))] + [
            whole(ch_count * jobs), part(ch_count * far_jobs), part(jobs), whole(ch_count * slots), part(slots), part(slots),
            whole(ch_count * slots), part(slots), part(slots), whole(ch_count * jobs), part(ch_count * far_jobs), part(jobs), part(far_jobs),
            lines, lines, spectrum, spectrum, spectrum, turning,
            single, single, single, single,
            several(LOCAL_SLOTS), several(JOB_SLOTS), several(LOCAL_SLOTS),
            single, single, single,
            several(JOB_SLOTS), several(JOB_SLOTS), several(JOB_SLOTS), several(JOB_SLOTS),
        ],
        compiler_params=pltpu.CompilerParams(vmem_limit_bytes=VMEM_LIMIT, collective_id=0, has_side_effects=True),
        name="layer",
    )(*inputs)
    grads = pl.pallas_call(
        hand_out,
        in_specs=[vmem] * len(grads),
        out_specs=[pl.BlockSpec(memory_space=pltpu.HBM)] * len(grads),
        out_shape=[jax.ShapeDtypeStruct(array.shape, array.dtype) for array in grads],
        scratch_shapes=[several(len(grads))],
        compiler_params=pltpu.CompilerParams(vmem_limit_bytes=1024 * 1024),
        name="hand_out",
    )(*grads)
    return (grads[0][None], grads[1][None], grads[2][None], grads[3])


def solution(mesh):
    in_specs = (
        P("ch", "seq", None),
        P("ch", "seq", None),
        P("ch", "seq", None),
        P("ch", "seq", None),
        P("seq", None),
        P(),
    )
    out_specs = (P("ch", "seq", None), P("ch", "seq", None), P("ch", "seq", None), P("seq", "ch"))

    def body(*arrays):
        seq_count, ch_count = mesh.shape["seq"], mesh.shape["ch"]
        _, tokens, channels = arrays[0].shape
        fits = ch_count == 2 and tokens == LANES and seq_count == PLANES * QUARTERS and channels == ch_count * len(PLAN) * LANES
        return (fast_shards if fits else shards)(*arrays)

    return jax.shard_map(body, mesh=mesh, in_specs=in_specs, out_specs=out_specs, check_vma=False)
```

```python
import math

import numpy as np

import jax
import jax.numpy as jnp
from jax import lax
from jax.experimental import pallas as pl
from jax.experimental.pallas import tpu as pltpu
from jax.sharding import PartitionSpec as P


def angle_table(row_index, col_index, modulus):
    turn_count = row_index[:, None] * col_index[None, :] % modulus
    angles = turn_count.astype(jnp.float32) * (2.0 * math.pi / modulus)
    return (jnp.cos(angles), jnp.sin(angles))


def contract(pattern, table, operand):
    return jnp.einsum(
        pattern, table, operand, precision=lax.Precision.HIGHEST, preferred_element_type=jnp.float32
    )


def rotate(pattern, cos_table, sin_table, sense_sign, real_part, imag_part, want_imag):
    if imag_part is None:
        cos_term = contract(pattern, cos_table, real_part)
        return (cos_term, sense_sign * contract(pattern, sin_table, real_part))
    real_out = contract(pattern, cos_table, real_part) - sense_sign * contract(
        pattern, sin_table, imag_part
    )
    if not want_imag:
        return (real_out, None)
    imag_out = contract(pattern, cos_table, imag_part) + sense_sign * contract(
        pattern, sin_table, real_part
    )
    return (real_out, imag_out)


def twist(cos_table, sin_table, sense_sign, real_part, imag_part):
    return (
        real_part * cos_table - sense_sign * imag_part * sin_table,
        imag_part * cos_table + sense_sign * real_part * sin_table,
    )


def spectral_terms(z_real, z_imag, g_real, g_imag, h_real, h_imag):
    conv_real = z_real * h_real - z_imag * h_imag
    conv_imag = z_real * h_imag + z_imag * h_real
    back_real = h_real * g_real + h_imag * g_imag
    back_imag = h_real * g_imag - h_imag * g_real
    corr_real = z_real * g_real + z_imag * g_imag
    corr_imag = z_real * g_imag - z_imag * g_real
    return (conv_real - back_imag, conv_imag + back_real, corr_real, corr_imag)


def shards(query_gate, key_input, value_input, grad_output, filter_raw, skip_gain):
    seq_count = lax.axis_size("seq")
    key_f = key_input[0].astype(jnp.float32)
    value_f = value_input[0].astype(jnp.float32)
    out_f = grad_output[0].astype(jnp.float32)
    mixed = key_f * value_f
    gated = out_f * query_gate[0].astype(jnp.float32)
    tokens, channels = mixed.shape
    seq_length = tokens * seq_count
    full_length = 2 * seq_length
    inverse_scale = 1.0 / full_length
    filter_taps = filter_raw.astype(jnp.float32) * seq_length ** (-0.5)
    freq_one = jnp.arange(2 * seq_count, dtype=jnp.int32)
    block_index = jnp.arange(seq_count, dtype=jnp.int32)
    offset_index = jnp.arange(tokens, dtype=jnp.int32)
    cos_one, sin_one = angle_table(freq_one, block_index, 2 * seq_count)
    cos_inv, sin_inv = angle_table(block_index, freq_one, 2 * seq_count)
    cos_two, sin_two = angle_table(offset_index, offset_index, tokens)
    local_width = channels // seq_count
    arrived = (
        lax.all_to_all(mixed.T, "seq", split_axis=0, concat_axis=1, tiled=True),
        lax.all_to_all(gated.T, "seq", split_axis=0, concat_axis=1, tiled=True),
        lax.all_to_all(filter_taps.T, "seq", split_axis=0, concat_axis=1, tiled=True),
    )
    cos_tw, sin_tw = angle_table(freq_one, offset_index, full_length)
    spectra = []
    for line_data in arrived:
        lines = line_data.reshape(local_width, seq_count, tokens)
        real_part, imag_part = rotate("kn,cnm->ckm", cos_one, sin_one, -1.0, lines, None, True)
        real_part, imag_part = twist(cos_tw, sin_tw, -1.0, real_part, imag_part)
        spectra.append(rotate("jm,ckm->ckj", cos_two, sin_two, -1.0, real_part, imag_part, True))
    packed_real, packed_imag, corr_real, corr_imag = spectral_terms(
        spectra[0][0], spectra[0][1], spectra[1][0], spectra[1][1], spectra[2][0], spectra[2][1]
    )
    pr_mid, pi_mid = rotate("mj,ckj->ckm", cos_two, sin_two, 1.0, packed_real, packed_imag, True)
    pr_mid, pi_mid = twist(cos_tw, sin_tw, 1.0, pr_mid, pi_mid)
    cr_mid, ci_mid = rotate("mj,ckj->ckm", cos_two, sin_two, 1.0, corr_real, corr_imag, True)
    cr_mid, ci_mid = twist(cos_tw, sin_tw, 1.0, cr_mid, ci_mid)
    conv_lines, back_lines = rotate("nk,ckm->cnm", cos_inv, sin_inv, 1.0, pr_mid, pi_mid, True)
    corr_lines = rotate("nk,ckm->cnm", cos_inv, sin_inv, 1.0, cr_mid, ci_mid, False)[0]
    conv_lines = (conv_lines * inverse_scale).reshape(local_width, seq_length)
    back_lines = (back_lines * inverse_scale).reshape(local_width, seq_length)
    corr_lines = (corr_lines * inverse_scale).reshape(local_width, seq_length)
    returned = (
        lax.all_to_all(conv_lines, "seq", split_axis=1, concat_axis=0, tiled=True),
        lax.all_to_all(back_lines, "seq", split_axis=1, concat_axis=0, tiled=True),
        lax.all_to_all(corr_lines, "seq", split_axis=1, concat_axis=0, tiled=True),
    )
    conv_time = returned[0].T
    back_time = returned[1].T
    corr_time = returned[2].T
    conv_full = conv_time + skip_gain * mixed
    back_full = back_time + skip_gain * gated
    grad_query = (out_f * conv_full).astype(jnp.bfloat16)[None]
    grad_key = (back_full * value_f).astype(jnp.bfloat16)[None]
    grad_value = (back_full * key_f).astype(jnp.bfloat16)[None]
    grad_filter = lax.psum_scatter(
        corr_time * seq_length ** (-0.5), "ch", scatter_dimension=1, tiled=True
    )
    return (grad_query, grad_key, grad_value, grad_filter)


LANES = 128
VMEM_LIMIT = 60 * 1024 * 1024


def times_root(pair, turn, size):
    real, imag = pair
    turn %= size
    if turn == 0:
        return pair
    if 4 * turn == size:
        return (-imag, real)
    if 2 * turn == size:
        return (-real, -imag)
    if 4 * turn == 3 * size:
        return (imag, -real)
    cosine = math.cos(2.0 * math.pi * turn / size)
    sine = math.sin(2.0 * math.pi * turn / size)
    return (real * cosine - imag * sine, real * sine + imag * cosine)


def complex_dft(values, sense):
    size = len(values)
    if size == 1:
        return values
    even = complex_dft(values[0::2], sense)
    odd = complex_dft(values[1::2], sense)
    low, high = [], []
    for k in range(size // 2):
        er, ei = even[k]
        tr, ti = times_root(odd[k], sense * k, size)
        low.append((er + tr, ei + ti))
        high.append((er - tr, ei - ti))
    return low + high


def half_spectrum(values, size):
    if size == 2:
        return [(values[0] + values[1], None), (values[0] - values[1], None)]
    half, quarter = size // 2, size // 4
    if len(values) == half:
        total, difference = values, values
    else:
        total = [values[n] + values[n + half] for n in range(half)]
        difference = [values[n] - values[n + half] for n in range(half)]
    out = [None] * (half + 1)
    out[0::2] = half_spectrum(total, half)
    turned = [times_root((difference[n], -difference[n + quarter]), -n, size) for n in range(quarter)]
    for index, (real, imag) in enumerate(complex_dft(turned, -1)):
        k = 1 + 4 * index
        if k <= half:
            out[k] = (real, imag)
        else:
            out[size - k] = (real, -imag)
    return out


def real_from_half(terms, size, first_half):
    if size == 2:
        return [terms[0][0] + terms[1][0], terms[0][0] - terms[1][0]]
    half, quarter = size // 2, size // 4
    even = real_from_half(terms[0::2], half, False)
    chosen = []
    for index in range(quarter):
        k = 1 + 4 * index
        if k <= half:
            chosen.append(terms[k])
        else:
            real, imag = terms[size - k]
            chosen.append((real, -imag))
    turned = [times_root(pair, n, size) for n, pair in enumerate(complex_dft(chosen, 1))]
    odd = [pair[0] for pair in turned] + [-pair[1] for pair in turned]
    out = [even[n] + odd[n] for n in range(half)]
    if first_half:
        return out
    return out + [even[n] - odd[n] for n in range(half)]


def split_bf16(value):
    high = value.astype(jnp.bfloat16)
    return high, (value - high.astype(jnp.float32)).astype(jnp.bfloat16)


def three_dot(table_high, table_low, value):
    high, low = split_bf16(value)
    dot = lambda a, b: jnp.dot(a, b, preferred_element_type=jnp.float32)
    return dot(table_high, high) + (dot(table_high, low) + dot(table_low, high))


QUARTERS = 4
QUARTER = LANES // QUARTERS
PLANES = 4
AT_ONCE = 6
PLAN = (
    (2, 0, 0, 0),
    (3, 0, 0, 1),
    (1, 0, None, None),
    (2, 1, 0, 2),
    (3, 1, 0, 3),
    (1, 1, None, None),
    (2, 2, 0, 4),
    (3, 2, 1, 0),
)
ORDER = (0, 1, 2, 3, 4, 5, 6, 7)
FAR = tuple(group for group, entry in enumerate(PLAN) if entry[2] is not None)
RELAYED = ()
OWNED = tuple(tuple(g for g, entry in enumerate(PLAN) if entry[0] == plane) for plane in range(PLANES))
LOCAL = tuple(tuple(g for g in FAR if PLAN[g][2] == plane) for plane in range(PLANES))
SLOTS = max(len(groups) for groups in OWNED)
LOCAL_SLOTS = max(len(groups) for groups in LOCAL)
NEAR_SLOTS = len(OWNED[1])


def left_mask(shape):
    return lax.broadcasted_iota(jnp.int32, shape, 1) < LANES // 2


def even_mask(shape):
    return lax.broadcasted_iota(jnp.int32, shape, 1) & QUARTER == 0


def swap_halves(value):
    return pltpu.roll(value, LANES // 2, 1)


def turn_quarters(value, count):
    count %= QUARTERS
    return pltpu.roll(value, count * QUARTER, 1) if count else value


def choose_quarters(values):
    lane = lax.broadcasted_iota(jnp.int32, values[0].shape, 1)
    out = values[-1]
    for index in reversed(range(QUARTERS - 1)):
        out = jnp.where(lane < (index + 1) * QUARTER, values[index], out)
    return out


def transpose_quarters(values):
    turned = [turn_quarters(value, index) for index, value in enumerate(values)]
    mixed = [choose_quarters([turned[(u - a) % QUARTERS] for u in range(QUARTERS)]) for a in range(QUARTERS)]
    return [turn_quarters(value, -index) for index, value in enumerate(mixed)]


def interleave(one, two):
    even = even_mask(one.shape)
    return jnp.where(even, one, turn_quarters(two, 1)), jnp.where(even, turn_quarters(one, -1), two)


def offsets(count):
    return sorted(range(count), key=lambda step: abs(2 * step - count))


def repeat(first, count, at_once, body):
    def several(index, carry):
        for inner in range(at_once):
            body(first + index * at_once + inner)
        return carry

    lax.fori_loop(0, (count - first) // at_once, several, 0)


def greet_all(seq_count, ch_count, me_seq, me_ch):
    barrier = pltpu.get_barrier_semaphore()
    for step in offsets(seq_count):
        for turn in range(ch_count):
            if step or turn:
                partner = {"seq": lax.rem(me_seq + step, seq_count), "ch": lax.rem(me_ch + turn, ch_count)}
                pl.semaphore_signal(barrier, inc=1, device_id=partner, device_id_type=pl.DeviceIdType.MESH)
    return barrier


def layer_kernel(
    seq_count, ch_count,
    query_hbm, key_hbm, value_hbm, out_hbm, filter_hbm, skip_hbm, fwd_hbm, inv_hbm, tw_hbm,
    gq_ref, gk_ref, gv_ref, gf_ref,
    query_ref, key_ref, value_ref, out_ref, filter_ref, skip_ref, fwd_ref, inv_ref, tw_ref, load_sem,
    send, send_half, taps_send, recv, recv_half, taps_recv,
    result, result_half, corr_result, back, back_half, corr, corr_far,
    lines, taps_lines, spec, taps_spec, corr_spec, tw_scr, relay,
    send_sem, half_send_sem, taps_send_sem, local_taps_send_sem,
    recv_sem, half_recv_sem, taps_recv_sem,
    back_send_sem, back_half_send_sem, corr_send_sem, relay_sem, relay_taps_sem,
    back_sem, back_half_sem, corr_sem, corr_far_sem,
):
    me_seq, me_ch = lax.axis_index("seq"), lax.axis_index("ch")
    tokens, channels = key_ref.shape
    half_tokens, part_tokens = tokens // 2, tokens // QUARTERS
    half_seq = seq_count // 2
    width = seq_count // PLANES
    plane, place = lax.div(me_seq, width), lax.rem(me_seq, width)
    high = lax.div(plane, PLANES // 2)
    low = 1 - high
    scale = (seq_count * tokens) ** -0.5
    side_channels = channels // ch_count
    jobs = QUARTERS * len(PLAN)
    far_jobs = QUARTERS * len(FAR)
    local_whole = NEAR_SLOTS * ch_count * seq_count
    local_part = NEAR_SLOTS * seq_count

    def look(table):
        out = 0
        for value, known in table:
            out = out + jnp.where(known, value, 0)
        return out

    loads = [
        pltpu.make_async_copy(source, target, load_sem.at[index])
        for index, (source, target) in enumerate((
            (key_hbm, key_ref), (value_hbm, value_ref), (out_hbm, out_ref), (query_hbm, query_ref), (filter_hbm, filter_ref),
            (tw_hbm, tw_ref), (fwd_hbm, fwd_ref), (inv_hbm, inv_ref), (skip_hbm, skip_ref),
        ))
    ]
    for load in loads:
        load.start()
    barrier = greet_all(seq_count, ch_count, me_seq, me_ch)

    def start(source, target, seq, ch, send_at, recv_at):
        pltpu.make_async_remote_copy(
            src_ref=source, dst_ref=target, send_sem=send_at, recv_sem=recv_at,
            device_id={"seq": seq, "ch": ch}, device_id_type=pl.DeviceIdType.MESH,
        ).start()

    def span(ref, count, send_at, recv_at):
        return pltpu.make_async_remote_copy(
            src_ref=ref.at[pl.ds(0, count)], dst_ref=ref.at[pl.ds(0, count)], send_sem=send_at, recv_sem=recv_at,
            device_id={"seq": me_seq, "ch": me_ch}, device_id_type=pl.DeviceIdType.MESH,
        )

    def arrive(ref, count, sem):
        span(ref, count, sem, sem).wait_recv()

    def depart(ref, count, sem):
        if count:
            span(ref, count, sem, sem).wait_send()

    def prepare(group, side):
        lanes = pl.ds(pl.multiple_of(side * side_channels + group * LANES, LANES), LANES)
        base = side * jobs + QUARTERS * group

        for chunk in range(half_tokens // 16):
            pieces = []
            rows = [pl.ds(chunk * 16 + first, 16) for first in (0, half_tokens)]
            for one, two in ((key_ref, value_ref), (out_ref, query_ref)):
                for at in rows:
                    pieces.append(one[at, lanes].astype(jnp.float32) * two[at, lanes].astype(jnp.float32))
            for index, piece in enumerate(transpose_quarters(pieces)):
                send[base + index, rows[0], :] = piece

    def halve(group, side):
        far = FAR.index(group)
        for index in range(QUARTERS):
            piece = send[side * jobs + QUARTERS * group + index]
            top, bottom = piece[:part_tokens], piece[part_tokens:]
            send_half[side * far_jobs + QUARTERS * far + index] = jnp.where(left_mask(top.shape), top, swap_halves(bottom))

    def prepare_taps(group):
        lanes = pl.ds(pl.multiple_of(me_ch * side_channels + group * LANES, LANES), LANES)
        pieces = [filter_ref[part_tokens * k:part_tokens * (k + 1), lanes].astype(jnp.float32) * scale for k in range(QUARTERS)]
        for index, piece in enumerate(transpose_quarters(pieces)):
            taps_send[QUARTERS * group + index] = piece

    def turns():
        return [(step, turn) for step in offsets(width) for turn in reversed(range(ch_count))]

    def send_taps(group):
        owner, slot, near_plane, near_slot = PLAN[group]
        far = near_plane is not None
        for step in offsets(width):
            at = lax.rem(place + step, width)
            source = taps_send.at[QUARTERS * group + at]

            def to_owner():
                start(source, taps_recv.at[slot * seq_count + me_seq], owner * width + at, me_ch, taps_send_sem, taps_recv_sem.at[slot])

            def to_local():
                start(
                    source, taps_recv.at[near_plane * local_part + near_slot * half_seq + me_seq], near_plane * width + at, me_ch,
                    local_taps_send_sem, taps_recv_sem.at[SLOTS + near_slot],
                )

            sends = plane != owner if step == 0 else plane >= 0
            if group in RELAYED:
                sends = sends & (plane > 0)
            pl.when(sends)(to_owner)
            if far:
                pl.when((low == 1) & (plane != near_plane) if step == 0 else low == 1)(to_local)

        @pl.when(plane == owner)
        def _():
            taps_recv[slot * seq_count + me_seq] = taps_send[QUARTERS * group + place]

        if far:

            @pl.when(plane == near_plane)
            def _():
                taps_recv[near_plane * local_part + near_slot * half_seq + me_seq] = taps_send[QUARTERS * group + place]

    def send_group(group):
        owner, slot, near_plane, near_slot = PLAN[group]

        def whole(target_plane, index, sem):
            for step, turn in turns():
                at, ch = lax.rem(place + step, width), lax.rem(me_ch + turn, ch_count)

                def go():
                    start(send.at[ch * jobs + QUARTERS * group + at], recv.at[index], target_plane * width + at, ch, send_sem, sem)

                if step or turn:
                    go()
                else:
                    pl.when(plane != target_plane)(go)

                    @pl.when(plane == target_plane)
                    def _():
                        recv[index] = send[me_ch * jobs + QUARTERS * group + place]

        if near_plane is None:
            whole(owner, (slot * ch_count + me_ch) * seq_count + me_seq, recv_sem.at[slot])
            return

        @pl.when(plane > 0 if group in RELAYED else low == 1)
        def _():
            @pl.when(low == 1)
            def _():
                for step, turn in turns():
                    at, ch = lax.rem(place + step, width), lax.rem(me_ch + turn, ch_count)
                    start(
                        send_half.at[ch * far_jobs + QUARTERS * FAR.index(group) + at],
                        recv_half.at[slot * seq_count + me_ch * half_seq + me_seq],
                        owner * width + at, ch, half_send_sem, half_recv_sem.at[slot],
                    )

        @pl.when(high == 1)
        def _():
            whole(owner, (slot * ch_count + me_ch) * half_seq + me_seq - half_seq, recv_sem.at[slot])

        @pl.when(low == 1)
        def _():
            index = near_plane * local_whole + (near_slot * ch_count + me_ch) * half_seq + me_seq
            whole(near_plane, index, recv_sem.at[SLOTS + near_slot])

    def ready(group):
        other = lax.rem(me_ch + 1, ch_count)
        prepare_taps(group)
        prepare(group, other)
        prepare(group, me_ch)

        if group in FAR:
            pl.when(low == 1)(lambda: halves(group))

    def halves(group):
        halve(group, 0)
        halve(group, 1)

    for load in loads[:5]:
        load.wait()
    ready(0)
    pl.semaphore_wait(barrier, seq_count * ch_count - 1)

    for group in range(len(PLAN)):
        if group:
            ready(group)
        send_group(group)
        send_taps(group)
    for load in loads[5:]:
        load.wait()
    for k in range(seq_count + 1):
        for part in range(2):
            tw_scr[k, part] = jnp.broadcast_to(tw_ref[part, :, k:k + 1], (tokens, LANES))

    def analyse(source, target, blocks):
        def body(chunk, carry):
            rows = pl.ds(pl.multiple_of(chunk * 8, 8), 8)
            for k, (real, imag) in enumerate(half_spectrum([source[n, rows, :] for n in range(blocks)], 2 * blocks)):
                target[k, 0, rows, :] = real
                target[k, 1, rows, :] = jnp.zeros_like(real) if imag is None else imag
            return carry

        lax.fori_loop(0, tokens // 8, body, 0)

    def synthesise(source, target, blocks):
        def body(chunk, carry):
            rows = pl.ds(pl.multiple_of(chunk * 8, 8), 8)
            terms = [(source[k, 0, rows, :], source[k, 1, rows, :]) for k in range(blocks + 1)]
            for n, value in enumerate(real_from_half(terms, 2 * blocks, True)):
                target[n, rows, :] = value
            return carry

        lax.fori_loop(0, tokens // 8, body, 0)

    def across(table, real, imag):
        both = three_dot(table[0], table[1], jnp.concatenate([real, imag], axis=0))
        return both[:tokens], both[tokens:]

    def convolve(blocks):
        stride = seq_count // blocks
        analyse(lines, spec, blocks)
        analyse(taps_lines, taps_spec, blocks)
        forward = (fwd_ref[0], fwd_ref[1])
        inverse = (inv_ref[0], inv_ref[1])

        def middle(index, carry):
            ks = [index * AT_ONCE + inner for inner in range(AT_ONCE)]
            turns_at = [(tw_scr[stride * k, 0], tw_scr[stride * k, 1]) for k in ks]
            reals, imags = [], []
            for k, (cosine, sine) in zip(ks, turns_at):
                for held in (spec, taps_spec):
                    real, imag = held[k, 0], held[k, 1]
                    reals.append(real * cosine + imag * sine)
                    imags.append(imag * cosine - real * sine)
            real, imag = across(forward, jnp.concatenate(reals, axis=1), jnp.concatenate(imags, axis=1))
            reals, imags = [], []
            for inner in range(AT_ONCE):
                first = 2 * LANES * inner
                a_r, a_i = real[:, first:first + LANES], imag[:, first:first + LANES]
                h_r, h_i = real[:, first + LANES:first + 2 * LANES], imag[:, first + LANES:first + 2 * LANES]
                h_i = jnp.where(left_mask(h_i.shape), h_i, -h_i)
                g_r, g_i = swap_halves(a_r), swap_halves(a_i)
                reals += [a_r * h_r - a_i * h_i, a_r * g_r + a_i * g_i]
                imags += [a_r * h_i + a_i * h_r, a_r * g_i - a_i * g_r]
            real, imag = across(inverse, jnp.concatenate(reals, axis=1), jnp.concatenate(imags, axis=1))
            for inner, (k, (cosine, sine)) in enumerate(zip(ks, turns_at)):
                weight = jnp.where((k == 0) | (k == blocks), 0.5 / (blocks * tokens), 1.0 / (blocks * tokens))
                cosine, sine = cosine * weight, sine * weight
                for side, held in enumerate((spec, corr_spec)):
                    first = LANES * (2 * inner + side)
                    br, bi = real[:, first:first + LANES], imag[:, first:first + LANES]
                    held[k, 0] = br * cosine - bi * sine
                    held[k, 1] = bi * cosine + br * sine
            return carry

        lax.fori_loop(0, blocks // AT_ONCE + 1, middle, 0)
        synthesise(spec, lines, blocks)
        synthesise(corr_spec, taps_lines, blocks)

    def open_taps(first, blocks):
        def body(n):
            packed = taps_recv[first + n]
            turned = [turn_quarters(packed, count) for count in range(QUARTERS)]
            for k in range(QUARTERS):
                taps_lines[n, part_tokens * k:part_tokens * (k + 1), :] = choose_quarters([turned[(u - k) % QUARTERS] for u in range(QUARTERS)])

        repeat(0, blocks, 8, body)

    def open_whole(start_at, blocks, first):
        def body(n):
            base = start_at + n - first
            top, bottom = interleave(recv[base], recv[base + blocks - first])
            lines[n, :half_tokens, :] = top
            lines[n, half_tokens:, :] = bottom

        repeat(first, blocks, 4, body)

    def open_half(slot):
        def body(n):
            one, two = recv_half[slot * seq_count + n], recv_half[slot * seq_count + half_seq + n]
            left = left_mask(one.shape)
            for first in (0, part_tokens):
                top, bottom = interleave(one, two)
                lines[n, first:first + part_tokens, :] = jnp.where(left, top, 0.0)
                lines[n, half_tokens + first:half_tokens + first + part_tokens, :] = jnp.where(left, bottom, 0.0)
                one, two = swap_halves(one), swap_halves(two)

        repeat(0, half_seq, 4, body)

    def close_whole(start_at, blocks, first):
        def body(n):
            base = start_at + n - first
            one, two = interleave(lines[n, :half_tokens, :], lines[n, half_tokens:, :])
            result[base] = one
            result[base + blocks - first] = two

        repeat(first, blocks, 4, body)

    def close_half(slot):
        def body(n):
            for index, piece in enumerate(interleave(lines[n, :half_tokens, :], lines[n, half_tokens:, :])):
                top, bottom = piece[:part_tokens], piece[part_tokens:]
                result_half[slot * seq_count + index * half_seq + n] = jnp.where(left_mask(top.shape), swap_halves(bottom), top)

        repeat(0, half_seq, 4, body)

    def close_corr(first, blocks):
        def body(n):
            pieces = []
            for k in range(QUARTERS):
                piece = taps_lines[n, part_tokens * k:part_tokens * (k + 1), :]
                pieces.append(turn_quarters((piece + turn_quarters(piece, -1)) * scale, k))
            corr_result[first + n] = choose_quarters(pieces)

        repeat(0, blocks, 4, body)

    def deliver(base, corr_base, group, first, count):
        job = QUARTERS * group + place
        for step in offsets(count):
            at = lax.rem(me_seq + step, count)
            for turn in range(ch_count):
                ch = lax.rem(me_ch + turn, ch_count)
                if step or turn:
                    start(result.at[base + ch * count + at], back.at[me_ch * jobs + job], first + at, ch, back_send_sem, back_sem.at[group])
            if step:
                start(corr_result.at[corr_base + first + at], corr.at[job], first + at, me_ch, corr_send_sem, corr_sem.at[group])
        back[me_ch * jobs + job] = result[base + me_ch * count + me_seq - first]
        corr[job] = corr_result[corr_base + me_seq]

    def deliver_half(slot, group):
        far = QUARTERS * look([(FAR.index(g), group == g) for g in FAR]) + place
        for step in offsets(half_seq):
            seq = lax.rem(me_seq + step, half_seq)
            for turn in range(ch_count):
                ch = lax.rem(me_ch + turn, ch_count)
                start(
                    result_half.at[slot * seq_count + ch * half_seq + seq], back_half.at[me_ch * far_jobs + far],
                    seq, ch, back_half_send_sem, back_half_sem.at[group],
                )
            start(corr_result.at[slot * seq_count + seq], corr_far.at[far], seq, me_ch, corr_send_sem, corr_far_sem.at[group])

    others = seq_count * ch_count - 1

    def owner_job(slot, carry):
        group = look([(g, (plane == PLAN[g][0]) & (slot == PLAN[g][1])) for g in range(len(PLAN))])
        arrive(taps_recv, seq_count - 1, taps_recv_sem.at[slot])
        open_taps(slot * seq_count, seq_count)
        near_base = slot * ch_count * seq_count
        far_base = slot * ch_count * half_seq

        @pl.when(high == 0)
        def _():
            arrive(recv, others, recv_sem.at[slot])
            open_whole(near_base, seq_count, 0)

        @pl.when(high == 1)
        def _():
            arrive(recv_half, seq_count, half_recv_sem.at[slot])
            open_half(slot)
            arrive(recv, seq_count - 1, recv_sem.at[slot])
            open_whole(far_base, seq_count, half_seq)

        convolve(seq_count)
        close_corr(slot * seq_count, seq_count)

        @pl.when(high == 0)
        def _():
            close_whole(near_base, seq_count, 0)
            deliver(near_base, slot * seq_count, group, 0, seq_count)

        @pl.when(high == 1)
        def _():
            close_half(slot)
            close_whole(far_base, seq_count, half_seq)
            deliver_half(slot, group)
            deliver(far_base, slot * seq_count, group, half_seq, half_seq)

        return carry

    def local_arrive(slot):
        arrive(taps_recv, half_seq - 1, taps_recv_sem.at[SLOTS + slot])
        arrive(recv, seq_count - 1, recv_sem.at[SLOTS + slot])

    def local_job(slot, carry):
        group = look([(g, (plane == PLAN[g][2]) & (slot == PLAN[g][3])) for g in FAR])
        base = plane * local_whole + slot * ch_count * half_seq
        part_base = plane * local_part + slot * half_seq
        pl.when(plane == 0)(lambda: local_arrive(slot)) if RELAYED else local_arrive(slot)
        open_taps(part_base, half_seq)
        open_whole(base, half_seq, 0)
        convolve(half_seq)
        close_corr(part_base, half_seq)
        close_whole(base, half_seq, 0)
        deliver(base, part_base, group, 0, half_seq)
        return carry

    def hand_on(group):
        owner, slot, near_plane, near_slot = PLAN[group]
        local_arrive(near_slot)
        seq = owner * width + place
        for n in range(width):
            start(
                taps_recv.at[near_plane * local_part + near_slot * half_seq + n], taps_recv.at[slot * seq_count + n],
                seq, me_ch, relay_taps_sem, taps_recv_sem.at[slot],
            )
        for ch in range(ch_count):
            for n in range(width):
                piece = recv[near_plane * local_whole + (near_slot * ch_count + ch) * half_seq + n]
                top, bottom = piece[:part_tokens], piece[part_tokens:]
                relay[(near_slot * ch_count + ch) * width + n] = jnp.where(left_mask(top.shape), top, swap_halves(bottom))
        for ch in range(ch_count):
            for n in range(width):
                start(
                    relay.at[(near_slot * ch_count + ch) * width + n], recv_half.at[slot * seq_count + ch * half_seq + n],
                    seq, me_ch, relay_sem, half_recv_sem.at[slot],
                )

    @pl.when(plane == 1)
    def _():
        for group in RELAYED:
            hand_on(group)

    lax.fori_loop(0, look([(len(groups), plane == p) for p, groups in enumerate(OWNED)]), owner_job, 0)
    lax.fori_loop(0, look([(len(groups), plane == p) for p, groups in enumerate(LOCAL)]), local_job, 0)

    def finish(group, side):
        lanes = pl.ds(pl.multiple_of(side * side_channels + group * LANES, LANES), LANES)
        base = side * jobs + QUARTERS * group
        skip = skip_ref[:, lanes]

        for chunk in range(half_tokens // 16):
            rows = [pl.ds(chunk * 16 + first, 16) for first in (0, half_tokens)]
            pieces = transpose_quarters([back[base + index, rows[0], :] for index in range(QUARTERS)])
            for at, conv, behind in zip(rows, pieces[:2], pieces[2:]):
                query_f = query_ref[at, lanes].astype(jnp.float32)
                key_f = key_ref[at, lanes].astype(jnp.float32)
                value_f = value_ref[at, lanes].astype(jnp.float32)
                out_f = out_ref[at, lanes].astype(jnp.float32)
                conv = conv + skip * (key_f * value_f)
                behind = behind + skip * (out_f * query_f)
                gq_ref[at, lanes] = (out_f * conv).astype(jnp.bfloat16)
                gk_ref[at, lanes] = (behind * value_f).astype(jnp.bfloat16)
                gv_ref[at, lanes] = (behind * key_f).astype(jnp.bfloat16)

    def finish_corr(group):
        lanes = pl.ds(pl.multiple_of(group * LANES, LANES), LANES)
        pieces = transpose_quarters([corr[QUARTERS * group + index] for index in range(QUARTERS)])
        for k, piece in enumerate(pieces):
            gf_ref[part_tokens * k:part_tokens * (k + 1), lanes] = piece

    def join_half(group):
        far = FAR.index(group)
        for side in range(ch_count):
            for index in range(QUARTERS):
                piece = back_half[side * far_jobs + QUARTERS * far + index]
                left = left_mask(piece.shape)
                place_at = side * jobs + QUARTERS * group + index
                back[place_at, :part_tokens, :] += jnp.where(left, 0.0, piece)
                back[place_at, part_tokens:, :] += jnp.where(left, 0.0, swap_halves(piece))
        for index in range(QUARTERS):
            corr[QUARTERS * group + index] += corr_far[QUARTERS * far + index]

    for group in ORDER:
        owner, _, near_plane, _ = PLAN[group]
        mine = plane == owner
        if near_plane is not None:
            mine = mine | (plane == near_plane)
        for own in (0, 1):

            @pl.when(mine if own else jnp.logical_not(mine))
            def _():
                arrive(back, QUARTERS * ch_count - own, back_sem.at[group])
                arrive(corr, QUARTERS - own, corr_sem.at[group])

        if near_plane is not None:

            @pl.when(low == 1)
            def _():
                arrive(back_half, QUARTERS * ch_count, back_half_sem.at[group])
                arrive(corr_far, QUARTERS, corr_far_sem.at[group])
                join_half(group)

        finish(group, 0)
        finish(group, 1)
        finish_corr(group)

    for p in range(PLANES):
        is_low = p < PLANES // 2
        owned, local = len(OWNED[p]), len(LOCAL[p])
        direct = len(FAR) - (0 if p else len(RELAYED))

        @pl.when(plane == p)
        def _():
            depart(send, ch_count * jobs - owned - local, send_sem)
            depart(send_half, ch_count * QUARTERS * direct if is_low else 0, half_send_sem)
            depart(taps_send, jobs - owned - (0 if p else QUARTERS * len(RELAYED)), taps_send_sem)
            depart(taps_send, far_jobs - local if is_low else 0, local_taps_send_sem)
            depart(result, owned * (others if is_low else seq_count - 1) + local * (seq_count - 1), back_send_sem)
            depart(result_half, 0 if is_low else owned * seq_count, back_half_send_sem)
            depart(corr_result, owned * (seq_count - 1) + local * (half_seq - 1), corr_send_sem)
            if p == 1 and RELAYED:
                depart(relay, len(RELAYED) * ch_count * width, relay_sem)
                depart(taps_recv, len(RELAYED) * width, relay_taps_sem)


def tables(seq_count, tokens):
    index = np.arange(tokens)
    angle = 2.0 * np.pi / tokens * (index[:, None] * index[None, :] % tokens)
    cosine, sine = np.cos(angle), np.sin(angle)
    forward = np.block([[cosine, sine], [-sine, cosine]]).astype(np.float32)
    inverse = np.block([[cosine, -sine], [sine, cosine]]).astype(np.float32)

    def pieces(table):
        table = jnp.asarray(table)
        return jnp.stack(split_bf16(table))

    turn = 2.0 * np.pi / (2 * seq_count * tokens) * (np.arange(seq_count + 1)[:, None] * index[None, :])
    twiddle = jnp.asarray(np.stack([np.cos(turn).T, np.sin(turn).T]).astype(np.float32))
    return pieces(forward), pieces(inverse), twiddle


def hand_out(*refs):
    count = len(refs) // 2
    copies = [pltpu.make_async_copy(refs[i], refs[count + i], refs[-1].at[i]) for i in range(count)]
    for copy in copies:
        copy.start()
    for copy in copies:
        copy.wait()


def fast_shards(query_gate, key_input, value_input, grad_output, filter_raw, skip_gain):
    seq_count, ch_count = lax.axis_size("seq"), lax.axis_size("ch")
    _, tokens, channels = key_input.shape
    vmem = pl.BlockSpec(memory_space=pltpu.VMEM)
    jobs = QUARTERS * len(PLAN)
    far_jobs = QUARTERS * len(FAR)
    whole = lambda count: pltpu.VMEM((count, tokens // 2, LANES), jnp.float32)
    part = lambda count: pltpu.VMEM((count, tokens // QUARTERS, LANES), jnp.float32)
    spectrum = pltpu.VMEM((seq_count + AT_ONCE, 2, tokens, LANES), jnp.float32)
    turning = pltpu.VMEM((seq_count + 2 * AT_ONCE, 2, tokens, LANES), jnp.float32)
    lines = pltpu.VMEM((seq_count, tokens, LANES), jnp.float32)
    slots = SLOTS * seq_count
    wholes = max(ch_count * NEAR_SLOTS + len(LOCAL[1]), SLOTS, LOCAL_SLOTS) * seq_count
    single = pltpu.SemaphoreType.DMA
    several = lambda count: pltpu.SemaphoreType.DMA((count,))
    inputs = (query_gate[0], key_input[0], value_input[0], grad_output[0], filter_raw, skip_gain[None], *tables(seq_count, tokens))
    grads = pl.pallas_call(
        lambda *refs: layer_kernel(seq_count, ch_count, *refs),
        in_specs=[pl.BlockSpec(memory_space=pltpu.HBM)] * len(inputs),
        out_specs=[vmem] * 4,
        out_shape=[pltpu.VMEM((tokens, channels), jnp.bfloat16)] * 3 + [pltpu.VMEM((tokens, channels // ch_count), jnp.float32)],
        scratch_shapes=[pltpu.VMEM(array.shape, array.dtype) for array in inputs] + [several(len(inputs))] + [
            whole(ch_count * jobs), part(ch_count * far_jobs), part(jobs), whole(wholes), part(slots), part(slots),
            whole(wholes), part(slots), part(slots), whole(ch_count * jobs), part(ch_count * far_jobs), part(jobs), part(far_jobs),
            lines, lines, spectrum, spectrum, spectrum, turning, part(max(len(RELAYED), 1) * seq_count // 2),
            single, single, single, single,
            several(SLOTS + LOCAL_SLOTS), several(SLOTS), several(SLOTS + LOCAL_SLOTS),
            single, single, single, single, single,
            several(len(PLAN)), several(len(PLAN)), several(len(PLAN)), several(len(PLAN)),
        ],
        compiler_params=pltpu.CompilerParams(vmem_limit_bytes=VMEM_LIMIT, collective_id=0, has_side_effects=True),
        name="layer",
    )(*inputs)
    grads = pl.pallas_call(
        hand_out,
        in_specs=[vmem] * len(grads),
        out_specs=[pl.BlockSpec(memory_space=pltpu.HBM)] * len(grads),
        out_shape=[jax.ShapeDtypeStruct(array.shape, array.dtype) for array in grads],
        scratch_shapes=[several(len(grads))],
        compiler_params=pltpu.CompilerParams(vmem_limit_bytes=1024 * 1024),
        name="hand_out",
    )(*grads)
    return (grads[0][None], grads[1][None], grads[2][None], grads[3])


def solution(mesh):
    in_specs = (
        P("ch", "seq", None),
        P("ch", "seq", None),
        P("ch", "seq", None),
        P("ch", "seq", None),
        P("seq", None),
        P(),
    )
    out_specs = (P("ch", "seq", None), P("ch", "seq", None), P("ch", "seq", None), P("seq", "ch"))

    def body(*arrays):
        seq_count, ch_count = mesh.shape["seq"], mesh.shape["ch"]
        _, tokens, channels = arrays[0].shape
        fits = ch_count == 2 and tokens == LANES and seq_count == PLANES * QUARTERS and channels == ch_count * len(PLAN) * LANES
        return (fast_shards if fits else shards)(*arrays)

    return jax.shard_map(body, mesh=mesh, in_specs=in_specs, out_specs=out_specs, check_vma=False)
```

```python
import math

import numpy as np

import jax
import jax.numpy as jnp
from jax import lax
from jax.experimental import pallas as pl
from jax.experimental.pallas import tpu as pltpu
from jax.sharding import PartitionSpec as P


def angle_table(row_index, col_index, modulus):
    turn_count = row_index[:, None] * col_index[None, :] % modulus
    angles = turn_count.astype(jnp.float32) * (2.0 * math.pi / modulus)
    return (jnp.cos(angles), jnp.sin(angles))


def contract(pattern, table, operand):
    return jnp.einsum(
        pattern, table, operand, precision=lax.Precision.HIGHEST, preferred_element_type=jnp.float32
    )


def rotate(pattern, cos_table, sin_table, sense_sign, real_part, imag_part, want_imag):
    if imag_part is None:
        cos_term = contract(pattern, cos_table, real_part)
        return (cos_term, sense_sign * contract(pattern, sin_table, real_part))
    real_out = contract(pattern, cos_table, real_part) - sense_sign * contract(
        pattern, sin_table, imag_part
    )
    if not want_imag:
        return (real_out, None)
    imag_out = contract(pattern, cos_table, imag_part) + sense_sign * contract(
        pattern, sin_table, real_part
    )
    return (real_out, imag_out)


def twist(cos_table, sin_table, sense_sign, real_part, imag_part):
    return (
        real_part * cos_table - sense_sign * imag_part * sin_table,
        imag_part * cos_table + sense_sign * real_part * sin_table,
    )


def spectral_terms(z_real, z_imag, g_real, g_imag, h_real, h_imag):
    conv_real = z_real * h_real - z_imag * h_imag
    conv_imag = z_real * h_imag + z_imag * h_real
    back_real = h_real * g_real + h_imag * g_imag
    back_imag = h_real * g_imag - h_imag * g_real
    corr_real = z_real * g_real + z_imag * g_imag
    corr_imag = z_real * g_imag - z_imag * g_real
    return (conv_real - back_imag, conv_imag + back_real, corr_real, corr_imag)


def shards(query_gate, key_input, value_input, grad_output, filter_raw, skip_gain):
    seq_count = lax.axis_size("seq")
    key_f = key_input[0].astype(jnp.float32)
    value_f = value_input[0].astype(jnp.float32)
    out_f = grad_output[0].astype(jnp.float32)
    mixed = key_f * value_f
    gated = out_f * query_gate[0].astype(jnp.float32)
    tokens, channels = mixed.shape
    seq_length = tokens * seq_count
    full_length = 2 * seq_length
    inverse_scale = 1.0 / full_length
    filter_taps = filter_raw.astype(jnp.float32) * seq_length ** (-0.5)
    freq_one = jnp.arange(2 * seq_count, dtype=jnp.int32)
    block_index = jnp.arange(seq_count, dtype=jnp.int32)
    offset_index = jnp.arange(tokens, dtype=jnp.int32)
    cos_one, sin_one = angle_table(freq_one, block_index, 2 * seq_count)
    cos_inv, sin_inv = angle_table(block_index, freq_one, 2 * seq_count)
    cos_two, sin_two = angle_table(offset_index, offset_index, tokens)
    local_width = channels // seq_count
    arrived = (
        lax.all_to_all(mixed.T, "seq", split_axis=0, concat_axis=1, tiled=True),
        lax.all_to_all(gated.T, "seq", split_axis=0, concat_axis=1, tiled=True),
        lax.all_to_all(filter_taps.T, "seq", split_axis=0, concat_axis=1, tiled=True),
    )
    cos_tw, sin_tw = angle_table(freq_one, offset_index, full_length)
    spectra = []
    for line_data in arrived:
        lines = line_data.reshape(local_width, seq_count, tokens)
        real_part, imag_part = rotate("kn,cnm->ckm", cos_one, sin_one, -1.0, lines, None, True)
        real_part, imag_part = twist(cos_tw, sin_tw, -1.0, real_part, imag_part)
        spectra.append(rotate("jm,ckm->ckj", cos_two, sin_two, -1.0, real_part, imag_part, True))
    packed_real, packed_imag, corr_real, corr_imag = spectral_terms(
        spectra[0][0], spectra[0][1], spectra[1][0], spectra[1][1], spectra[2][0], spectra[2][1]
    )
    pr_mid, pi_mid = rotate("mj,ckj->ckm", cos_two, sin_two, 1.0, packed_real, packed_imag, True)
    pr_mid, pi_mid = twist(cos_tw, sin_tw, 1.0, pr_mid, pi_mid)
    cr_mid, ci_mid = rotate("mj,ckj->ckm", cos_two, sin_two, 1.0, corr_real, corr_imag, True)
    cr_mid, ci_mid = twist(cos_tw, sin_tw, 1.0, cr_mid, ci_mid)
    conv_lines, back_lines = rotate("nk,ckm->cnm", cos_inv, sin_inv, 1.0, pr_mid, pi_mid, True)
    corr_lines = rotate("nk,ckm->cnm", cos_inv, sin_inv, 1.0, cr_mid, ci_mid, False)[0]
    conv_lines = (conv_lines * inverse_scale).reshape(local_width, seq_length)
    back_lines = (back_lines * inverse_scale).reshape(local_width, seq_length)
    corr_lines = (corr_lines * inverse_scale).reshape(local_width, seq_length)
    returned = (
        lax.all_to_all(conv_lines, "seq", split_axis=1, concat_axis=0, tiled=True),
        lax.all_to_all(back_lines, "seq", split_axis=1, concat_axis=0, tiled=True),
        lax.all_to_all(corr_lines, "seq", split_axis=1, concat_axis=0, tiled=True),
    )
    conv_time = returned[0].T
    back_time = returned[1].T
    corr_time = returned[2].T
    conv_full = conv_time + skip_gain * mixed
    back_full = back_time + skip_gain * gated
    grad_query = (out_f * conv_full).astype(jnp.bfloat16)[None]
    grad_key = (back_full * value_f).astype(jnp.bfloat16)[None]
    grad_value = (back_full * key_f).astype(jnp.bfloat16)[None]
    grad_filter = lax.psum_scatter(
        corr_time * seq_length ** (-0.5), "ch", scatter_dimension=1, tiled=True
    )
    return (grad_query, grad_key, grad_value, grad_filter)


LANES = 128
VMEM_LIMIT = 60 * 1024 * 1024


def times_root(pair, turn, size):
    real, imag = pair
    turn %= size
    if turn == 0:
        return pair
    if 4 * turn == size:
        return (-imag, real)
    if 2 * turn == size:
        return (-real, -imag)
    if 4 * turn == 3 * size:
        return (imag, -real)
    cosine = math.cos(2.0 * math.pi * turn / size)
    sine = math.sin(2.0 * math.pi * turn / size)
    return (real * cosine - imag * sine, real * sine + imag * cosine)


def complex_dft(values, sense):
    size = len(values)
    if size == 1:
        return values
    even = complex_dft(values[0::2], sense)
    odd = complex_dft(values[1::2], sense)
    low, high = [], []
    for k in range(size // 2):
        er, ei = even[k]
        tr, ti = times_root(odd[k], sense * k, size)
        low.append((er + tr, ei + ti))
        high.append((er - tr, ei - ti))
    return low + high


def half_spectrum(values, size):
    if size == 2:
        return [(values[0] + values[1], None), (values[0] - values[1], None)]
    half, quarter = size // 2, size // 4
    if len(values) == half:
        total, difference = values, values
    else:
        total = [values[n] + values[n + half] for n in range(half)]
        difference = [values[n] - values[n + half] for n in range(half)]
    out = [None] * (half + 1)
    out[0::2] = half_spectrum(total, half)
    turned = [times_root((difference[n], -difference[n + quarter]), -n, size) for n in range(quarter)]
    for index, (real, imag) in enumerate(complex_dft(turned, -1)):
        k = 1 + 4 * index
        if k <= half:
            out[k] = (real, imag)
        else:
            out[size - k] = (real, -imag)
    return out


def real_from_half(terms, size, first_half):
    if size == 2:
        return [terms[0][0] + terms[1][0], terms[0][0] - terms[1][0]]
    half, quarter = size // 2, size // 4
    even = real_from_half(terms[0::2], half, False)
    chosen = []
    for index in range(quarter):
        k = 1 + 4 * index
        if k <= half:
            chosen.append(terms[k])
        else:
            real, imag = terms[size - k]
            chosen.append((real, -imag))
    turned = [times_root(pair, n, size) for n, pair in enumerate(complex_dft(chosen, 1))]
    odd = [pair[0] for pair in turned] + [-pair[1] for pair in turned]
    out = [even[n] + odd[n] for n in range(half)]
    if first_half:
        return out
    return out + [even[n] - odd[n] for n in range(half)]


def split_bf16(value):
    high = value.astype(jnp.bfloat16)
    return high, (value - high.astype(jnp.float32)).astype(jnp.bfloat16)


def three_dot(table_high, table_low, value):
    high, low = split_bf16(value)
    dot = lambda a, b: jnp.dot(a, b, preferred_element_type=jnp.float32)
    return dot(table_high, high) + (dot(table_high, low) + dot(table_low, high))


QUARTERS = 4
QUARTER = LANES // QUARTERS
PLANES = 4
AT_ONCE = 6
LATE = 2
PLAN = (
    (2, 0, 0, 0),
    (3, 0, 0, 1),
    (1, 0, None, None),
    (2, 1, 0, 2),
    (3, 1, 0, 3),
    (1, 1, None, None),
    (2, 2, 0, 4),
    (3, 2, 1, 0),
)
ORDER = (0, 1, 2, 3, 4, 5, 6, 7)
FAR = tuple(group for group, entry in enumerate(PLAN) if entry[2] is not None)
RELAYED = ()
OWNED = tuple(tuple(g for g, entry in enumerate(PLAN) if entry[0] == plane) for plane in range(PLANES))
LOCAL = tuple(tuple(g for g in FAR if PLAN[g][2] == plane) for plane in range(PLANES))
SLOTS = max(len(groups) for groups in OWNED)
LOCAL_SLOTS = max(len(groups) for groups in LOCAL)
NEAR_SLOTS = len(OWNED[1])


def left_mask(shape):
    return lax.broadcasted_iota(jnp.int32, shape, 1) < LANES // 2


def even_mask(shape):
    return lax.broadcasted_iota(jnp.int32, shape, 1) & QUARTER == 0


def swap_halves(value):
    return pltpu.roll(value, LANES // 2, 1)


def turn_quarters(value, count):
    count %= QUARTERS
    return pltpu.roll(value, count * QUARTER, 1) if count else value


def choose_quarters(values):
    lane = lax.broadcasted_iota(jnp.int32, values[0].shape, 1)
    out = values[-1]
    for index in reversed(range(QUARTERS - 1)):
        out = jnp.where(lane < (index + 1) * QUARTER, values[index], out)
    return out


def transpose_quarters(values):
    turned = [turn_quarters(value, index) for index, value in enumerate(values)]
    mixed = [choose_quarters([turned[(u - a) % QUARTERS] for u in range(QUARTERS)]) for a in range(QUARTERS)]
    return [turn_quarters(value, -index) for index, value in enumerate(mixed)]


def interleave(one, two):
    even = even_mask(one.shape)
    return jnp.where(even, one, turn_quarters(two, 1)), jnp.where(even, turn_quarters(one, -1), two)


def offsets(count):
    return sorted(range(count), key=lambda step: abs(2 * step - count))


def repeat(first, count, at_once, body):
    def several(index, carry):
        for inner in range(at_once):
            body(first + index * at_once + inner)
        return carry

    lax.fori_loop(0, (count - first) // at_once, several, 0)


def greet_all(seq_count, ch_count, me_seq, me_ch):
    barrier = pltpu.get_barrier_semaphore()
    for step in offsets(seq_count):
        for turn in range(ch_count):
            if step or turn:
                partner = {"seq": lax.rem(me_seq + step, seq_count), "ch": lax.rem(me_ch + turn, ch_count)}
                pl.semaphore_signal(barrier, inc=1, device_id=partner, device_id_type=pl.DeviceIdType.MESH)
    return barrier


def layer_kernel(
    seq_count, ch_count,
    query_hbm, key_hbm, value_hbm, out_hbm, filter_hbm, skip_hbm, fwd_hbm, inv_hbm, tw_hbm,
    gq_ref, gk_ref, gv_ref, gf_ref,
    query_ref, key_ref, value_ref, out_ref, filter_ref, skip_ref, fwd_ref, inv_ref, tw_ref, load_sem,
    send, send_half, taps_send, recv, recv_half, taps_recv,
    result, result_half, corr_result, back, back_half, corr, corr_far,
    lines, taps_lines, spec, taps_spec, corr_spec, tw_scr, relay,
    send_sem, half_send_sem, taps_send_sem, local_taps_send_sem,
    recv_sem, half_recv_sem, taps_recv_sem,
    back_send_sem, back_half_send_sem, corr_send_sem, relay_sem, relay_taps_sem,
    back_sem, back_half_sem, corr_sem, corr_far_sem,
):
    me_seq, me_ch = lax.axis_index("seq"), lax.axis_index("ch")
    tokens, channels = key_ref.shape
    half_tokens, part_tokens = tokens // 2, tokens // QUARTERS
    half_seq = seq_count // 2
    width = seq_count // PLANES
    plane, place = lax.div(me_seq, width), lax.rem(me_seq, width)
    high = lax.div(plane, PLANES // 2)
    low = 1 - high
    scale = (seq_count * tokens) ** -0.5
    side_channels = channels // ch_count
    jobs = QUARTERS * len(PLAN)
    far_jobs = QUARTERS * len(FAR)
    local_whole = NEAR_SLOTS * ch_count * seq_count
    local_part = NEAR_SLOTS * seq_count

    def look(table):
        out = 0
        for value, known in table:
            out = out + jnp.where(known, value, 0)
        return out

    loads = [
        pltpu.make_async_copy(source, target, load_sem.at[index])
        for index, (source, target) in enumerate((
            (key_hbm, key_ref), (value_hbm, value_ref), (out_hbm, out_ref), (query_hbm, query_ref), (filter_hbm, filter_ref),
            (tw_hbm, tw_ref), (fwd_hbm, fwd_ref), (inv_hbm, inv_ref), (skip_hbm, skip_ref),
        ))
    ]
    for load in loads:
        load.start()
    barrier = greet_all(seq_count, ch_count, me_seq, me_ch)

    def start(source, target, seq, ch, send_at, recv_at):
        pltpu.make_async_remote_copy(
            src_ref=source, dst_ref=target, send_sem=send_at, recv_sem=recv_at,
            device_id={"seq": seq, "ch": ch}, device_id_type=pl.DeviceIdType.MESH,
        ).start()

    def span(ref, count, send_at, recv_at):
        return pltpu.make_async_remote_copy(
            src_ref=ref.at[pl.ds(0, count)], dst_ref=ref.at[pl.ds(0, count)], send_sem=send_at, recv_sem=recv_at,
            device_id={"seq": me_seq, "ch": me_ch}, device_id_type=pl.DeviceIdType.MESH,
        )

    def arrive(ref, count, sem):
        span(ref, count, sem, sem).wait_recv()

    def depart(ref, count, sem):
        if count:
            span(ref, count, sem, sem).wait_send()

    def prepare(group, side):
        lanes = pl.ds(pl.multiple_of(side * side_channels + group * LANES, LANES), LANES)
        base = side * jobs + QUARTERS * group

        for chunk in range(half_tokens // 16):
            pieces = []
            rows = [pl.ds(chunk * 16 + first, 16) for first in (0, half_tokens)]
            for one, two in ((key_ref, value_ref), (out_ref, query_ref)):
                for at in rows:
                    pieces.append(one[at, lanes].astype(jnp.float32) * two[at, lanes].astype(jnp.float32))
            for index, piece in enumerate(transpose_quarters(pieces)):
                send[base + index, rows[0], :] = piece

    def halve(group, side):
        far = FAR.index(group)
        for index in range(QUARTERS):
            piece = send[side * jobs + QUARTERS * group + index]
            top, bottom = piece[:part_tokens], piece[part_tokens:]
            send_half[side * far_jobs + QUARTERS * far + index] = jnp.where(left_mask(top.shape), top, swap_halves(bottom))

    def prepare_taps(group):
        lanes = pl.ds(pl.multiple_of(me_ch * side_channels + group * LANES, LANES), LANES)
        pieces = [filter_ref[part_tokens * k:part_tokens * (k + 1), lanes].astype(jnp.float32) * scale for k in range(QUARTERS)]
        for index, piece in enumerate(transpose_quarters(pieces)):
            taps_send[QUARTERS * group + index] = piece

    def turns():
        return [(step, turn) for step in offsets(width) for turn in reversed(range(ch_count))]

    def send_taps(group):
        owner, slot, near_plane, near_slot = PLAN[group]
        far = near_plane is not None
        for step in offsets(width):
            at = lax.rem(place + step, width)
            source = taps_send.at[QUARTERS * group + at]

            def to_owner():
                start(source, taps_recv.at[slot * seq_count + me_seq], owner * width + at, me_ch, taps_send_sem, taps_recv_sem.at[slot])

            def to_local():
                start(
                    source, taps_recv.at[near_plane * local_part + near_slot * half_seq + me_seq], near_plane * width + at, me_ch,
                    local_taps_send_sem, taps_recv_sem.at[SLOTS + near_slot],
                )

            sends = plane != owner if step == 0 else plane >= 0
            if group in RELAYED:
                sends = sends & (plane > 0)
            pl.when(sends)(to_owner)
            if far:
                pl.when((low == 1) & (plane != near_plane) if step == 0 else low == 1)(to_local)

        @pl.when(plane == owner)
        def _():
            taps_recv[slot * seq_count + me_seq] = taps_send[QUARTERS * group + place]

        if far:

            @pl.when(plane == near_plane)
            def _():
                taps_recv[near_plane * local_part + near_slot * half_seq + me_seq] = taps_send[QUARTERS * group + place]

    def whole(group, target_plane, index, sem):
        for step, turn in turns():
            at, ch = lax.rem(place + step, width), lax.rem(me_ch + turn, ch_count)

            def go():
                start(send.at[ch * jobs + QUARTERS * group + at], recv.at[index], target_plane * width + at, ch, send_sem, sem)

            if step or turn:
                go()
            else:
                pl.when(plane != target_plane)(go)

                @pl.when(plane == target_plane)
                def _():
                    recv[index] = send[me_ch * jobs + QUARTERS * group + place]

    def send_group(group):
        owner, slot, near_plane, near_slot = PLAN[group]

        if near_plane is None:
            whole(group, owner, (slot * ch_count + me_ch) * seq_count + me_seq, recv_sem.at[slot])
            return

        @pl.when(plane > 0 if group in RELAYED else low == 1)
        def _():
            @pl.when(low == 1)
            def _():
                for step, turn in turns():
                    at, ch = lax.rem(place + step, width), lax.rem(me_ch + turn, ch_count)
                    start(
                        send_half.at[ch * far_jobs + QUARTERS * FAR.index(group) + at],
                        recv_half.at[slot * seq_count + me_ch * half_seq + me_seq],
                        owner * width + at, ch, half_send_sem, half_recv_sem.at[slot],
                    )

        @pl.when(high == 1)
        def _():
            whole(group, owner, (slot * ch_count + me_ch) * half_seq + me_seq - half_seq, recv_sem.at[slot])

    def send_local(group):
        owner, slot, near_plane, near_slot = PLAN[group]

        @pl.when(low == 1)
        def _():
            index = near_plane * local_whole + (near_slot * ch_count + me_ch) * half_seq + me_seq
            whole(group, near_plane, index, recv_sem.at[SLOTS + near_slot])

    def ready(group):
        other = lax.rem(me_ch + 1, ch_count)
        prepare_taps(group)
        prepare(group, other)
        prepare(group, me_ch)

        if group in FAR:
            pl.when(low == 1)(lambda: halves(group))

    def halves(group):
        halve(group, 0)
        halve(group, 1)

    for load in loads[:5]:
        load.wait()
    ready(0)
    pl.semaphore_wait(barrier, seq_count * ch_count - 1)

    for group in range(len(PLAN)):
        if group:
            ready(group)
        send_taps(group)
        send_group(group)
        if group - LATE in FAR:
            send_local(group - LATE)
    for group in range(len(PLAN) - LATE, len(PLAN)):
        if group in FAR:
            send_local(group)
    for load in loads[5:]:
        load.wait()
    for k in range(seq_count + 1):
        for part in range(2):
            tw_scr[k, part] = jnp.broadcast_to(tw_ref[part, :, k:k + 1], (tokens, LANES))

    def analyse(source, target, blocks):
        def body(chunk, carry):
            rows = pl.ds(pl.multiple_of(chunk * 8, 8), 8)
            for k, (real, imag) in enumerate(half_spectrum([source[n, rows, :] for n in range(blocks)], 2 * blocks)):
                target[k, 0, rows, :] = real
                target[k, 1, rows, :] = jnp.zeros_like(real) if imag is None else imag
            return carry

        lax.fori_loop(0, tokens // 8, body, 0)

    def synthesise(source, target, blocks):
        def body(chunk, carry):
            rows = pl.ds(pl.multiple_of(chunk * 8, 8), 8)
            terms = [(source[k, 0, rows, :], source[k, 1, rows, :]) for k in range(blocks + 1)]
            for n, value in enumerate(real_from_half(terms, 2 * blocks, True)):
                target[n, rows, :] = value
            return carry

        lax.fori_loop(0, tokens // 8, body, 0)

    def across(table, real, imag):
        both = three_dot(table[0], table[1], jnp.concatenate([real, imag], axis=0))
        return both[:tokens], both[tokens:]

    def convolve(blocks):
        stride = seq_count // blocks
        analyse(lines, spec, blocks)
        analyse(taps_lines, taps_spec, blocks)
        forward = (fwd_ref[0], fwd_ref[1])
        inverse = (inv_ref[0], inv_ref[1])

        def middle(index, carry):
            ks = [index * AT_ONCE + inner for inner in range(AT_ONCE)]
            turns_at = [(tw_scr[stride * k, 0], tw_scr[stride * k, 1]) for k in ks]
            reals, imags = [], []
            for k, (cosine, sine) in zip(ks, turns_at):
                for held in (spec, taps_spec):
                    real, imag = held[k, 0], held[k, 1]
                    reals.append(real * cosine + imag * sine)
                    imags.append(imag * cosine - real * sine)
            real, imag = across(forward, jnp.concatenate(reals, axis=1), jnp.concatenate(imags, axis=1))
            reals, imags = [], []
            for inner in range(AT_ONCE):
                first = 2 * LANES * inner
                a_r, a_i = real[:, first:first + LANES], imag[:, first:first + LANES]
                h_r, h_i = real[:, first + LANES:first + 2 * LANES], imag[:, first + LANES:first + 2 * LANES]
                h_i = jnp.where(left_mask(h_i.shape), h_i, -h_i)
                g_r, g_i = swap_halves(a_r), swap_halves(a_i)
                reals += [a_r * h_r - a_i * h_i, a_r * g_r + a_i * g_i]
                imags += [a_r * h_i + a_i * h_r, a_r * g_i - a_i * g_r]
            real, imag = across(inverse, jnp.concatenate(reals, axis=1), jnp.concatenate(imags, axis=1))
            for inner, (k, (cosine, sine)) in enumerate(zip(ks, turns_at)):
                weight = jnp.where((k == 0) | (k == blocks), 0.5 / (blocks * tokens), 1.0 / (blocks * tokens))
                cosine, sine = cosine * weight, sine * weight
                for side, held in enumerate((spec, corr_spec)):
                    first = LANES * (2 * inner + side)
                    br, bi = real[:, first:first + LANES], imag[:, first:first + LANES]
                    held[k, 0] = br * cosine - bi * sine
                    held[k, 1] = bi * cosine + br * sine
            return carry

        lax.fori_loop(0, blocks // AT_ONCE + 1, middle, 0)
        synthesise(spec, lines, blocks)
        synthesise(corr_spec, taps_lines, blocks)

    def open_taps(first, blocks):
        def body(n):
            packed = taps_recv[first + n]
            turned = [turn_quarters(packed, count) for count in range(QUARTERS)]
            for k in range(QUARTERS):
                taps_lines[n, part_tokens * k:part_tokens * (k + 1), :] = choose_quarters([turned[(u - k) % QUARTERS] for u in range(QUARTERS)])

        repeat(0, blocks, 8, body)

    def open_whole(start_at, blocks, first):
        def body(n):
            base = start_at + n - first
            top, bottom = interleave(recv[base], recv[base + blocks - first])
            lines[n, :half_tokens, :] = top
            lines[n, half_tokens:, :] = bottom

        repeat(first, blocks, 4, body)

    def open_half(slot):
        def body(n):
            one, two = recv_half[slot * seq_count + n], recv_half[slot * seq_count + half_seq + n]
            left = left_mask(one.shape)
            for first in (0, part_tokens):
                top, bottom = interleave(one, two)
                lines[n, first:first + part_tokens, :] = jnp.where(left, top, 0.0)
                lines[n, half_tokens + first:half_tokens + first + part_tokens, :] = jnp.where(left, bottom, 0.0)
                one, two = swap_halves(one), swap_halves(two)

        repeat(0, half_seq, 4, body)

    def close_whole(start_at, blocks, first):
        def body(n):
            base = start_at + n - first
            one, two = interleave(lines[n, :half_tokens, :], lines[n, half_tokens:, :])
            result[base] = one
            result[base + blocks - first] = two

        repeat(first, blocks, 4, body)

    def close_half(slot):
        def body(n):
            for index, piece in enumerate(interleave(lines[n, :half_tokens, :], lines[n, half_tokens:, :])):
                top, bottom = piece[:part_tokens], piece[part_tokens:]
                result_half[slot * seq_count + index * half_seq + n] = jnp.where(left_mask(top.shape), swap_halves(bottom), top)

        repeat(0, half_seq, 4, body)

    def close_corr(first, blocks):
        def body(n):
            pieces = []
            for k in range(QUARTERS):
                piece = taps_lines[n, part_tokens * k:part_tokens * (k + 1), :]
                pieces.append(turn_quarters((piece + turn_quarters(piece, -1)) * scale, k))
            corr_result[first + n] = choose_quarters(pieces)

        repeat(0, blocks, 4, body)

    def deliver(base, corr_base, group, first, count):
        job = QUARTERS * group + place
        for step in offsets(count):
            at = lax.rem(me_seq + step, count)
            for turn in range(ch_count):
                ch = lax.rem(me_ch + turn, ch_count)
                if step or turn:
                    start(result.at[base + ch * count + at], back.at[me_ch * jobs + job], first + at, ch, back_send_sem, back_sem.at[group])
            if step:
                start(corr_result.at[corr_base + first + at], corr.at[job], first + at, me_ch, corr_send_sem, corr_sem.at[group])
        back[me_ch * jobs + job] = result[base + me_ch * count + me_seq - first]
        corr[job] = corr_result[corr_base + me_seq]

    def deliver_half(slot, group):
        far = QUARTERS * look([(FAR.index(g), group == g) for g in FAR]) + place
        for step in offsets(half_seq):
            seq = lax.rem(me_seq + step, half_seq)
            for turn in range(ch_count):
                ch = lax.rem(me_ch + turn, ch_count)
                start(
                    result_half.at[slot * seq_count + ch * half_seq + seq], back_half.at[me_ch * far_jobs + far],
                    seq, ch, back_half_send_sem, back_half_sem.at[group],
                )
            start(corr_result.at[slot * seq_count + seq], corr_far.at[far], seq, me_ch, corr_send_sem, corr_far_sem.at[group])

    others = seq_count * ch_count - 1

    def owner_job(slot, carry):
        group = look([(g, (plane == PLAN[g][0]) & (slot == PLAN[g][1])) for g in range(len(PLAN))])
        arrive(taps_recv, seq_count - 1, taps_recv_sem.at[slot])
        open_taps(slot * seq_count, seq_count)
        near_base = slot * ch_count * seq_count
        far_base = slot * ch_count * half_seq

        @pl.when(high == 0)
        def _():
            arrive(recv, others, recv_sem.at[slot])
            open_whole(near_base, seq_count, 0)

        @pl.when(high == 1)
        def _():
            arrive(recv_half, seq_count, half_recv_sem.at[slot])
            open_half(slot)
            arrive(recv, seq_count - 1, recv_sem.at[slot])
            open_whole(far_base, seq_count, half_seq)

        convolve(seq_count)
        close_corr(slot * seq_count, seq_count)

        @pl.when(high == 0)
        def _():
            close_whole(near_base, seq_count, 0)
            deliver(near_base, slot * seq_count, group, 0, seq_count)

        @pl.when(high == 1)
        def _():
            close_half(slot)
            close_whole(far_base, seq_count, half_seq)
            deliver_half(slot, group)
            deliver(far_base, slot * seq_count, group, half_seq, half_seq)

        return carry

    def local_arrive(slot):
        arrive(taps_recv, half_seq - 1, taps_recv_sem.at[SLOTS + slot])
        arrive(recv, seq_count - 1, recv_sem.at[SLOTS + slot])

    def local_job(slot, carry):
        group = look([(g, (plane == PLAN[g][2]) & (slot == PLAN[g][3])) for g in FAR])
        base = plane * local_whole + slot * ch_count * half_seq
        part_base = plane * local_part + slot * half_seq
        pl.when(plane == 0)(lambda: local_arrive(slot)) if RELAYED else local_arrive(slot)
        open_taps(part_base, half_seq)
        open_whole(base, half_seq, 0)
        convolve(half_seq)
        close_corr(part_base, half_seq)
        close_whole(base, half_seq, 0)
        deliver(base, part_base, group, 0, half_seq)
        return carry

    def hand_on(group):
        owner, slot, near_plane, near_slot = PLAN[group]
        local_arrive(near_slot)
        seq = owner * width + place
        for n in range(width):
            start(
                taps_recv.at[near_plane * local_part + near_slot * half_seq + n], taps_recv.at[slot * seq_count + n],
                seq, me_ch, relay_taps_sem, taps_recv_sem.at[slot],
            )
        for ch in range(ch_count):
            for n in range(width):
                piece = recv[near_plane * local_whole + (near_slot * ch_count + ch) * half_seq + n]
                top, bottom = piece[:part_tokens], piece[part_tokens:]
                relay[(near_slot * ch_count + ch) * width + n] = jnp.where(left_mask(top.shape), top, swap_halves(bottom))
        for ch in range(ch_count):
            for n in range(width):
                start(
                    relay.at[(near_slot * ch_count + ch) * width + n], recv_half.at[slot * seq_count + ch * half_seq + n],
                    seq, me_ch, relay_sem, half_recv_sem.at[slot],
                )

    @pl.when(plane == 1)
    def _():
        for group in RELAYED:
            hand_on(group)

    lax.fori_loop(0, look([(len(groups), plane == p) for p, groups in enumerate(OWNED)]), owner_job, 0)
    lax.fori_loop(0, look([(len(groups), plane == p) for p, groups in enumerate(LOCAL)]), local_job, 0)

    def finish(group, side):
        lanes = pl.ds(pl.multiple_of(side * side_channels + group * LANES, LANES), LANES)
        base = side * jobs + QUARTERS * group
        skip = skip_ref[:, lanes]

        for chunk in range(half_tokens // 16):
            rows = [pl.ds(chunk * 16 + first, 16) for first in (0, half_tokens)]
            pieces = transpose_quarters([back[base + index, rows[0], :] for index in range(QUARTERS)])
            for at, conv, behind in zip(rows, pieces[:2], pieces[2:]):
                query_f = query_ref[at, lanes].astype(jnp.float32)
                key_f = key_ref[at, lanes].astype(jnp.float32)
                value_f = value_ref[at, lanes].astype(jnp.float32)
                out_f = out_ref[at, lanes].astype(jnp.float32)
                conv = conv + skip * (key_f * value_f)
                behind = behind + skip * (out_f * query_f)
                gq_ref[at, lanes] = (out_f * conv).astype(jnp.bfloat16)
                gk_ref[at, lanes] = (behind * value_f).astype(jnp.bfloat16)
                gv_ref[at, lanes] = (behind * key_f).astype(jnp.bfloat16)

    def finish_corr(group):
        lanes = pl.ds(pl.multiple_of(group * LANES, LANES), LANES)
        pieces = transpose_quarters([corr[QUARTERS * group + index] for index in range(QUARTERS)])
        for k, piece in enumerate(pieces):
            gf_ref[part_tokens * k:part_tokens * (k + 1), lanes] = piece

    def join_half(group):
        far = FAR.index(group)
        for side in range(ch_count):
            for index in range(QUARTERS):
                piece = back_half[side * far_jobs + QUARTERS * far + index]
                left = left_mask(piece.shape)
                place_at = side * jobs + QUARTERS * group + index
                back[place_at, :part_tokens, :] += jnp.where(left, 0.0, piece)
                back[place_at, part_tokens:, :] += jnp.where(left, 0.0, swap_halves(piece))
        for index in range(QUARTERS):
            corr[QUARTERS * group + index] += corr_far[QUARTERS * far + index]

    for group in ORDER:
        owner, _, near_plane, _ = PLAN[group]
        mine = plane == owner
        if near_plane is not None:
            mine = mine | (plane == near_plane)
        for own in (0, 1):

            @pl.when(mine if own else jnp.logical_not(mine))
            def _():
                arrive(back, QUARTERS * ch_count - own, back_sem.at[group])
                arrive(corr, QUARTERS - own, corr_sem.at[group])

        if near_plane is not None:

            @pl.when(low == 1)
            def _():
                arrive(back_half, QUARTERS * ch_count, back_half_sem.at[group])
                arrive(corr_far, QUARTERS, corr_far_sem.at[group])
                join_half(group)

        finish(group, 0)
        finish(group, 1)
        finish_corr(group)

    for p in range(PLANES):
        is_low = p < PLANES // 2
        owned, local = len(OWNED[p]), len(LOCAL[p])
        direct = len(FAR) - (0 if p else len(RELAYED))

        @pl.when(plane == p)
        def _():
            depart(send, ch_count * jobs - owned - local, send_sem)
            depart(send_half, ch_count * QUARTERS * direct if is_low else 0, half_send_sem)
            depart(taps_send, jobs - owned - (0 if p else QUARTERS * len(RELAYED)), taps_send_sem)
            depart(taps_send, far_jobs - local if is_low else 0, local_taps_send_sem)
            depart(result, owned * (others if is_low else seq_count - 1) + local * (seq_count - 1), back_send_sem)
            depart(result_half, 0 if is_low else owned * seq_count, back_half_send_sem)
            depart(corr_result, owned * (seq_count - 1) + local * (half_seq - 1), corr_send_sem)
            if p == 1 and RELAYED:
                depart(relay, len(RELAYED) * ch_count * width, relay_sem)
                depart(taps_recv, len(RELAYED) * width, relay_taps_sem)


def tables(seq_count, tokens):
    index = np.arange(tokens)
    angle = 2.0 * np.pi / tokens * (index[:, None] * index[None, :] % tokens)
    cosine, sine = np.cos(angle), np.sin(angle)
    forward = np.block([[cosine, sine], [-sine, cosine]]).astype(np.float32)
    inverse = np.block([[cosine, -sine], [sine, cosine]]).astype(np.float32)

    def pieces(table):
        table = jnp.asarray(table)
        return jnp.stack(split_bf16(table))

    turn = 2.0 * np.pi / (2 * seq_count * tokens) * (np.arange(seq_count + 1)[:, None] * index[None, :])
    twiddle = jnp.asarray(np.stack([np.cos(turn).T, np.sin(turn).T]).astype(np.float32))
    return pieces(forward), pieces(inverse), twiddle


def hand_out(*refs):
    count = len(refs) // 2
    copies = [pltpu.make_async_copy(refs[i], refs[count + i], refs[-1].at[i]) for i in range(count)]
    for copy in copies:
        copy.start()
    for copy in copies:
        copy.wait()


def fast_shards(query_gate, key_input, value_input, grad_output, filter_raw, skip_gain):
    seq_count, ch_count = lax.axis_size("seq"), lax.axis_size("ch")
    _, tokens, channels = key_input.shape
    vmem = pl.BlockSpec(memory_space=pltpu.VMEM)
    jobs = QUARTERS * len(PLAN)
    far_jobs = QUARTERS * len(FAR)
    whole = lambda count: pltpu.VMEM((count, tokens // 2, LANES), jnp.float32)
    part = lambda count: pltpu.VMEM((count, tokens // QUARTERS, LANES), jnp.float32)
    spectrum = pltpu.VMEM((seq_count + AT_ONCE, 2, tokens, LANES), jnp.float32)
    turning = pltpu.VMEM((seq_count + 2 * AT_ONCE, 2, tokens, LANES), jnp.float32)
    lines = pltpu.VMEM((seq_count, tokens, LANES), jnp.float32)
    slots = SLOTS * seq_count
    wholes = max(ch_count * NEAR_SLOTS + len(LOCAL[1]), SLOTS, LOCAL_SLOTS) * seq_count
    single = pltpu.SemaphoreType.DMA
    several = lambda count: pltpu.SemaphoreType.DMA((count,))
    inputs = (query_gate[0], key_input[0], value_input[0], grad_output[0], filter_raw, skip_gain[None], *tables(seq_count, tokens))
    grads = pl.pallas_call(
        lambda *refs: layer_kernel(seq_count, ch_count, *refs),
        in_specs=[pl.BlockSpec(memory_space=pltpu.HBM)] * len(inputs),
        out_specs=[vmem] * 4,
        out_shape=[pltpu.VMEM((tokens, channels), jnp.bfloat16)] * 3 + [pltpu.VMEM((tokens, channels // ch_count), jnp.float32)],
        scratch_shapes=[pltpu.VMEM(array.shape, array.dtype) for array in inputs] + [several(len(inputs))] + [
            whole(ch_count * jobs), part(ch_count * far_jobs), part(jobs), whole(wholes), part(slots), part(slots),
            whole(wholes), part(slots), part(slots), whole(ch_count * jobs), part(ch_count * far_jobs), part(jobs), part(far_jobs),
            lines, lines, spectrum, spectrum, spectrum, turning, part(max(len(RELAYED), 1) * seq_count // 2),
            single, single, single, single,
            several(SLOTS + LOCAL_SLOTS), several(SLOTS), several(SLOTS + LOCAL_SLOTS),
            single, single, single, single, single,
            several(len(PLAN)), several(len(PLAN)), several(len(PLAN)), several(len(PLAN)),
        ],
        compiler_params=pltpu.CompilerParams(vmem_limit_bytes=VMEM_LIMIT, collective_id=0, has_side_effects=True),
        name="layer",
    )(*inputs)
    grads = pl.pallas_call(
        hand_out,
        in_specs=[vmem] * len(grads),
        out_specs=[pl.BlockSpec(memory_space=pltpu.HBM)] * len(grads),
        out_shape=[jax.ShapeDtypeStruct(array.shape, array.dtype) for array in grads],
        scratch_shapes=[several(len(grads))],
        compiler_params=pltpu.CompilerParams(vmem_limit_bytes=1024 * 1024),
        name="hand_out",
    )(*grads)
    return (grads[0][None], grads[1][None], grads[2][None], grads[3])


def solution(mesh):
    in_specs = (
        P("ch", "seq", None),
        P("ch", "seq", None),
        P("ch", "seq", None),
        P("ch", "seq", None),
        P("seq", None),
        P(),
    )
    out_specs = (P("ch", "seq", None), P("ch", "seq", None), P("ch", "seq", None), P("seq", "ch"))

    def body(*arrays):
        seq_count, ch_count = mesh.shape["seq"], mesh.shape["ch"]
        _, tokens, channels = arrays[0].shape
        fits = ch_count == 2 and tokens == LANES and seq_count == PLANES * QUARTERS and channels == ch_count * len(PLAN) * LANES
        return (fast_shards if fits else shards)(*arrays)

    return jax.shard_map(body, mesh=mesh, in_specs=in_specs, out_specs=out_specs, check_vma=False)
```

```python
import math

import numpy as np

import jax
import jax.numpy as jnp
from jax import lax
from jax.experimental import pallas as pl
from jax.experimental.pallas import tpu as pltpu
from jax.sharding import PartitionSpec as P


def angle_table(row_index, col_index, modulus):
    turn_count = row_index[:, None] * col_index[None, :] % modulus
    angles = turn_count.astype(jnp.float32) * (2.0 * math.pi / modulus)
    return (jnp.cos(angles), jnp.sin(angles))


def contract(pattern, table, operand):
    return jnp.einsum(
        pattern, table, operand, precision=lax.Precision.HIGHEST, preferred_element_type=jnp.float32
    )


def rotate(pattern, cos_table, sin_table, sense_sign, real_part, imag_part, want_imag):
    if imag_part is None:
        cos_term = contract(pattern, cos_table, real_part)
        return (cos_term, sense_sign * contract(pattern, sin_table, real_part))
    real_out = contract(pattern, cos_table, real_part) - sense_sign * contract(
        pattern, sin_table, imag_part
    )
    if not want_imag:
        return (real_out, None)
    imag_out = contract(pattern, cos_table, imag_part) + sense_sign * contract(
        pattern, sin_table, real_part
    )
    return (real_out, imag_out)


def twist(cos_table, sin_table, sense_sign, real_part, imag_part):
    return (
        real_part * cos_table - sense_sign * imag_part * sin_table,
        imag_part * cos_table + sense_sign * real_part * sin_table,
    )


def spectral_terms(z_real, z_imag, g_real, g_imag, h_real, h_imag):
    conv_real = z_real * h_real - z_imag * h_imag
    conv_imag = z_real * h_imag + z_imag * h_real
    back_real = h_real * g_real + h_imag * g_imag
    back_imag = h_real * g_imag - h_imag * g_real
    corr_real = z_real * g_real + z_imag * g_imag
    corr_imag = z_real * g_imag - z_imag * g_real
    return (conv_real - back_imag, conv_imag + back_real, corr_real, corr_imag)


def shards(query_gate, key_input, value_input, grad_output, filter_raw, skip_gain):
    seq_count = lax.axis_size("seq")
    key_f = key_input[0].astype(jnp.float32)
    value_f = value_input[0].astype(jnp.float32)
    out_f = grad_output[0].astype(jnp.float32)
    mixed = key_f * value_f
    gated = out_f * query_gate[0].astype(jnp.float32)
    tokens, channels = mixed.shape
    seq_length = tokens * seq_count
    full_length = 2 * seq_length
    inverse_scale = 1.0 / full_length
    filter_taps = filter_raw.astype(jnp.float32) * seq_length ** (-0.5)
    freq_one = jnp.arange(2 * seq_count, dtype=jnp.int32)
    block_index = jnp.arange(seq_count, dtype=jnp.int32)
    offset_index = jnp.arange(tokens, dtype=jnp.int32)
    cos_one, sin_one = angle_table(freq_one, block_index, 2 * seq_count)
    cos_inv, sin_inv = angle_table(block_index, freq_one, 2 * seq_count)
    cos_two, sin_two = angle_table(offset_index, offset_index, tokens)
    local_width = channels // seq_count
    arrived = (
        lax.all_to_all(mixed.T, "seq", split_axis=0, concat_axis=1, tiled=True),
        lax.all_to_all(gated.T, "seq", split_axis=0, concat_axis=1, tiled=True),
        lax.all_to_all(filter_taps.T, "seq", split_axis=0, concat_axis=1, tiled=True),
    )
    cos_tw, sin_tw = angle_table(freq_one, offset_index, full_length)
    spectra = []
    for line_data in arrived:
        lines = line_data.reshape(local_width, seq_count, tokens)
        real_part, imag_part = rotate("kn,cnm->ckm", cos_one, sin_one, -1.0, lines, None, True)
        real_part, imag_part = twist(cos_tw, sin_tw, -1.0, real_part, imag_part)
        spectra.append(rotate("jm,ckm->ckj", cos_two, sin_two, -1.0, real_part, imag_part, True))
    packed_real, packed_imag, corr_real, corr_imag = spectral_terms(
        spectra[0][0], spectra[0][1], spectra[1][0], spectra[1][1], spectra[2][0], spectra[2][1]
    )
    pr_mid, pi_mid = rotate("mj,ckj->ckm", cos_two, sin_two, 1.0, packed_real, packed_imag, True)
    pr_mid, pi_mid = twist(cos_tw, sin_tw, 1.0, pr_mid, pi_mid)
    cr_mid, ci_mid = rotate("mj,ckj->ckm", cos_two, sin_two, 1.0, corr_real, corr_imag, True)
    cr_mid, ci_mid = twist(cos_tw, sin_tw, 1.0, cr_mid, ci_mid)
    conv_lines, back_lines = rotate("nk,ckm->cnm", cos_inv, sin_inv, 1.0, pr_mid, pi_mid, True)
    corr_lines = rotate("nk,ckm->cnm", cos_inv, sin_inv, 1.0, cr_mid, ci_mid, False)[0]
    conv_lines = (conv_lines * inverse_scale).reshape(local_width, seq_length)
    back_lines = (back_lines * inverse_scale).reshape(local_width, seq_length)
    corr_lines = (corr_lines * inverse_scale).reshape(local_width, seq_length)
    returned = (
        lax.all_to_all(conv_lines, "seq", split_axis=1, concat_axis=0, tiled=True),
        lax.all_to_all(back_lines, "seq", split_axis=1, concat_axis=0, tiled=True),
        lax.all_to_all(corr_lines, "seq", split_axis=1, concat_axis=0, tiled=True),
    )
    conv_time = returned[0].T
    back_time = returned[1].T
    corr_time = returned[2].T
    conv_full = conv_time + skip_gain * mixed
    back_full = back_time + skip_gain * gated
    grad_query = (out_f * conv_full).astype(jnp.bfloat16)[None]
    grad_key = (back_full * value_f).astype(jnp.bfloat16)[None]
    grad_value = (back_full * key_f).astype(jnp.bfloat16)[None]
    grad_filter = lax.psum_scatter(
        corr_time * seq_length ** (-0.5), "ch", scatter_dimension=1, tiled=True
    )
    return (grad_query, grad_key, grad_value, grad_filter)


LANES = 128
VMEM_LIMIT = 60 * 1024 * 1024


def times_root(pair, turn, size):
    real, imag = pair
    turn %= size
    if turn == 0:
        return pair
    if 4 * turn == size:
        return (-imag, real)
    if 2 * turn == size:
        return (-real, -imag)
    if 4 * turn == 3 * size:
        return (imag, -real)
    cosine = math.cos(2.0 * math.pi * turn / size)
    sine = math.sin(2.0 * math.pi * turn / size)
    return (real * cosine - imag * sine, real * sine + imag * cosine)


def complex_dft(values, sense):
    size = len(values)
    if size == 1:
        return values
    even = complex_dft(values[0::2], sense)
    odd = complex_dft(values[1::2], sense)
    low, high = [], []
    for k in range(size // 2):
        er, ei = even[k]
        tr, ti = times_root(odd[k], sense * k, size)
        low.append((er + tr, ei + ti))
        high.append((er - tr, ei - ti))
    return low + high


def half_spectrum(values, size):
    if size == 2:
        return [(values[0] + values[1], None), (values[0] - values[1], None)]
    half, quarter = size // 2, size // 4
    if len(values) == half:
        total, difference = values, values
    else:
        total = [values[n] + values[n + half] for n in range(half)]
        difference = [values[n] - values[n + half] for n in range(half)]
    out = [None] * (half + 1)
    out[0::2] = half_spectrum(total, half)
    turned = [times_root((difference[n], -difference[n + quarter]), -n, size) for n in range(quarter)]
    for index, (real, imag) in enumerate(complex_dft(turned, -1)):
        k = 1 + 4 * index
        if k <= half:
            out[k] = (real, imag)
        else:
            out[size - k] = (real, -imag)
    return out


def real_from_half(terms, size, first_half):
    if size == 2:
        return [terms[0][0] + terms[1][0], terms[0][0] - terms[1][0]]
    half, quarter = size // 2, size // 4
    even = real_from_half(terms[0::2], half, False)
    chosen = []
    for index in range(quarter):
        k = 1 + 4 * index
        if k <= half:
            chosen.append(terms[k])
        else:
            real, imag = terms[size - k]
            chosen.append((real, -imag))
    turned = [times_root(pair, n, size) for n, pair in enumerate(complex_dft(chosen, 1))]
    odd = [pair[0] for pair in turned] + [-pair[1] for pair in turned]
    out = [even[n] + odd[n] for n in range(half)]
    if first_half:
        return out
    return out + [even[n] - odd[n] for n in range(half)]


def split_bf16(value):
    high = value.astype(jnp.bfloat16)
    return high, (value - high.astype(jnp.float32)).astype(jnp.bfloat16)


def three_dot(table_high, table_low, value):
    high, low = split_bf16(value)
    dot = lambda a, b: jnp.dot(a, b, preferred_element_type=jnp.float32)
    return dot(table_high, high) + (dot(table_high, low) + dot(table_low, high))


QUARTERS = 4
QUARTER = LANES // QUARTERS
PLANES = 4
AT_ONCE = 6
LATE = 2
PLAN = (
    (2, 0, 0, 0),
    (3, 0, 0, 1),
    (1, 0, None, None),
    (2, 1, 0, 2),
    (3, 1, 0, 3),
    (1, 1, None, None),
    (2, 2, 0, 4),
    (3, 2, 1, 0),
)
ORDER = (0, 1, 2, 3, 4, 5, 6, 7)
FAR = tuple(group for group, entry in enumerate(PLAN) if entry[2] is not None)
RELAYED = ()
OWNED = tuple(tuple(g for g, entry in enumerate(PLAN) if entry[0] == plane) for plane in range(PLANES))
LOCAL = tuple(tuple(g for g in FAR if PLAN[g][2] == plane) for plane in range(PLANES))
SLOTS = max(len(groups) for groups in OWNED)
LOCAL_SLOTS = max(len(groups) for groups in LOCAL)
NEAR_SLOTS = len(OWNED[1])


def left_mask(shape):
    return lax.broadcasted_iota(jnp.int32, shape, 1) < LANES // 2


def even_mask(shape):
    return lax.broadcasted_iota(jnp.int32, shape, 1) & QUARTER == 0


def swap_halves(value):
    return pltpu.roll(value, LANES // 2, 1)


def turn_quarters(value, count):
    count %= QUARTERS
    return pltpu.roll(value, count * QUARTER, 1) if count else value


def choose_quarters(values):
    lane = lax.broadcasted_iota(jnp.int32, values[0].shape, 1)
    out = values[-1]
    for index in reversed(range(QUARTERS - 1)):
        out = jnp.where(lane < (index + 1) * QUARTER, values[index], out)
    return out


def transpose_quarters(values):
    turned = [turn_quarters(value, index) for index, value in enumerate(values)]
    mixed = [choose_quarters([turned[(u - a) % QUARTERS] for u in range(QUARTERS)]) for a in range(QUARTERS)]
    return [turn_quarters(value, -index) for index, value in enumerate(mixed)]


def interleave(one, two):
    even = even_mask(one.shape)
    return jnp.where(even, one, turn_quarters(two, 1)), jnp.where(even, turn_quarters(one, -1), two)


def offsets(count):
    return sorted(range(count), key=lambda step: abs(2 * step - count))


def repeat(first, count, at_once, body):
    def several(index, carry):
        for inner in range(at_once):
            body(first + index * at_once + inner)
        return carry

    lax.fori_loop(0, (count - first) // at_once, several, 0)


def greet_all(seq_count, ch_count, me_seq, me_ch):
    barrier = pltpu.get_barrier_semaphore()
    for step in offsets(seq_count):
        for turn in range(ch_count):
            if step or turn:
                partner = {"seq": lax.rem(me_seq + step, seq_count), "ch": lax.rem(me_ch + turn, ch_count)}
                pl.semaphore_signal(barrier, inc=1, device_id=partner, device_id_type=pl.DeviceIdType.MESH)
    return barrier


def layer_kernel(
    seq_count, ch_count,
    query_hbm, key_hbm, value_hbm, out_hbm, filter_hbm, skip_hbm, fwd_hbm, inv_hbm, tw_hbm,
    gq_ref, gk_ref, gv_ref, gf_ref,
    query_ref, key_ref, value_ref, out_ref, filter_ref, skip_ref, fwd_ref, inv_ref, tw_ref, load_sem,
    send, send_half, taps_send, recv, recv_half, taps_recv,
    result, result_half, corr_result, back, back_half, corr, corr_far,
    lines, taps_lines, spec, taps_spec, corr_spec, tw_scr, relay,
    send_sem, half_send_sem, taps_send_sem, local_taps_send_sem,
    recv_sem, half_recv_sem, taps_recv_sem,
    back_send_sem, back_half_send_sem, corr_send_sem, relay_sem, relay_taps_sem,
    back_sem, back_half_sem, corr_sem, corr_far_sem,
):
    me_seq, me_ch = lax.axis_index("seq"), lax.axis_index("ch")
    tokens, channels = key_ref.shape
    half_tokens, part_tokens = tokens // 2, tokens // QUARTERS
    half_seq = seq_count // 2
    width = seq_count // PLANES
    plane, place = lax.div(me_seq, width), lax.rem(me_seq, width)
    high = lax.div(plane, PLANES // 2)
    low = 1 - high
    scale = (seq_count * tokens) ** -0.5
    side_channels = channels // ch_count
    jobs = QUARTERS * len(PLAN)
    far_jobs = QUARTERS * len(FAR)
    local_whole = NEAR_SLOTS * ch_count * seq_count
    local_part = NEAR_SLOTS * seq_count

    def look(table):
        out = 0
        for value, known in table:
            out = out + jnp.where(known, value, 0)
        return out

    loads = [
        pltpu.make_async_copy(source, target, load_sem.at[index])
        for index, (source, target) in enumerate((
            (key_hbm, key_ref), (value_hbm, value_ref), (out_hbm, out_ref), (query_hbm, query_ref), (filter_hbm, filter_ref),
            (tw_hbm, tw_ref), (fwd_hbm, fwd_ref), (inv_hbm, inv_ref), (skip_hbm, skip_ref),
        ))
    ]
    for load in loads:
        load.start()
    barrier = greet_all(seq_count, ch_count, me_seq, me_ch)

    def start(source, target, seq, ch, send_at, recv_at):
        pltpu.make_async_remote_copy(
            src_ref=source, dst_ref=target, send_sem=send_at, recv_sem=recv_at,
            device_id={"seq": seq, "ch": ch}, device_id_type=pl.DeviceIdType.MESH,
        ).start()

    def span(ref, count, send_at, recv_at):
        return pltpu.make_async_remote_copy(
            src_ref=ref.at[pl.ds(0, count)], dst_ref=ref.at[pl.ds(0, count)], send_sem=send_at, recv_sem=recv_at,
            device_id={"seq": me_seq, "ch": me_ch}, device_id_type=pl.DeviceIdType.MESH,
        )

    def arrive(ref, count, sem):
        span(ref, count, sem, sem).wait_recv()

    def depart(ref, count, sem):
        if count:
            span(ref, count, sem, sem).wait_send()

    def prepare(group, side):
        lanes = pl.ds(pl.multiple_of(side * side_channels + group * LANES, LANES), LANES)
        base = side * jobs + QUARTERS * group

        for chunk in range(half_tokens // 16):
            pieces = []
            rows = [pl.ds(chunk * 16 + first, 16) for first in (0, half_tokens)]
            for one, two in ((key_ref, value_ref), (out_ref, query_ref)):
                for at in rows:
                    pieces.append(one[at, lanes].astype(jnp.float32) * two[at, lanes].astype(jnp.float32))
            for index, piece in enumerate(transpose_quarters(pieces)):
                send[base + index, rows[0], :] = piece

    def halve(group, side):
        far = FAR.index(group)
        for index in range(QUARTERS):
            piece = send[side * jobs + QUARTERS * group + index]
            top, bottom = piece[:part_tokens], piece[part_tokens:]
            send_half[side * far_jobs + QUARTERS * far + index] = jnp.where(left_mask(top.shape), top, swap_halves(bottom))

    def prepare_taps(group):
        lanes = pl.ds(pl.multiple_of(me_ch * side_channels + group * LANES, LANES), LANES)
        pieces = [filter_ref[part_tokens * k:part_tokens * (k + 1), lanes].astype(jnp.float32) * scale for k in range(QUARTERS)]
        for index, piece in enumerate(transpose_quarters(pieces)):
            taps_send[QUARTERS * group + index] = piece

    def turns():
        return [(step, turn) for step in offsets(width) for turn in reversed(range(ch_count))]

    def send_taps(group):
        owner, slot, near_plane, near_slot = PLAN[group]
        far = near_plane is not None
        for step in offsets(width):
            at = lax.rem(place + step, width)
            source = taps_send.at[QUARTERS * group + at]

            def to_owner():
                start(source, taps_recv.at[slot * seq_count + me_seq], owner * width + at, me_ch, taps_send_sem, taps_recv_sem.at[slot])

            def to_local():
                start(
                    source, taps_recv.at[near_plane * local_part + near_slot * half_seq + me_seq], near_plane * width + at, me_ch,
                    local_taps_send_sem, taps_recv_sem.at[SLOTS + near_slot],
                )

            sends = plane != owner if step == 0 else plane >= 0
            if group in RELAYED:
                sends = sends & (plane > 0)
            pl.when(sends)(to_owner)
            if far:
                pl.when((low == 1) & (plane != near_plane) if step == 0 else low == 1)(to_local)

        @pl.when(plane == owner)
        def _():
            taps_recv[slot * seq_count + me_seq] = taps_send[QUARTERS * group + place]

        if far:

            @pl.when(plane == near_plane)
            def _():
                taps_recv[near_plane * local_part + near_slot * half_seq + me_seq] = taps_send[QUARTERS * group + place]

    def whole(group, target_plane, index, sem):
        for step, turn in turns():
            at, ch = lax.rem(place + step, width), lax.rem(me_ch + turn, ch_count)

            def go():
                start(send.at[ch * jobs + QUARTERS * group + at], recv.at[index], target_plane * width + at, ch, send_sem, sem)

            if step or turn:
                go()
            else:
                pl.when(plane != target_plane)(go)

                @pl.when(plane == target_plane)
                def _():
                    recv[index] = send[me_ch * jobs + QUARTERS * group + place]

    def send_group(group):
        owner, slot, near_plane, near_slot = PLAN[group]

        if near_plane is None:
            whole(group, owner, (slot * ch_count + me_ch) * seq_count + me_seq, recv_sem.at[slot])
            return

        @pl.when(plane > 0 if group in RELAYED else low == 1)
        def _():
            @pl.when(low == 1)
            def _():
                for step, turn in turns():
                    at, ch = lax.rem(place + step, width), lax.rem(me_ch + turn, ch_count)
                    start(
                        send_half.at[ch * far_jobs + QUARTERS * FAR.index(group) + at],
                        recv_half.at[slot * seq_count + me_ch * half_seq + me_seq],
                        owner * width + at, ch, half_send_sem, half_recv_sem.at[slot],
                    )

        @pl.when(high == 1)
        def _():
            whole(group, owner, (slot * ch_count + me_ch) * half_seq + me_seq - half_seq, recv_sem.at[slot])

    def send_local(group):
        owner, slot, near_plane, near_slot = PLAN[group]

        @pl.when(low == 1)
        def _():
            index = near_plane * local_whole + (near_slot * ch_count + me_ch) * half_seq + me_seq
            whole(group, near_plane, index, recv_sem.at[SLOTS + near_slot])

    def ready(group):
        other = lax.rem(me_ch + 1, ch_count)
        prepare_taps(group)
        prepare(group, other)
        prepare(group, me_ch)

        if group in FAR:
            pl.when(low == 1)(lambda: halves(group))

    def halves(group):
        halve(group, 0)
        halve(group, 1)

    for load in loads[:5]:
        load.wait()
    ready(0)
    pl.semaphore_wait(barrier, seq_count * ch_count - 1)

    for group in range(len(PLAN)):
        if group:
            ready(group)
        send_taps(group)
        send_group(group)
        if group - LATE in FAR:
            send_local(group - LATE)
    for group in range(len(PLAN) - LATE, len(PLAN)):
        if group in FAR:
            send_local(group)
    for load in loads[5:]:
        load.wait()
    for k in range(seq_count + 1):
        for part in range(2):
            tw_scr[k, part] = jnp.broadcast_to(tw_ref[part, :, k:k + 1], (tokens, LANES))

    def analyse(source, target, blocks):
        def body(chunk, carry):
            rows = pl.ds(pl.multiple_of(chunk * 8, 8), 8)
            for k, (real, imag) in enumerate(half_spectrum([source[n, rows, :] for n in range(blocks)], 2 * blocks)):
                target[k, 0, rows, :] = real
                target[k, 1, rows, :] = jnp.zeros_like(real) if imag is None else imag
            return carry

        lax.fori_loop(0, tokens // 8, body, 0)

    def synthesise(source, target, blocks):
        def body(chunk, carry):
            rows = pl.ds(pl.multiple_of(chunk * 8, 8), 8)
            terms = [(source[k, 0, rows, :], source[k, 1, rows, :]) for k in range(blocks + 1)]
            for n, value in enumerate(real_from_half(terms, 2 * blocks, True)):
                target[n, rows, :] = value
            return carry

        lax.fori_loop(0, tokens // 8, body, 0)

    def across(table, real, imag):
        both = three_dot(table[0], table[1], jnp.concatenate([real, imag], axis=0))
        return both[:tokens], both[tokens:]

    def convolve(blocks):
        stride = seq_count // blocks
        analyse(lines, spec, blocks)
        analyse(taps_lines, taps_spec, blocks)
        forward = (fwd_ref[0], fwd_ref[1])
        inverse = (inv_ref[0], inv_ref[1])

        def middle(index, carry):
            ks = [index * AT_ONCE + inner for inner in range(AT_ONCE)]
            turns_at = [(tw_scr[stride * k, 0], tw_scr[stride * k, 1]) for k in ks]
            reals, imags = [], []
            for k, (cosine, sine) in zip(ks, turns_at):
                for held in (spec, taps_spec):
                    real, imag = held[k, 0], held[k, 1]
                    reals.append(real * cosine + imag * sine)
                    imags.append(imag * cosine - real * sine)
            real, imag = across(forward, jnp.concatenate(reals, axis=1), jnp.concatenate(imags, axis=1))
            reals, imags = [], []
            for inner in range(AT_ONCE):
                first = 2 * LANES * inner
                a_r, a_i = real[:, first:first + LANES], imag[:, first:first + LANES]
                h_r, h_i = real[:, first + LANES:first + 2 * LANES], imag[:, first + LANES:first + 2 * LANES]
                h_i = jnp.where(left_mask(h_i.shape), h_i, -h_i)
                g_r, g_i = swap_halves(a_r), swap_halves(a_i)
                reals += [a_r * h_r - a_i * h_i, a_r * g_r + a_i * g_i]
                imags += [a_r * h_i + a_i * h_r, a_r * g_i - a_i * g_r]
            real, imag = across(inverse, jnp.concatenate(reals, axis=1), jnp.concatenate(imags, axis=1))
            for inner, (k, (cosine, sine)) in enumerate(zip(ks, turns_at)):
                weight = jnp.where((k == 0) | (k == blocks), 0.5 / (blocks * tokens), 1.0 / (blocks * tokens))
                cosine, sine = cosine * weight, sine * weight
                for side, held in enumerate((spec, corr_spec)):
                    first = LANES * (2 * inner + side)
                    br, bi = real[:, first:first + LANES], imag[:, first:first + LANES]
                    held[k, 0] = br * cosine - bi * sine
                    held[k, 1] = bi * cosine + br * sine
            return carry

        lax.fori_loop(0, blocks // AT_ONCE + 1, middle, 0)
        synthesise(spec, lines, blocks)
        synthesise(corr_spec, taps_lines, blocks)

    def open_taps(first, blocks):
        def body(n):
            packed = taps_recv[first + n]
            turned = [turn_quarters(packed, count) for count in range(QUARTERS)]
            for k in range(QUARTERS):
                taps_lines[n, part_tokens * k:part_tokens * (k + 1), :] = choose_quarters([turned[(u - k) % QUARTERS] for u in range(QUARTERS)])

        repeat(0, blocks, 8, body)

    def open_whole(start_at, blocks, first):
        def body(n):
            base = start_at + n - first
            top, bottom = interleave(recv[base], recv[base + blocks - first])
            lines[n, :half_tokens, :] = top
            lines[n, half_tokens:, :] = bottom

        repeat(first, blocks, 4, body)

    def open_half(slot):
        def body(n):
            one, two = recv_half[slot * seq_count + n], recv_half[slot * seq_count + half_seq + n]
            left = left_mask(one.shape)
            for first in (0, part_tokens):
                top, bottom = interleave(one, two)
                lines[n, first:first + part_tokens, :] = jnp.where(left, top, 0.0)
                lines[n, half_tokens + first:half_tokens + first + part_tokens, :] = jnp.where(left, bottom, 0.0)
                one, two = swap_halves(one), swap_halves(two)

        repeat(0, half_seq, 4, body)

    def close_whole(start_at, blocks, first):
        def body(n):
            base = start_at + n - first
            one, two = interleave(lines[n, :half_tokens, :], lines[n, half_tokens:, :])
            result[base] = one
            result[base + blocks - first] = two

        repeat(first, blocks, 4, body)

    def close_half(slot):
        def body(n):
            for index, piece in enumerate(interleave(lines[n, :half_tokens, :], lines[n, half_tokens:, :])):
                top, bottom = piece[:part_tokens], piece[part_tokens:]
                result_half[slot * seq_count + index * half_seq + n] = jnp.where(left_mask(top.shape), swap_halves(bottom), top)

        repeat(0, half_seq, 4, body)

    def close_corr(first, blocks):
        def body(n):
            pieces = []
            for k in range(QUARTERS):
                piece = taps_lines[n, part_tokens * k:part_tokens * (k + 1), :]
                pieces.append(turn_quarters((piece + turn_quarters(piece, -1)) * scale, k))
            corr_result[first + n] = choose_quarters(pieces)

        repeat(0, blocks, 4, body)

    def deliver(base, corr_base, group, first, count):
        job = QUARTERS * group + place
        for step in offsets(count):
            at = lax.rem(me_seq + step, count)
            for turn in range(ch_count):
                ch = lax.rem(me_ch + turn, ch_count)
                if step or turn:
                    start(result.at[base + ch * count + at], back.at[me_ch * jobs + job], first + at, ch, back_send_sem, back_sem.at[group])
            if step:
                start(corr_result.at[corr_base + first + at], corr.at[job], first + at, me_ch, corr_send_sem, corr_sem.at[group])
        back[me_ch * jobs + job] = result[base + me_ch * count + me_seq - first]
        corr[job] = corr_result[corr_base + me_seq]

    def deliver_half(slot, group):
        far = QUARTERS * look([(FAR.index(g), group == g) for g in FAR]) + place
        for step in offsets(half_seq):
            seq = lax.rem(me_seq + step, half_seq)
            for turn in range(ch_count):
                ch = lax.rem(me_ch + turn, ch_count)
                start(
                    result_half.at[slot * seq_count + ch * half_seq + seq], back_half.at[me_ch * far_jobs + far],
                    seq, ch, back_half_send_sem, back_half_sem.at[group],
                )
            start(corr_result.at[slot * seq_count + seq], corr_far.at[far], seq, me_ch, corr_send_sem, corr_far_sem.at[group])

    others = seq_count * ch_count - 1

    def owner_job(slot, carry):
        group = look([(g, (plane == PLAN[g][0]) & (slot == PLAN[g][1])) for g in range(len(PLAN))])
        arrive(taps_recv, seq_count - 1, taps_recv_sem.at[slot])
        open_taps(slot * seq_count, seq_count)
        near_base = slot * ch_count * seq_count
        far_base = slot * ch_count * half_seq

        @pl.when(high == 0)
        def _():
            arrive(recv, others, recv_sem.at[slot])
            open_whole(near_base, seq_count, 0)

        @pl.when(high == 1)
        def _():
            arrive(recv_half, seq_count, half_recv_sem.at[slot])
            open_half(slot)
            arrive(recv, seq_count - 1, recv_sem.at[slot])
            open_whole(far_base, seq_count, half_seq)

        convolve(seq_count)
        close_corr(slot * seq_count, seq_count)

        @pl.when(high == 0)
        def _():
            close_whole(near_base, seq_count, 0)
            deliver(near_base, slot * seq_count, group, 0, seq_count)

        @pl.when(high == 1)
        def _():
            close_half(slot)
            deliver_half(slot, group)
            close_whole(far_base, seq_count, half_seq)
            deliver(far_base, slot * seq_count, group, half_seq, half_seq)

        return carry

    def local_arrive(slot):
        arrive(taps_recv, half_seq - 1, taps_recv_sem.at[SLOTS + slot])
        arrive(recv, seq_count - 1, recv_sem.at[SLOTS + slot])

    def local_job(slot, carry):
        group = look([(g, (plane == PLAN[g][2]) & (slot == PLAN[g][3])) for g in FAR])
        base = plane * local_whole + slot * ch_count * half_seq
        part_base = plane * local_part + slot * half_seq
        pl.when(plane == 0)(lambda: local_arrive(slot)) if RELAYED else local_arrive(slot)
        open_taps(part_base, half_seq)
        open_whole(base, half_seq, 0)
        convolve(half_seq)
        close_corr(part_base, half_seq)
        close_whole(base, half_seq, 0)
        deliver(base, part_base, group, 0, half_seq)
        return carry

    def hand_on(group):
        owner, slot, near_plane, near_slot = PLAN[group]
        local_arrive(near_slot)
        seq = owner * width + place
        for n in range(width):
            start(
                taps_recv.at[near_plane * local_part + near_slot * half_seq + n], taps_recv.at[slot * seq_count + n],
                seq, me_ch, relay_taps_sem, taps_recv_sem.at[slot],
            )
        for ch in range(ch_count):
            for n in range(width):
                piece = recv[near_plane * local_whole + (near_slot * ch_count + ch) * half_seq + n]
                top, bottom = piece[:part_tokens], piece[part_tokens:]
                relay[(near_slot * ch_count + ch) * width + n] = jnp.where(left_mask(top.shape), top, swap_halves(bottom))
        for ch in range(ch_count):
            for n in range(width):
                start(
                    relay.at[(near_slot * ch_count + ch) * width + n], recv_half.at[slot * seq_count + ch * half_seq + n],
                    seq, me_ch, relay_sem, half_recv_sem.at[slot],
                )

    @pl.when(plane == 1)
    def _():
        for group in RELAYED:
            hand_on(group)

    lax.fori_loop(0, look([(len(groups), plane == p) for p, groups in enumerate(OWNED)]), owner_job, 0)
    lax.fori_loop(0, look([(len(groups), plane == p) for p, groups in enumerate(LOCAL)]), local_job, 0)

    def finish(group, side):
        lanes = pl.ds(pl.multiple_of(side * side_channels + group * LANES, LANES), LANES)
        base = side * jobs + QUARTERS * group
        skip = skip_ref[:, lanes]

        for chunk in range(half_tokens // 16):
            rows = [pl.ds(chunk * 16 + first, 16) for first in (0, half_tokens)]
            pieces = transpose_quarters([back[base + index, rows[0], :] for index in range(QUARTERS)])
            for at, conv, behind in zip(rows, pieces[:2], pieces[2:]):
                query_f = query_ref[at, lanes].astype(jnp.float32)
                key_f = key_ref[at, lanes].astype(jnp.float32)
                value_f = value_ref[at, lanes].astype(jnp.float32)
                out_f = out_ref[at, lanes].astype(jnp.float32)
                conv = conv + skip * (key_f * value_f)
                behind = behind + skip * (out_f * query_f)
                gq_ref[at, lanes] = (out_f * conv).astype(jnp.bfloat16)
                gk_ref[at, lanes] = (behind * value_f).astype(jnp.bfloat16)
                gv_ref[at, lanes] = (behind * key_f).astype(jnp.bfloat16)

    def finish_corr(group):
        lanes = pl.ds(pl.multiple_of(group * LANES, LANES), LANES)
        pieces = transpose_quarters([corr[QUARTERS * group + index] for index in range(QUARTERS)])
        for k, piece in enumerate(pieces):
            gf_ref[part_tokens * k:part_tokens * (k + 1), lanes] = piece

    def join_half(group):
        far = FAR.index(group)
        for side in range(ch_count):
            for index in range(QUARTERS):
                piece = back_half[side * far_jobs + QUARTERS * far + index]
                left = left_mask(piece.shape)
                place_at = side * jobs + QUARTERS * group + index
                back[place_at, :part_tokens, :] += jnp.where(left, 0.0, piece)
                back[place_at, part_tokens:, :] += jnp.where(left, 0.0, swap_halves(piece))
        for index in range(QUARTERS):
            corr[QUARTERS * group + index] += corr_far[QUARTERS * far + index]

    for group in ORDER:
        owner, _, near_plane, _ = PLAN[group]
        mine = plane == owner
        if near_plane is not None:
            mine = mine | (plane == near_plane)
        for own in (0, 1):

            @pl.when(mine if own else jnp.logical_not(mine))
            def _():
                arrive(back, QUARTERS * ch_count - own, back_sem.at[group])
                arrive(corr, QUARTERS - own, corr_sem.at[group])

        if near_plane is not None:

            @pl.when(low == 1)
            def _():
                arrive(back_half, QUARTERS * ch_count, back_half_sem.at[group])
                arrive(corr_far, QUARTERS, corr_far_sem.at[group])
                join_half(group)

        finish(group, 0)
        finish(group, 1)
        finish_corr(group)

    for p in range(PLANES):
        is_low = p < PLANES // 2
        owned, local = len(OWNED[p]), len(LOCAL[p])
        direct = len(FAR) - (0 if p else len(RELAYED))

        @pl.when(plane == p)
        def _():
            depart(send, ch_count * jobs - owned - local, send_sem)
            depart(send_half, ch_count * QUARTERS * direct if is_low else 0, half_send_sem)
            depart(taps_send, jobs - owned - (0 if p else QUARTERS * len(RELAYED)), taps_send_sem)
            depart(taps_send, far_jobs - local if is_low else 0, local_taps_send_sem)
            depart(result, owned * (others if is_low else seq_count - 1) + local * (seq_count - 1), back_send_sem)
            depart(result_half, 0 if is_low else owned * seq_count, back_half_send_sem)
            depart(corr_result, owned * (seq_count - 1) + local * (half_seq - 1), corr_send_sem)
            if p == 1 and RELAYED:
                depart(relay, len(RELAYED) * ch_count * width, relay_sem)
                depart(taps_recv, len(RELAYED) * width, relay_taps_sem)


def tables(seq_count, tokens):
    index = np.arange(tokens)
    angle = 2.0 * np.pi / tokens * (index[:, None] * index[None, :] % tokens)
    cosine, sine = np.cos(angle), np.sin(angle)
    forward = np.block([[cosine, sine], [-sine, cosine]]).astype(np.float32)
    inverse = np.block([[cosine, -sine], [sine, cosine]]).astype(np.float32)

    def pieces(table):
        table = jnp.asarray(table)
        return jnp.stack(split_bf16(table))

    turn = 2.0 * np.pi / (2 * seq_count * tokens) * (np.arange(seq_count + 1)[:, None] * index[None, :])
    twiddle = jnp.asarray(np.stack([np.cos(turn).T, np.sin(turn).T]).astype(np.float32))
    return pieces(forward), pieces(inverse), twiddle


def hand_out(*refs):
    count = len(refs) // 2
    copies = [pltpu.make_async_copy(refs[i], refs[count + i], refs[-1].at[i]) for i in range(count)]
    for copy in copies:
        copy.start()
    for copy in copies:
        copy.wait()


def fast_shards(query_gate, key_input, value_input, grad_output, filter_raw, skip_gain):
    seq_count, ch_count = lax.axis_size("seq"), lax.axis_size("ch")
    _, tokens, channels = key_input.shape
    vmem = pl.BlockSpec(memory_space=pltpu.VMEM)
    jobs = QUARTERS * len(PLAN)
    far_jobs = QUARTERS * len(FAR)
    whole = lambda count: pltpu.VMEM((count, tokens // 2, LANES), jnp.float32)
    part = lambda count: pltpu.VMEM((count, tokens // QUARTERS, LANES), jnp.float32)
    spectrum = pltpu.VMEM((seq_count + AT_ONCE, 2, tokens, LANES), jnp.float32)
    turning = pltpu.VMEM((seq_count + 2 * AT_ONCE, 2, tokens, LANES), jnp.float32)
    lines = pltpu.VMEM((seq_count, tokens, LANES), jnp.float32)
    slots = SLOTS * seq_count
    wholes = max(ch_count * NEAR_SLOTS + len(LOCAL[1]), SLOTS, LOCAL_SLOTS) * seq_count
    single = pltpu.SemaphoreType.DMA
    several = lambda count: pltpu.SemaphoreType.DMA((count,))
    inputs = (query_gate[0], key_input[0], value_input[0], grad_output[0], filter_raw, skip_gain[None], *tables(seq_count, tokens))
    grads = pl.pallas_call(
        lambda *refs: layer_kernel(seq_count, ch_count, *refs),
        in_specs=[pl.BlockSpec(memory_space=pltpu.HBM)] * len(inputs),
        out_specs=[vmem] * 4,
        out_shape=[pltpu.VMEM((tokens, channels), jnp.bfloat16)] * 3 + [pltpu.VMEM((tokens, channels // ch_count), jnp.float32)],
        scratch_shapes=[pltpu.VMEM(array.shape, array.dtype) for array in inputs] + [several(len(inputs))] + [
            whole(ch_count * jobs), part(ch_count * far_jobs), part(jobs), whole(wholes), part(slots), part(slots),
            whole(wholes), part(slots), part(slots), whole(ch_count * jobs), part(ch_count * far_jobs), part(jobs), part(far_jobs),
            lines, lines, spectrum, spectrum, spectrum, turning, part(max(len(RELAYED), 1) * seq_count // 2),
            single, single, single, single,
            several(SLOTS + LOCAL_SLOTS), several(SLOTS), several(SLOTS + LOCAL_SLOTS),
            single, single, single, single, single,
            several(len(PLAN)), several(len(PLAN)), several(len(PLAN)), several(len(PLAN)),
        ],
        compiler_params=pltpu.CompilerParams(vmem_limit_bytes=VMEM_LIMIT, collective_id=0, has_side_effects=True),
        name="layer",
    )(*inputs)
    grads = pl.pallas_call(
        hand_out,
        in_specs=[vmem] * len(grads),
        out_specs=[pl.BlockSpec(memory_space=pltpu.HBM)] * len(grads),
        out_shape=[jax.ShapeDtypeStruct(array.shape, array.dtype) for array in grads],
        scratch_shapes=[several(len(grads))],
        compiler_params=pltpu.CompilerParams(vmem_limit_bytes=1024 * 1024),
        name="hand_out",
    )(*grads)
    return (grads[0][None], grads[1][None], grads[2][None], grads[3])


def solution(mesh):
    in_specs = (
        P("ch", "seq", None),
        P("ch", "seq", None),
        P("ch", "seq", None),
        P("ch", "seq", None),
        P("seq", None),
        P(),
    )
    out_specs = (P("ch", "seq", None), P("ch", "seq", None), P("ch", "seq", None), P("seq", "ch"))

    def body(*arrays):
        seq_count, ch_count = mesh.shape["seq"], mesh.shape["ch"]
        _, tokens, channels = arrays[0].shape
        fits = ch_count == 2 and tokens == LANES and seq_count == PLANES * QUARTERS and channels == ch_count * len(PLAN) * LANES
        return (fast_shards if fits else shards)(*arrays)

    return jax.shard_map(body, mesh=mesh, in_specs=in_specs, out_specs=out_specs, check_vma=False)
```
